128 devices in a mesh: proto: 64 (over z, y, x), data: 2 (over core).
Axes of the slice: x: 4, y: 4, z: 4, core: 2. Of those that a mesh axis runs over, the one named last changes fastest.
Arguments:
- emb_one: bfloat16 [4096, 256], P('data')
- emb_two: bfloat16 [4096, 256], P('data')
- protos: bfloat16 [16384, 256], P('proto')
Outputs:
- output 1: float32 [4096, 16384], P('data', 'proto')
- output 2: float32 [4096, 16384], P('data', 'proto')
- output 3: float32 [], replicated
- output 4: float32 [4096, 256], P('data')
- output 5: float32 [4096, 256], P('data')
- output 6: float32 [16384, 256], P('proto')
All inputs are finite; a program needn't handle non-finite values.
Results may differ from the reference program's by a relative error of at most 0.001.
Values are sent between devices in bfloat16 or wider.
A program may use at most 1 GiB of HBM per device.

```python
import jax
import jax.numpy as jnp

ROWS_DEV = 2048
DATA_GROUPS = 2
NUM_PROTOS = 16384
EMBED_DIM = 256
SINKHORN_ITERS = 3
EPSILON = 0.05
TEMP_TAU = 0.1
NOISE_SCALE = 0.8
TOTAL_ROWS = ROWS_DEV * DATA_GROUPS


def unit_rows(matrix):
    return matrix / jnp.sqrt(jnp.sum(matrix * matrix, axis=1, keepdims=True))


def setup_inputs(seed: int = 0) -> dict:
    key = jax.random.key(seed)
    key_protos, key_home, key_one, key_two = jax.random.split(key, 4)
    protos = unit_rows(jax.random.normal(key_protos, (NUM_PROTOS, EMBED_DIM), jnp.float32))
    shard_ids = jnp.arange(TOTAL_ROWS, dtype=jnp.int32) // ROWS_DEV
    home_ids = shard_ids + DATA_GROUPS * jax.random.randint(key_home, (TOTAL_ROWS,), 0, NUM_PROTOS // DATA_GROUPS)
    centers = protos[home_ids]
    noise_one = jax.random.normal(key_one, (TOTAL_ROWS, EMBED_DIM), jnp.float32) * (NOISE_SCALE * EMBED_DIM ** -0.5)
    noise_two = jax.random.normal(key_two, (TOTAL_ROWS, EMBED_DIM), jnp.float32) * (NOISE_SCALE * EMBED_DIM ** -0.5)
    return {'emb_one': unit_rows(centers + noise_one).astype(jnp.bfloat16),
            'emb_two': unit_rows(centers + noise_two).astype(jnp.bfloat16),
            'protos': protos.astype(jnp.bfloat16)}


def sinkhorn_codes(scores):
    transport = jnp.exp(scores / EPSILON)
    for _ in range(SINKHORN_ITERS):
        col_sum = jnp.sum(transport, axis=0)
        transport = transport / (NUM_PROTOS * col_sum)
        row_sum = jnp.sum(transport, axis=1, keepdims=True)
        transport = transport / (TOTAL_ROWS * row_sum)
    return TOTAL_ROWS * transport


def log_probs(scores):
    logits = scores / TEMP_TAU
    return logits - jnp.log(jnp.sum(jnp.exp(logits), axis=1, keepdims=True))


def reference(emb_one, emb_two, protos):
    scores_one = jnp.dot(emb_one, protos.T, preferred_element_type=jnp.float32)
    scores_two = jnp.dot(emb_two, protos.T, preferred_element_type=jnp.float32)
    codes_one = sinkhorn_codes(scores_one)
    codes_two = sinkhorn_codes(scores_two)
    logp_one = log_probs(scores_one)
    logp_two = log_probs(scores_two)
    loss_value = -(jnp.sum(codes_two * logp_one) + jnp.sum(codes_one * logp_two)) / (2 * TOTAL_ROWS)
    grad_scale = 2 * TOTAL_ROWS * TEMP_TAU
    logit_grad_one = ((jnp.exp(logp_one) - codes_two) / grad_scale).astype(jnp.bfloat16)
    logit_grad_two = ((jnp.exp(logp_two) - codes_one) / grad_scale).astype(jnp.bfloat16)
    grad_one = jnp.dot(logit_grad_one, protos, preferred_element_type=jnp.float32)
    grad_two = jnp.dot(logit_grad_two, protos, preferred_element_type=jnp.float32)
    grad_protos = (jnp.dot(logit_grad_one.T, emb_one, preferred_element_type=jnp.float32)
                   + jnp.dot(logit_grad_two.T, emb_two, preferred_element_type=jnp.float32))
    return codes_one, codes_two, loss_value, grad_one, grad_two, grad_protos
```

```python
import functools

import jax
import jax.numpy as jnp
from jax import lax
from jax.experimental import pallas as pl
from jax.experimental.pallas import tpu as pltpu
from jax.sharding import PartitionSpec as P

EPSILON = 0.05
TEMP_TAU = 0.1
ITERS = 3
LINE = 4
AXES = 3
MESH = pl.DeviceIdType.MESH
F32 = jnp.float32
LANES = 128


def _nt(a, b):
    return lax.dot_general(a, b, (((1,), (1,)), ((), ())), preferred_element_type=F32)


def _eye():
    r = lax.broadcasted_iota(jnp.int32, (LANES, LANES), 0)
    c = lax.broadcasted_iota(jnp.int32, (LANES, LANES), 1)
    return r == c


def _parts(n):
    tiles = n // LANES
    cuts = [tiles * j // AXES * LANES for j in range(AXES + 1)]
    return [(cuts[j], cuts[j + 1]) for j in range(AXES)]


def sinkhorn_kernel(total_rows, total_protos, z1, z2, c_ref, r_out, v_out, d_out,
                    e_scr, cacc, vb, ub, stage, csend, crecv, first, later,
                    c_ssem, c_rsem, s_ssem, s_rsem):
    me = lax.axis_index('proto')
    core = lax.axis_index('data')
    rows = z1.shape[0]
    cols = c_ref.shape[0]
    parts = _parts(rows)
    pos = [lax.rem(me, LINE), lax.rem(me // LINE, LINE), me // (LINE * LINE)]
    stride = [1, LINE, LINE * LINE]

    def peer(axis, d):
        return me + (lax.rem(pos[axis] + d, LINE) - pos[axis]) * stride[axis]

    barrier = pltpu.get_barrier_semaphore()
    pl.semaphore_signal(barrier, inc=1, device_id=(me, 1 - core), device_id_type=MESH)
    for axis in range(AXES):
        for d in range(1, LINE):
            pl.semaphore_signal(barrier, inc=1, device_id=(peer(axis, d), core), device_id_type=MESH)

    cb = c_ref[...]
    for view, z in enumerate((z1, z2)):
        cacc[view] = jnp.zeros((cols, LANES), F32)

        def body(i, _, view=view, z=z):
            n0 = pl.multiple_of(i * 256, 256)
            s = _nt(cb, z[pl.ds(n0, 256), :])
            f = jnp.exp(s * (1.0 / TEMP_TAU))
            stage[0, 2 + view:3 + view, pl.ds(n0, 256)] = jnp.sum(f, axis=0, keepdims=True)
            e = f * f
            e_scr[view, :, pl.ds(n0, 256)] = e
            cacc[view] += e[:, :LANES] + e[:, LANES:]
            return 0
        lax.fori_loop(0, rows // 256, body, 0)

    pl.semaphore_wait(barrier, 1 + AXES * (LINE - 1))

    for it in range(ITERS):
        eye = _eye()
        for view in range(2):
            for h in range(2):
                s = jnp.sum(cacc[view, h * LANES:(h + 1) * LANES, :], axis=1, keepdims=True)
                csend[it, 2 * view + h:2 * view + h + 1, :] = jnp.sum(
                    jnp.where(eye, s, 0.0), axis=0, keepdims=True)
        cp = pltpu.make_async_remote_copy(csend.at[it], crecv.at[it], c_ssem.at[it], c_rsem.at[it],
                                          device_id=(me, 1 - core), device_id_type=MESH)
        cp.start()
        cp.wait()
        vrow = 1.0 / (float(total_protos) * (csend[it] + crecv[it]))
        if it == ITERS - 1:
            v_out[...] = vrow
        for view in range(2):
            for h in range(2):
                k = 2 * view + h
                col = jnp.sum(jnp.where(eye, vrow[k:k + 1, :], 0.0), axis=1, keepdims=True)
                vb[view, h * LANES:(h + 1) * LANES, :] = jnp.broadcast_to(col, (LANES, LANES))
        buf = first if it == 0 else later.at[it - 1]
        for view in range(2):
            def rbody(j, _, view=view):
                acc = [jnp.zeros((8, LANES), F32) for _ in range(4)]
                for g in range(cols // 8):
                    w = vb[view, 8 * g:8 * g + 8, :]
                    for t in range(4):
                        l0 = pl.multiple_of(j * 512 + t * LANES, LANES)
                        acc[t] = acc[t] + e_scr[view, 8 * g:8 * g + 8, pl.ds(l0, LANES)] * w
                for t in range(4):
                    l0 = pl.multiple_of(j * 512 + t * LANES, LANES)
                    stage[it, view:view + 1, pl.ds(l0, LANES)] = jnp.sum(acc[t], axis=0, keepdims=True)
                return 0
            lax.fori_loop(0, rows // 512, rbody, 0)
        for j, (l0, l1) in enumerate(parts):
            buf[0, pos[j], :, l0:l1] = stage[it, :buf.shape[2], l0:l1]
        for st in range(AXES):
            copies = []
            for d in (2, 1, 3):
                for j, (l0, l1) in enumerate(parts):
                    ax = (st + j) % AXES
                    idx = ((it * AXES + st) * AXES + j) * (LINE - 1) + d - 1
                    src = buf.at[st, pos[ax], :, l0:l1]
                    cp = pltpu.make_async_remote_copy(src, src, s_ssem.at[idx], s_rsem.at[idx],
                                                      device_id=(peer(ax, d), core), device_id_type=MESH)
                    cp.start()
                    copies.append(cp)
            for j, (l0, l1) in enumerate(parts):
                ax = (st + j) % AXES
                for d in range(1, LINE):
                    idx = ((it * AXES + st) * AXES + j) * (LINE - 1) + d - 1
                    dst = buf.at[st, lax.rem(pos[ax] + LINE - d, LINE), :, l0:l1]
                    pltpu.make_async_remote_copy(dst, dst, s_ssem.at[idx], s_rsem.at[idx],
                                                 device_id=(peer(ax, d), core), device_id_type=MESH).wait_recv()
                tot = (buf[st, 0, :, l0:l1] + buf[st, 1, :, l0:l1]) + (buf[st, 2, :, l0:l1] + buf[st, 3, :, l0:l1])
                if st < AXES - 1:
                    buf[st + 1, pos[(st + 1 + j) % AXES], :, l0:l1] = tot
                else:
                    if it == 0:
                        d_out[:, l0:l1] = tot[2:4]
                        tot = tot[0:2]
                    if it == ITERS - 1:
                        r_out[:, l0:l1] = tot
                    else:
                        u = 1.0 / (float(total_rows) * tot)
                        for view in range(2):
                            ub[view, :, l0:l1] = jnp.broadcast_to(u[view:view + 1], (8, l1 - l0))
            for cp in copies:
                cp.wait_send()
        if it < ITERS - 1:
            for view in range(2):
                def cbody(g, _, view=view):
                    for gg in range(4):
                        k0 = pl.multiple_of(g * 32 + gg * 8, 8)
                        acc = [None] * 4
                        for t in range(rows // LANES):
                            x = e_scr[view, pl.ds(k0, 8), t * LANES:(t + 1) * LANES] * ub[view, :, t * LANES:(t + 1) * LANES]
                            acc[t % 4] = x if acc[t % 4] is None else acc[t % 4] + x
                        cacc[view, pl.ds(k0, 8), :] = (acc[0] + acc[1]) + (acc[2] + acc[3])
                    return 0
                lax.fori_loop(0, cols // 32, cbody, 0)


def solution(mesh):
    proto_size = mesh.shape['proto']
    data_size = mesh.shape['data']

    def local_step(emb_one, emb_two, protos):
        rows, cols = emb_one.shape[0], protos.shape[0]
        total_rows = rows * data_size
        total_protos = cols * proto_size
        vm = pl.BlockSpec(memory_space=pltpu.VMEM)
        nsem = ITERS * AXES * AXES * (LINE - 1)
        r3, v3, den = pl.pallas_call(
            functools.partial(sinkhorn_kernel, total_rows, total_protos),
            out_shape=(jax.ShapeDtypeStruct((2, rows), F32),
                       jax.ShapeDtypeStruct((4, LANES), F32),
                       jax.ShapeDtypeStruct((2, rows), F32)),
            in_specs=[vm] * 3,
            out_specs=(vm,) * 3,
            scratch_shapes=[
                pltpu.VMEM((2, cols, rows), F32),
                pltpu.VMEM((2, cols, LANES), F32),
                pltpu.VMEM((2, cols, LANES), F32),
                pltpu.VMEM((2, 8, rows), F32),
                pltpu.VMEM((ITERS, 4, rows), F32),
                pltpu.VMEM((ITERS, 4, LANES), F32),
                pltpu.VMEM((ITERS, 4, LANES), F32),
                pltpu.VMEM((AXES, LINE, 4, rows), F32),
                pltpu.VMEM((ITERS - 1, AXES, LINE, 2, rows), F32),
                pltpu.SemaphoreType.DMA((ITERS,)),
                pltpu.SemaphoreType.DMA((ITERS,)),
                pltpu.SemaphoreType.DMA((nsem,)),
                pltpu.SemaphoreType.DMA((nsem,)),
            ],
            compiler_params=pltpu.CompilerParams(collective_id=0, has_side_effects=True),
        )(emb_one, emb_two, protos)
        vrow = v3.reshape(2, cols)

        def view_terms(emb, i):
            scores = jnp.einsum('nd,kd->nk', emb, protos, preferred_element_type=F32)
            logits = scores / TEMP_TAU
            codes = jnp.exp(scores / EPSILON) * vrow[i][None, :] / r3[i][:, None]
            return codes, logits - jnp.log(den[i])[:, None]

        codes_one, logp_one = view_terms(emb_one, 0)
        codes_two, logp_two = view_terms(emb_two, 1)
        part_loss = jnp.sum(codes_two * logp_one) + jnp.sum(codes_one * logp_two)
        loss_value = -lax.psum(part_loss, ('proto', 'data')) / (2 * total_rows)
        grad_scale = 2 * total_rows * TEMP_TAU
        hone = ((jnp.exp(logp_one) - codes_two) / grad_scale).astype(jnp.bfloat16)
        htwo = ((jnp.exp(logp_two) - codes_one) / grad_scale).astype(jnp.bfloat16)
        grad_one = lax.psum(jnp.einsum('nk,kd->nd', hone, protos, preferred_element_type=F32), 'proto')
        grad_two = lax.psum(jnp.einsum('nk,kd->nd', htwo, protos, preferred_element_type=F32), 'proto')
        proto_part = (jnp.einsum('nk,nd->kd', hone, emb_one, preferred_element_type=F32)
                      + jnp.einsum('nk,nd->kd', htwo, emb_two, preferred_element_type=F32))
        grad_protos = lax.psum(proto_part, 'data')
        return codes_one, codes_two, loss_value, grad_one, grad_two, grad_protos

    return jax.shard_map(
        local_step, mesh=mesh,
        in_specs=(P('data', None), P('data', None), P('proto', None)),
        out_specs=(P('data', 'proto'), P('data', 'proto'), P(), P('data', None), P('data', None), P('proto', None)),
        check_vma=False)
```

```python
import functools
import re

import jax
import jax.numpy as jnp
from jax import lax
from jax.experimental import pallas as pl
from jax.experimental.pallas import tpu as pltpu
from jax.sharding import PartitionSpec as P

EPSILON = 0.05
TEMP_TAU = 0.1
ITERS = 3
LINE = 4
AXES = 3
MESH = pl.DeviceIdType.MESH
F32 = jnp.float32
BF16 = jnp.bfloat16
LANES = 128
SUM_PARTS = ((0, 640), (640, 1280), (1280, 2048))
C_PARTS = ((0, 48), (48, 96), (96, 128))
G_PARTS = ((0, 24), (24, 48), (48, 64))
AG_SEMS = 27
SLOTS = (
    'S',
    'sA10A11A12A13',
    'a10B10a11B11a12B12a13B13A20T00T10T30',
    'A21b10b11b12b13T20a20B20T01T03',
    'A23a21B21T11T13b20T02',
    'A22a23B23T31T33b21T12',
    'a22B22T21T23b23T32',
    'b22T22UR0',
    'R1',
)


def _nt(a, b):
    return lax.dot_general(a, b, (((1,), (1,)), ((), ())), preferred_element_type=F32)


def _nn(a, b):
    return jnp.dot(a, b, preferred_element_type=F32)


def _col_to_row(s):
    r = lax.broadcasted_iota(jnp.int32, (LANES, LANES), 0)
    c = lax.broadcasted_iota(jnp.int32, (LANES, LANES), 1)
    return jnp.sum(jnp.where(r == c, s, 0.0), axis=0, keepdims=True)


def _row_to_col(row, n=LANES, shift=0):
    r = lax.broadcasted_iota(jnp.int32, (n, LANES), 0)
    c = lax.broadcasted_iota(jnp.int32, (n, LANES), 1)
    return jnp.sum(jnp.where(c == r + shift, row, 0.0), axis=1, keepdims=True)


class _Gather:
    def __init__(self, env, buf, row0, parts, ssem, rsem):
        self.env, self.buf, self.row0, self.parts = env, buf, row0, parts
        self.ssem, self.rsem = ssem, rsem

    def at(self, j, i0, i1, i2, row0=None):
        ids = [None] * AXES
        for axis, i in zip((j, j + 1, j + 2), (i0, i1, i2)):
            ids[axis % AXES] = slice(None) if i is None else i
        r0, r1 = self.parts[j]
        base = self.row0 if row0 is None else row0
        rows = pl.ds(base + r0, r1 - r0) if isinstance(base, int) else pl.ds(pl.multiple_of(base + r0, 16), r1 - r0)
        return self.buf.at[ids[2], ids[1], ids[0], rows, :]

    def p(self, j, level, d):
        return self.env.p((j + level) % AXES, d)

    def send(self, j, k, ref, level, d):
        env, i = self.env, j * AG_SEMS + k
        cp = pltpu.make_async_remote_copy(ref, ref, self.ssem.at[i], self.rsem.at[i],
                                          device_id=env.peer((j + level) % AXES, d), device_id_type=MESH)
        cp.start()
        env.pending.append(cp)

    def recv(self, j, k, ref):
        i = j * AG_SEMS + k
        pltpu.make_async_remote_copy(ref, ref, self.ssem.at[i], self.rsem.at[i],
                                     device_id=self.env.me2, device_id_type=MESH).wait_recv()

    def s1_send(self):
        for d in (2, 1, 3):
            for j in range(AXES):
                self.send(j, d - 1, self.at(j, self.p(j, 0, 0), self.p(j, 1, 0), self.p(j, 2, 0)), 0, d)

    def s1_recv(self):
        for d in (1, 3, 2):
            for j in range(AXES):
                self.recv(j, d - 1, self.at(j, self.p(j, 0, LINE - d), self.p(j, 1, 0), self.p(j, 2, 0)))

    def chunk(self, j, level, k, m):
        if level == 1:
            return self.at(j, self.p(j, 0, k), self.p(j, 1, m), self.p(j, 2, 0))
        return self.at(j, None, self.p(j, 1, k), self.p(j, 2, m))

    def a_send(self, level, k):
        base = 3 if level == 1 else 15
        for j in range(AXES):
            ref = self.chunk(j, level, k, 0)
            self.send(j, base + k, ref, level, 1)
            self.send(j, base + 4 + k, ref, level, 3)

    def a_recv(self, level, k):
        base = 3 if level == 1 else 15
        for j in range(AXES):
            self.recv(j, base + k, self.chunk(j, level, k, 3))
            self.recv(j, base + 4 + k, self.chunk(j, level, k, 1))

    def b_send(self, level, k):
        base = 11 if level == 1 else 23
        for j in range(AXES):
            if k < 2:
                self.send(j, base + k, self.chunk(j, level, k, 3), level, 1)
            else:
                self.send(j, base + k, self.chunk(j, level, k, 1), level, 3)

    def b_recv(self, level, k):
        base = 11 if level == 1 else 23
        for j in range(AXES):
            self.recv(j, base + k, self.chunk(j, level, k, 2))


class _Env:
    def __init__(self):
        self.me = lax.axis_index('proto')
        self.core = lax.axis_index('data')
        me = self.me
        self.pos = [lax.rem(me, LINE), lax.rem(lax.div(me, LINE), LINE), lax.div(me, LINE * LINE)]
        self.stride = [1, LINE, LINE * LINE]
        self.pending = []
        self.me2 = (me, 1 - self.core)

    def p(self, axis, d):
        return self.pos[axis] if d == 0 else lax.rem(self.pos[axis] + d, LINE)

    def peer(self, axis, d):
        return (self.me + (self.p(axis, d) - self.pos[axis]) * self.stride[axis], self.core)


def step_kernel(total_rows, total_protos, z1, z2, c_ref,
                code1, code2, loss_out, g1, g2, gp_out,
                f_scr, e_scr, cfull, lrow, frow, gfull, vall, zr, dvec,
                cacc, vb, ub, stage, csend, crecv, first, later, lossb, losst, dacc, drecv,
                lsem, c_ssem, c_rsem, s_ssem, s_rsem, a_ssem, a_rsem, t_ssem, t_rsem,
                v_ssem, v_rsem, g_ssem, g_rsem, l_ssem, l_rsem):
    env = _Env()
    me, core, pos = env.me, env.core, env.pos
    partner = env.me2
    rows, cols = z1.shape[0], c_ref.shape[0]
    half = cols // 2
    mine = zr.shape[0] // 2
    blocks = LINE ** AXES
    fscale = 1.0 / (2 * total_rows * TEMP_TAU)
    zs = (z1, z2)

    barrier = pltpu.get_barrier_semaphore()
    pl.semaphore_signal(barrier, inc=1, device_id=partner, device_id_type=MESH)
    for axis in range(AXES):
        for d in range(1, LINE):
            pl.semaphore_signal(barrier, inc=1, device_id=env.peer(axis, d), device_id_type=MESH)

    h0 = pl.multiple_of(core * half, half)
    own = pltpu.make_async_copy(c_ref.at[pl.ds(h0, half), :],
                                cfull.at[pos[2], pos[1], pos[0], pl.ds(h0, half), :], lsem.at[0])
    own.start()
    gc = _Gather(env, cfull, core * half, C_PARTS, a_ssem, a_rsem)
    gg = _Gather(env, gfull, 0, G_PARTS, g_ssem, g_rsem)

    def remote(src, dst, ss, rs, dev):
        cp = pltpu.make_async_remote_copy(src, dst, ss, rs, device_id=dev, device_id_type=MESH)
        cp.start()
        env.pending.append(cp)
        return cp

    def twin_send(k, m):
        for j in range(AXES):
            i = j * 16 + k * 4 + m
            ref = gc.chunk(j, 2, k, m)
            remote(ref, ref, t_ssem.at[i], t_rsem.at[i], partner)

    def twin_recv(k, m):
        for j in range(AXES):
            i = j * 16 + k * 4 + m
            ref = gc.at(j, None, gc.p(j, 1, k), gc.p(j, 2, m), row0=(1 - core) * half)
            pltpu.make_async_remote_copy(ref, ref, t_ssem.at[i], t_rsem.at[i],
                                         device_id=partner, device_id_type=MESH).wait_recv()

    cb = c_ref[...]
    for view, z in enumerate(zs):
        cacc[view] = jnp.zeros((cols, LANES), F32)

        def body(i, _, view=view, z=z):
            n0 = pl.multiple_of(i * 256, 256)
            s = _nt(cb, z[pl.ds(n0, 256), :])
            f = jnp.exp(s * (1.0 / TEMP_TAU))
            stage[0, 2 + view:3 + view, pl.ds(n0, 256)] = jnp.sum(f, axis=0, keepdims=True)
            e = f * f
            f_scr[view, :, pl.ds(n0, 256)] = f
            e_scr[view, :, pl.ds(n0, 256)] = e
            cacc[view] += e[:, :LANES] + e[:, LANES:]
            return 0
        lax.fori_loop(0, rows // 256, body, 0)
        zr[view * mine:(view + 1) * mine, :] = z[pl.ds(pl.multiple_of(me * mine, mine), mine), :]

    own.wait()
    pl.semaphore_wait(barrier, 1 + AXES * (LINE - 1))

    def gather_rows(lo, hi):
        def sbody(i, _):
            q = lax.div(i, 2)
            z_, y_, x_ = lax.div(q, 16), lax.rem(lax.div(q, 4), 4), lax.rem(q, 4)
            k0 = pl.multiple_of(lax.rem(i, 2) * half, half)
            l = _nt(zr[...], cfull[z_, y_, x_, pl.ds(k0, half), :]) * (1.0 / TEMP_TAU)
            lrow[q, :, pl.ds(k0, half)] = l
            frow[q, :, pl.ds(k0, half)] = jnp.exp(l)
            return 0
        lax.fori_loop(lo, hi, sbody, 0, unroll=4)

    def run(g, ops):
        for op in re.findall('[a-zA-Z][0-9]*', ops):
            args = [int(c) for c in op[1:]]
            {'S': g.s1_send, 's': g.s1_recv, 'A': g.a_send, 'a': g.a_recv, 'B': g.b_send, 'b': g.b_recv,
             'T': twin_send, 'U': twin_all, 'R': gather_half}[op[0]](*args)

    def twin_all():
        for k in range(LINE):
            for m in range(LINE):
                twin_recv(k, m)

    def gather_half(i):
        gather_rows(i * blocks, (i + 1) * blocks)

    for it in range(ITERS):
        for view in range(2):
            for h in range(2):
                s = jnp.sum(cacc[view, h * LANES:(h + 1) * LANES, :], axis=1, keepdims=True)
                k = 2 * view + h
                csend[it, k:k + 1, :] = _col_to_row(s)
        cp = remote(csend.at[it], crecv.at[it], c_ssem.at[it], c_rsem.at[it], partner)
        cp.wait_recv()
        vrow = 1.0 / (float(total_protos) * (csend[it] + crecv[it]))
        last = it == ITERS - 1
        if last:
            vall[pos[2], pos[1], pos[0]] = vrow
        for view in range(2):
            for h in range(2):
                k = 2 * view + h
                vb[view, h * LANES:(h + 1) * LANES, :] = jnp.broadcast_to(_row_to_col(vrow[k:k + 1, :]), (LANES, LANES))
        buf = first if it == 0 else later.at[it - 1]

        def vsend(st):
            ref = vall.at[(pos[2], pos[1], pos[0])[:AXES - st]]
            for d in (2, 1, 3):
                i = st * 3 + d - 1
                remote(ref, ref, v_ssem.at[i], v_rsem.at[i], env.peer(st, d))

        def vrecv(st):
            for d in (1, 3, 2):
                i = st * 3 + d - 1
                ids = [pos[2], pos[1], pos[0]][:AXES - st]
                ids[-1] = env.p(st, LINE - d)
                ref = vall.at[tuple(ids)]
                pltpu.make_async_remote_copy(ref, ref, v_ssem.at[i], v_rsem.at[i],
                                             device_id=partner, device_id_type=MESH).wait_recv()

        if last:
            vsend(0)
        for view in range(2):
            def rbody(j, _, view=view):
                acc = [jnp.zeros((8, LANES), F32) for _ in range(4)]
                for g in range(cols // 8):
                    w = vb[view, 8 * g:8 * g + 8, :]
                    for t in range(4):
                        l0 = pl.multiple_of(j * 512 + t * LANES, LANES)
                        acc[t] = acc[t] + e_scr[view, 8 * g:8 * g + 8, pl.ds(l0, LANES)] * w
                for t in range(4):
                    l0 = pl.multiple_of(j * 512 + t * LANES, LANES)
                    stage[it, view:view + 1, pl.ds(l0, LANES)] = jnp.sum(acc[t], axis=0, keepdims=True)
                return 0
            lax.fori_loop(0, rows // 512, rbody, 0)
        for j, (l0, l1) in enumerate(SUM_PARTS):
            buf[0, pos[j], :, l0:l1] = stage[it, :buf.shape[2], l0:l1]
        for st in range(AXES):
            for d in (2, 1, 3):
                for j, (l0, l1) in enumerate(SUM_PARTS):
                    ax = (st + j) % AXES
                    i = ((it * AXES + st) * AXES + j) * (LINE - 1) + d - 1
                    src = buf.at[st, pos[ax], :, l0:l1]
                    remote(src, src, s_ssem.at[i], s_rsem.at[i], env.peer(ax, d))
            run(gc, SLOTS[it * AXES + st])
            if last:
                vrecv(st)
                if st < AXES - 1:
                    vsend(st + 1)
            for j, (l0, l1) in enumerate(SUM_PARTS):
                ax = (st + j) % AXES
                for d in range(1, LINE):
                    i = ((it * AXES + st) * AXES + j) * (LINE - 1) + d - 1
                    dst = buf.at[st, env.p(ax, LINE - d), :, l0:l1]
                    pltpu.make_async_remote_copy(dst, dst, s_ssem.at[i], s_rsem.at[i],
                                                 device_id=partner, device_id_type=MESH).wait_recv()
                tot = (buf[st, 0, :, l0:l1] + buf[st, 1, :, l0:l1]) + (buf[st, 2, :, l0:l1] + buf[st, 3, :, l0:l1])
                if st < AXES - 1:
                    buf[st + 1, pos[(st + 1 + j) % AXES], :, l0:l1] = tot
                else:
                    if it == 0:
                        dvec[2:4, l0:l1] = tot[2:4]
                        tot = tot[0:2]
                    if last:
                        dvec[0:2, l0:l1] = tot
                    else:
                        u = 1.0 / (float(total_rows) * tot)
                        for view in range(2):
                            ub[view, :, l0:l1] = jnp.broadcast_to(u[view:view + 1], (8, l1 - l0))
        if not last:
            for view in range(2):
                def cbody(g, _, view=view):
                    for gi in range(4):
                        k0 = pl.multiple_of(g * 32 + gi * 8, 8)
                        acc = [None] * 4
                        for t in range(rows // LANES):
                            ls = slice(t * LANES, (t + 1) * LANES)
                            x = e_scr[view, pl.ds(k0, 8), ls] * ub[view, :, ls]
                            acc[t % 4] = x if acc[t % 4] is None else acc[t % 4] + x
                        cacc[view, pl.ds(k0, 8), :] = (acc[0] + acc[1]) + (acc[2] + acc[3])
                    return 0
                lax.fori_loop(0, cols // 32, cbody, 0)

    tile = pl.multiple_of(lax.div(me * mine, LANES) * LANES, LANES)
    shift = lax.rem(me * mine, LANES)
    dv = dvec[:, pl.ds(tile, LANES)]
    col = [_row_to_col(dv[i:i + 1, :], mine, shift) for i in range(4)]
    rc = jnp.broadcast_to(1.0 / jnp.concatenate(col[0:2], axis=0), (2 * mine, LANES))
    den = jnp.concatenate(col[2:4], axis=0)
    dc = jnp.broadcast_to(1.0 / den, (2 * mine, LANES))
    ld = jnp.broadcast_to(jnp.log(den), (2 * mine, LANES))

    def block(q):
        z_, y_, x_ = lax.div(q, 16), lax.rem(lax.div(q, 4), 4), lax.rem(q, 4)
        return z_, y_, x_

    def code_rows(q, h):
        z_, y_, x_ = block(q)
        f = frow[q, :, h * LANES:(h + 1) * LANES]
        v0 = jnp.broadcast_to(vall[z_, y_, x_, h:h + 1, :], (mine, LANES))
        v1 = jnp.broadcast_to(vall[z_, y_, x_, 2 + h:3 + h, :], (mine, LANES))
        return f, f * f * (rc * jnp.concatenate([v0, v1], axis=0))

    def dzbody(q, acc):
        z_, y_, x_ = block(q)
        hs = []
        for h in range(2):
            f, code = code_rows(q, h)
            other = jnp.concatenate([code[mine:], code[:mine]], axis=0)
            hs.append(((f * dc - other) * fscale).astype(BF16))
        return acc + _nn(jnp.concatenate(hs, axis=1), cfull[z_, y_, x_])

    gfull[pos[2], pos[1], pos[0]] = lax.fori_loop(0, blocks, dzbody, jnp.zeros((2 * mine, cols), F32), unroll=4)

    dacc[...] = jnp.zeros((cols, cols), F32)

    def columns(i):
        def body(i, _):
            n0 = pl.multiple_of(i * cols, cols)
            inv = 1.0 / dvec[:, pl.ds(n0, cols)]
            code, prob = [], []
            for view in range(2):
                w = jnp.concatenate([vb[view], vb[view]], axis=1)
                code.append(e_scr[view, :, pl.ds(n0, 256)] * w * inv[view:view + 1, :])
                prob.append(f_scr[view, :, pl.ds(n0, 256)] * inv[2 + view:3 + view, :])
            for view, out in enumerate((code1, code2)):
                h = ((prob[view] - code[1 - view]) * fscale).astype(BF16)
                dacc[...] += _nn(h, zs[view][pl.ds(n0, 256), :])
                out[pl.ds(n0, 256), :] = code[view].T
            return 0
        lax.fori_loop(i * 2, i * 2 + 2, body, 0)

    gg.s1_send()

    def lbody(q, acc):
        for h in range(2):
            f, code = code_rows(q, h)
            lp = lrow[q, :, h * LANES:(h + 1) * LANES] - ld
            other = jnp.concatenate([code[mine:], code[:mine]], axis=0)
            acc = acc + other * lp
        return acc
    part = lax.fori_loop(0, blocks, lbody, jnp.zeros((2 * mine, LANES), F32), unroll=2)
    lossb[0, pos[0]] = jnp.sum(part.reshape(2 * mine // 8, 8, LANES), axis=0)

    def loss_send(st):
        ref = lossb.at[st, pos[st]]
        for d in (2, 1, 3):
            i = st * 3 + d - 1
            remote(ref, ref, l_ssem.at[i], l_rsem.at[i], env.peer(st, d))

    def loss_recv(st):
        for d in (1, 3, 2):
            i = st * 3 + d - 1
            ref = lossb.at[st, env.p(st, LINE - d)]
            pltpu.make_async_remote_copy(ref, ref, l_ssem.at[i], l_rsem.at[i],
                                         device_id=partner, device_id_type=MESH).wait_recv()
        return (lossb[st, 0] + lossb[st, 1]) + (lossb[st, 2] + lossb[st, 3])

    run(gg, 'sA10A11A12A13')
    loss_send(0)
    run(gg, 'A20')
    columns(0)
    run(gg, 'a10B10a11B11a12B12a13B13A21A23')
    lossb[1, pos[1]] = loss_recv(0)
    loss_send(1)
    columns(1)
    run(gg, 'b10b11b12b13A22a20B20')
    lossb[2, pos[2]] = loss_recv(1)
    loss_send(2)
    columns(2)
    run(gg, 'a21B21a23B23')
    columns(3)
    losst[0] = loss_recv(2)
    lcp = remote(losst.at[0], losst.at[1], l_ssem.at[9], l_rsem.at[9], partner)
    dcp = remote(dacc, drecv, l_ssem.at[10], l_rsem.at[10], partner)
    run(gg, 'a22B22')
    lcp.wait_recv()
    loss_out[...] = jnp.sum(losst[0] + losst[1], keepdims=True) * (-1.0 / (2 * total_rows))
    dcp.wait_recv()
    gp_out[...] = dacc[...] + drecv[...]
    run(gg, 'b20b21b23b22')

    def obody(q, _):
        z_, y_, x_ = block(q)
        n0 = pl.multiple_of(q * mine, mine)
        g1[pl.ds(n0, mine), :] = gfull[z_, y_, x_, :mine, :]
        g2[pl.ds(n0, mine), :] = gfull[z_, y_, x_, mine:, :]
        return 0
    lax.fori_loop(0, blocks, obody, 0)
    for cp in env.pending:
        cp.wait_send()


def solution(mesh):
    proto_size = mesh.shape['proto']
    data_size = mesh.shape['data']

    def local_step(emb_one, emb_two, protos):
        rows, dim = emb_one.shape
        cols = protos.shape[0]
        total_rows = rows * data_size
        total_protos = cols * proto_size
        mine = rows // proto_size
        vm = pl.BlockSpec(memory_space=pltpu.VMEM)
        nsem = ITERS * AXES * AXES * (LINE - 1)
        dma = lambda n: pltpu.SemaphoreType.DMA((n,))
        grid3 = (LINE,) * AXES
        sds = jax.ShapeDtypeStruct
        code1, code2, loss, g1, g2, gp = pl.pallas_call(
            functools.partial(step_kernel, total_rows, total_protos),
            out_shape=(sds((rows, cols), F32), sds((rows, cols), F32), sds((1, 1), F32),
                       sds((rows, dim), F32), sds((rows, dim), F32), sds((cols, dim), F32)),
            in_specs=[vm] * 3,
            out_specs=(vm,) * 6,
            scratch_shapes=[
                pltpu.VMEM((2, cols, rows), F32),
                pltpu.VMEM((2, cols, rows), F32),
                pltpu.VMEM(grid3 + (cols, dim), BF16),
                pltpu.VMEM((proto_size, 2 * mine, cols), F32),
                pltpu.VMEM((proto_size, 2 * mine, cols), F32),
                pltpu.VMEM(grid3 + (2 * mine, dim), F32),
                pltpu.VMEM(grid3 + (4, LANES), F32),
                pltpu.VMEM((2 * mine, dim), BF16),
                pltpu.VMEM((4, rows), F32),
                pltpu.VMEM((2, cols, LANES), F32),
                pltpu.VMEM((2, cols, LANES), F32),
                pltpu.VMEM((2, 8, rows), F32),
                pltpu.VMEM((ITERS, 4, rows), F32),
                pltpu.VMEM((ITERS, 4, LANES), F32),
                pltpu.VMEM((ITERS, 4, LANES), F32),
                pltpu.VMEM((AXES, LINE, 4, rows), F32),
                pltpu.VMEM((ITERS - 1, AXES, LINE, 2, rows), F32),
                pltpu.VMEM((AXES, LINE, 8, LANES), F32),
                pltpu.VMEM((2, 8, LANES), F32),
                pltpu.VMEM((cols, dim), F32),
                pltpu.VMEM((cols, dim), F32),
                dma(1), dma(ITERS), dma(ITERS), dma(nsem), dma(nsem),
                dma(AXES * AG_SEMS), dma(AXES * AG_SEMS), dma(48), dma(48),
                dma(9), dma(9), dma(AXES * AG_SEMS), dma(AXES * AG_SEMS), dma(11), dma(11),
            ],
            compiler_params=pltpu.CompilerParams(collective_id=0, has_side_effects=True),
        )(emb_one, emb_two, protos)
        return code1, code2, loss[0, 0], g1, g2, gp

    return jax.shard_map(
        local_step, mesh=mesh,
        in_specs=(P('data', None), P('data', None), P('proto', None)),
        out_specs=(P('data', 'proto'), P('data', 'proto'), P(), P('data', None), P('data', None), P('proto', None)),
        check_vma=False)
```

```python
import functools
import re

import jax
import jax.numpy as jnp
from jax import lax
from jax.experimental import pallas as pl
from jax.experimental.pallas import tpu as pltpu
from jax.sharding import PartitionSpec as P

EPSILON = 0.05
TEMP_TAU = 0.1
ITERS = 3
LINE = 4
AXES = 3
MESH = pl.DeviceIdType.MESH
F32 = jnp.float32
BF16 = jnp.bfloat16
LANES = 128
SUM_CUTS = (0, 1408, 2816, 4096)
C_CUTS = (0, 80, 160, 256)
G_CUTS = (0, 24, 48, 64)
AG_SEMS = 27
DISTS = (2, 1, 3)


def _nt(a, b):
    return lax.dot_general(a, b, (((1,), (1,)), ((), ())), preferred_element_type=F32)


def _nn(a, b):
    return jnp.dot(a, b, preferred_element_type=F32)


def _col_to_row(s):
    r = lax.broadcasted_iota(jnp.int32, (LANES, LANES), 0)
    c = lax.broadcasted_iota(jnp.int32, (LANES, LANES), 1)
    return jnp.sum(jnp.where(r == c, s, 0.0), axis=0, keepdims=True)


def _row_to_col(row, n=LANES, shift=0):
    r = lax.broadcasted_iota(jnp.int32, (n, LANES), 0)
    c = lax.broadcasted_iota(jnp.int32, (n, LANES), 1)
    return jnp.sum(jnp.where(c == r + shift, row, 0.0), axis=1, keepdims=True)


def _parts(cuts):
    return tuple(zip(cuts[:-1], cuts[1:]))


class _Env:
    def __init__(self):
        self.me = lax.axis_index('proto')
        self.core = lax.axis_index('data')
        me = self.me
        self.pos = [lax.rem(me, LINE), lax.rem(lax.div(me, LINE), LINE), lax.div(me, LINE * LINE)]
        self.stride = [1, LINE, LINE * LINE]
        self.pending = []
        self.partner = (me, 1 - self.core)

    def p(self, axis, d):
        return self.pos[axis] if d == 0 else lax.rem(self.pos[axis] + d, LINE)

    def peer(self, axis, d):
        return (self.me + (self.p(axis, d) - self.pos[axis]) * self.stride[axis], self.core)

    def remote(self, src, dst, ss, rs, dev):
        cp = pltpu.make_async_remote_copy(src, dst, ss, rs, device_id=dev, device_id_type=MESH)
        cp.start()
        self.pending.append(cp)
        return cp

    def arrived(self, ref, rs):
        pltpu.make_async_remote_copy(ref, ref, rs, rs, device_id=self.partner, device_id_type=MESH).wait_recv()

    def drain(self):
        for cp in self.pending:
            cp.wait_send()
        self.pending = []


class _Gather:
    def __init__(self, env, buf, cuts, ssem, rsem, twin=None):
        self.env, self.buf, self.parts = env, buf, _parts(cuts)
        self.ssem, self.rsem, self.twin = ssem, rsem, twin

    def at(self, j, i0, i1, i2):
        ids = [None] * AXES
        for axis, i in zip((j, j + 1, j + 2), (i0, i1, i2)):
            ids[axis % AXES] = slice(None) if i is None else i
        r0, r1 = self.parts[j]
        return self.buf.at[ids[2], ids[1], ids[0], r0:r1, :]

    def p(self, j, level, d):
        return self.env.p((j + level) % AXES, d)

    def send(self, j, k, ref, level, d, src=None):
        i = j * AG_SEMS + k
        self.env.remote(ref if src is None else src, ref, self.ssem.at[i], self.rsem.at[i],
                        self.env.peer((j + level) % AXES, d))

    def recv(self, j, k, ref):
        self.env.arrived(ref, self.rsem.at[j * AG_SEMS + k])

    def s1_send(self, src=None):
        for d in DISTS:
            for j, (r0, r1) in enumerate(self.parts):
                ref = self.at(j, self.p(j, 0, 0), self.p(j, 1, 0), self.p(j, 2, 0))
                self.send(j, d - 1, ref, 0, d, None if src is None else src.at[r0:r1, :])

    def s1_recv(self):
        for d in (1, 3, 2):
            for j in range(AXES):
                self.recv(j, d - 1, self.at(j, self.p(j, 0, LINE - d), self.p(j, 1, 0), self.p(j, 2, 0)))

    def chunk(self, j, level, k, m):
        if level == 1:
            return self.at(j, self.p(j, 0, k), self.p(j, 1, m), self.p(j, 2, 0))
        return self.at(j, None, self.p(j, 1, k), self.p(j, 2, m))

    def a_send(self, level, k):
        base = 12 * level - 9
        for j in range(AXES):
            ref = self.chunk(j, level, k, 0)
            self.send(j, base + k, ref, level, 1)
            self.send(j, base + LINE + k, ref, level, 3)

    def a_recv(self, level, k):
        base = 12 * level - 9
        for j in range(AXES):
            self.recv(j, base + k, self.chunk(j, level, k, 3))
            self.recv(j, base + LINE + k, self.chunk(j, level, k, 1))

    def b_send(self, level, k):
        base = 12 * level - 1
        d = 1 if k < 2 else 3
        for j in range(AXES):
            self.send(j, base + k, self.chunk(j, level, k, LINE - d), level, d)

    def b_recv(self, level, k):
        base = 12 * level - 1
        for j in range(AXES):
            self.recv(j, base + k, self.chunk(j, level, k, 2))

    def t_send(self, k, m):
        ts, tr = self.twin
        for j in range(AXES):
            i = (j * LINE + k) * LINE + m
            ref = self.chunk(j, 2, k, m)
            self.env.remote(ref, ref, ts.at[i], tr.at[i], self.env.partner)

    def t_recv(self):
        for j in range(AXES):
            for k in range(LINE):
                for m in range(LINE):
                    self.env.arrived(self.chunk(j, 2, k, m), self.twin[1].at[(j * LINE + k) * LINE + m])

    def run(self, ops):
        for op in re.findall('[a-zA-Z][0-9]*', ops):
            args = [int(c) for c in op[1:]]
            {'S': self.s1_send, 's': self.s1_recv, 'A': self.a_send, 'a': self.a_recv,
             'B': self.b_send, 'b': self.b_recv, 'T': self.t_send, 'U': self.t_recv}[op[0]](*args)


def write_kernel(mine, code1, code2, gfull, gp, o1, o2, g1, g2, og, sem):
    pairs = [(code1, o1), (code2, o2), (gp, og)]
    for view, out in enumerate((g1, g2)):
        pairs.append((gfull.at[:, view * mine:(view + 1) * mine, :], out))
    copies = [pltpu.make_async_copy(src, dst, sem.at[i]) for i, (src, dst) in enumerate(pairs)]
    for cp in copies:
        cp.start()
    for cp in copies:
        cp.wait()


def step_kernel(total_rows, total_protos, z1h, z2h, ch,
                code1, code2, loss_out, gfull, gp_out,
                z1, z2, y1, y2, c_ref, f_scr, e_scr, cfull, lrow, frow, vall, zr, dall,
                cacc, vb, ub, stage, csend, crecv, first, later, lossb, losst, dacc, drecv, dz, cst,
                lsem, c_ssem, c_rsem, s_ssem, s_rsem, a_ssem, a_rsem, t_ssem, t_rsem,
                v_ssem, v_rsem, g_ssem, g_rsem, l_ssem, l_rsem, x_ssem, x_rsem, o_sem):
    env = _Env()
    me, core, pos, partner = env.me, env.core, env.pos, env.partner
    remote = env.remote
    rows, cols = z1.shape[0], c_ref.shape[0]
    mine = zr.shape[0] // 2
    blocks = LINE ** AXES
    fscale = 1.0 / (2 * total_rows * TEMP_TAU)
    zs, ys = (z1, z2), (y1, y2)
    chunks = rows // cols

    barrier = pltpu.get_barrier_semaphore()
    pl.semaphore_signal(barrier, inc=1, device_id=partner, device_id_type=MESH)
    for axis in range(AXES):
        for d in DISTS:
            pl.semaphore_signal(barrier, inc=1, device_id=env.peer(axis, d), device_id_type=MESH)
    loads = [pltpu.make_async_copy(src, dst, lsem.at[i]) for i, (src, dst) in enumerate(
        ((ch, c_ref), (z1h, z1), (z2h, z2), (ch, cfull.at[pos[2], pos[1], pos[0]])))]
    gc = _Gather(env, cfull, C_CUTS, a_ssem, a_rsem, (t_ssem, t_rsem))
    gg = _Gather(env, gfull, G_CUTS, g_ssem, g_rsem)
    for cp in loads[:3]:
        cp.start()

    def scores(view):
        cacc[view] = jnp.zeros((cols, LANES), F32)

        def body(i, _):
            n0 = pl.multiple_of(i * cols, cols)
            s = _nt(c_ref[...], zs[view][pl.ds(n0, cols), :])
            f = jnp.exp(s * (1.0 / TEMP_TAU))
            stage[0, 2 + view:3 + view, pl.ds(n0, cols)] = jnp.sum(f, axis=0, keepdims=True)
            e = f * f
            f_scr[view, :, pl.ds(n0, cols)] = f
            e_scr[view, :, pl.ds(n0, cols)] = e
            cacc[view] += e[:, :LANES] + e[:, LANES:]
            return 0
        lax.fori_loop(0, chunks, body, 0, unroll=2)
        zr[view * mine:(view + 1) * mine, :] = zs[view][pl.ds(pl.multiple_of(me * mine, mine), mine), :]

    def other_scores(view):
        def body(i, _):
            n0 = pl.multiple_of(i * cols, cols)
            f = jnp.exp(_nt(c_ref[...], ys[view][pl.ds(n0, cols), :]) * (1.0 / TEMP_TAU))
            e_scr[view, :, pl.ds(rows + n0, cols)] = f * f
            return 0
        lax.fori_loop(0, chunks, body, 0, unroll=2)

    def row_scores(lo, hi):
        def body(q, _):
            z_, y_, x_ = block(q)
            l = _nt(zr[...], cfull[z_, y_, x_]) * (1.0 / TEMP_TAU)
            lrow[q] = l
            frow[q] = jnp.exp(l)
            return 0
        lax.fori_loop(lo, hi, body, 0, unroll=2)

    def block(q):
        return lax.div(q, LINE * LINE), lax.rem(lax.div(q, LINE), LINE), lax.rem(q, LINE)

    def column_sums(it):
        for view in range(2):
            for h in range(2):
                k = 2 * view + h
                s = jnp.sum(cacc[view, h * LANES:(h + 1) * LANES, :], axis=1, keepdims=True)
                csend[it, k:k + 1, :] = _col_to_row(s)

    def spread(vrow):
        for view in range(2):
            for h in range(2):
                k = 2 * view + h
                vb[view, h * LANES:(h + 1) * LANES, :] = jnp.broadcast_to(
                    _row_to_col(vrow[k:k + 1, :]), (LANES, LANES))

    def exchange():
        cp = remote(csend.at[0], crecv.at[0], c_ssem.at[0], c_rsem.at[0], partner)
        cp.wait_recv()
        return csend[0] + crecv[0]

    def row_sums(it, width):
        step = 4 * LANES
        for view in range(2):
            def body(j, _, view=view):
                acc = [jnp.zeros((8, LANES), F32) for _ in range(4)]
                offs = [pl.multiple_of(j * step + t * LANES, LANES) for t in range(4)]
                for g in range(0, cols, 8):
                    w = vb[view, g:g + 8, :]
                    for t, l0 in enumerate(offs):
                        acc[t] = acc[t] + e_scr[view, g:g + 8, pl.ds(l0, LANES)] * w
                for t, l0 in enumerate(offs):
                    stage[it, view:view + 1, pl.ds(l0, LANES)] = jnp.sum(acc[t], axis=0, keepdims=True)
                return 0
            lax.fori_loop(0, width // step, body, 0)

    def weighted_columns():
        for view in range(2):
            def body(g, _, view=view):
                for gi in range(2):
                    k0 = pl.multiple_of(g * 16 + gi * 8, 8)
                    acc = [None] * 4
                    for t in range(2 * rows // LANES):
                        ls = slice(t * LANES, (t + 1) * LANES)
                        x = e_scr[view, pl.ds(k0, 8), ls] * ub[view, :, ls]
                        acc[t % 4] = x if acc[t % 4] is None else acc[t % 4] + x
                    cacc[view, pl.ds(k0, 8), :] = (acc[0] + acc[1]) + (acc[2] + acc[3])
                return 0
            lax.fori_loop(0, cols // 16, body, 0)

    def v_refs(st, d):
        ids = [pos[2], pos[1], pos[0]][:AXES - st]
        ids[-1] = env.p(st, d)
        return vall.at[tuple(ids)]

    def vsend(st):
        for d in DISTS:
            i = st * AXES + d - 1
            remote(v_refs(st, 0), v_refs(st, 0), v_ssem.at[i], v_rsem.at[i], env.peer(st, d))

    def vrecv(st):
        for d in DISTS:
            env.arrived(v_refs(st, LINE - d), v_rsem.at[st * AXES + d - 1])

    def hidden(slot):
        if slot in (0, 1):
            env.arrived(ys[slot], x_rsem.at[slot])
            other_scores(slot)
        elif slot == 6:
            gc.t_recv()
            row_scores(0, 20)
        elif slot == 7:
            row_scores(20, 42)
        elif slot == 8:
            row_scores(42, blocks)

    @pl.when(core == 1)
    def _():
        loads[0].wait()
        for view in range(2):
            loads[1 + view].wait()
            scores(view)
        pl.semaphore_wait(barrier, 1 + AXES * (LINE - 1))
        column_sums(0)
        total = exchange()
        for it in range(ITERS):
            last = it == ITERS - 1
            vrow = 1.0 / (float(total_protos) * total)
            if last:
                vall[pos[2], pos[1], pos[0]] = vrow
                vsend(0)
            spread(vrow)
            row_sums(it, rows if it == 0 else 2 * rows)
            buf = first if it == 0 else later.at[it - 1]
            if it == 0:
                env.arrived(stage.at[0, :, rows:], x_rsem.at[2])
            for j, (l0, l1) in enumerate(_parts(SUM_CUTS)):
                buf[0, pos[j], :, l0:l1] = stage[it, :buf.shape[2], l0:l1]
            for st in range(AXES):
                for d in DISTS:
                    for j, (l0, l1) in enumerate(_parts(SUM_CUTS)):
                        ax = (st + j) % AXES
                        i = ((it * AXES + st) * AXES + j) * (LINE - 1) + d - 1
                        src = buf.at[st, pos[ax], :, l0:l1]
                        remote(src, src, s_ssem.at[i], s_rsem.at[i], env.peer(ax, d))
                hidden(it * AXES + st)
                if last:
                    vrecv(st)
                    if st < AXES - 1:
                        vsend(st + 1)
                for j, (l0, l1) in enumerate(_parts(SUM_CUTS)):
                    ax = (st + j) % AXES
                    for d in DISTS:
                        i = ((it * AXES + st) * AXES + j) * (LINE - 1) + d - 1
                        env.arrived(buf.at[st, env.p(ax, LINE - d), :, l0:l1], s_rsem.at[i])
                    tot = (buf[st, 0, :, l0:l1] + buf[st, 1, :, l0:l1]) + (buf[st, 2, :, l0:l1] + buf[st, 3, :, l0:l1])
                    if st < AXES - 1:
                        buf[st + 1, pos[(st + 1 + j) % AXES], :, l0:l1] = tot
                        continue
                    if it == 0:
                        dall[2:4, l0:l1] = tot[2:4]
                    if last:
                        dall[0:2, l0:l1] = tot
                    else:
                        u = 1.0 / (float(total_rows) * tot)
                        for view in range(2):
                            ub[view, :, l0:l1] = jnp.broadcast_to(u[view:view + 1], (8, l1 - l0))
            if not last:
                weighted_columns()
                column_sums(it + 1)
                total = csend[it + 1]
        remote(dall.at[:, rows:], dall.at[:, :rows], x_ssem.at[3], x_rsem.at[3], partner)
        remote(vall, vall, x_ssem.at[4], x_rsem.at[4], partner)
        env.drain()

    @pl.when(core == 0)
    def _():
        loads[3].start()
        loads[0].wait()
        loads[3].wait()
        pl.semaphore_wait(barrier, 1 + AXES * (LINE - 1))
        gc.run('S')
        loads[1].wait()
        remote(z1, y1, x_ssem.at[0], x_rsem.at[0], partner)
        scores(0)
        gc.run('sA10A11A12A13A20T00')
        loads[2].wait()
        scores(1)
        column_sums(0)
        vrow = 1.0 / (float(total_protos) * exchange())
        spread(vrow)
        row_sums(0, rows)
        remote(stage.at[0, :, :rows], stage.at[0, :, rows:], x_ssem.at[2], x_rsem.at[2], partner)
        remote(z2, y2, x_ssem.at[1], x_rsem.at[1], partner)
        gc.run('a10B10a11B11a12B12a13B13A21A23T10T30')
        gc.run('a20B20T01T03b10b11b12b13A22T20')
        gc.run('a21B21T11T13a23B23T31T33')
        gc.run('b20T02b21T12b23T32')
        gc.run('a22B22T21T23b22T22')
        row_scores(0, blocks)
        env.arrived(dall.at[:, :rows], x_rsem.at[3])
        env.arrived(vall, x_rsem.at[4])
        env.drain()

    tile = pl.multiple_of(lax.div(me * mine, LANES) * LANES, LANES)
    shift = lax.rem(me * mine, LANES)
    dv = dall[:, pl.ds(tile, LANES)]
    col = [_row_to_col(dv[i:i + 1, :], mine, shift) for i in range(4)]
    rc = jnp.broadcast_to(1.0 / jnp.concatenate(col[0:2], axis=0), (2 * mine, LANES))
    den = jnp.concatenate(col[2:4], axis=0)
    dc = jnp.broadcast_to(1.0 / den, (2 * mine, LANES))
    ld = jnp.broadcast_to(jnp.log(den), (2 * mine, LANES))

    def code_rows(q, h):
        z_, y_, x_ = block(q)
        f = frow[q, :, h * LANES:(h + 1) * LANES]
        v0 = jnp.broadcast_to(vall[z_, y_, x_, h:h + 1, :], (mine, LANES))
        v1 = jnp.broadcast_to(vall[z_, y_, x_, 2 + h:3 + h, :], (mine, LANES))
        return f, f * f * (rc * jnp.concatenate([v0, v1], axis=0))

    def dzbody(i, acc):
        hs = []
        for x_ in range(LINE):
            for h in range(2):
                f, code = code_rows(i * LINE + x_, h)
                other = jnp.concatenate([code[mine:], code[:mine]], axis=0)
                hs.append(((f * dc - other) * fscale).astype(BF16))
        cl = cfull[lax.div(i, LINE), lax.rem(i, LINE)].reshape(LINE * cols, cols)
        return acc + _nn(jnp.concatenate(hs, axis=1), cl)

    dz[...] = lax.fori_loop(0, LINE * LINE, dzbody, jnp.zeros((2 * mine, cols), F32), unroll=2)

    own = pltpu.make_async_copy(dz, gfull.at[pos[2], pos[1], pos[0]], o_sem.at[0])
    own.start()
    gg.s1_send(dz)
    spread(vall[pos[2], pos[1], pos[0]])
    dacc[...] = jnp.zeros((cols, cols), F32)

    def out_copy(view, i):
        n0 = pl.multiple_of(i * cols, cols)
        return pltpu.make_async_copy(cst.at[view, pl.ds(n0, cols), :], (code1, code2)[view].at[pl.ds(n0, cols), :],
                                     o_sem.at[2 + view * chunks + i])

    def columns(i):
        def body(i, _):
            n0 = pl.multiple_of(i * cols, cols)
            inv = 1.0 / dall[:, pl.ds(n0, cols)]
            code, prob = [], []
            for view in range(2):
                w = jnp.concatenate([vb[view], vb[view]], axis=1)
                code.append(e_scr[view, :, pl.ds(n0, cols)] * w * inv[view:view + 1, :])
                prob.append(f_scr[view, :, pl.ds(n0, cols)] * inv[2 + view:3 + view, :])
            for view in range(2):
                h = ((prob[view] - code[1 - view]) * fscale).astype(BF16)
                dacc[...] += _nn(h, zs[view][pl.ds(n0, cols), :])
                cst[view, pl.ds(n0, cols), :] = code[view].T
                out_copy(view, i).start()
            return 0
        lax.fori_loop(i * 2, i * 2 + 2, body, 0)

    def lbody(q, acc):
        for h in range(2):
            f, code = code_rows(q, h)
            lp = lrow[q, :, h * LANES:(h + 1) * LANES] - ld
            other = jnp.concatenate([code[mine:], code[:mine]], axis=0)
            acc = acc + other * lp
        return acc
    part = lax.fori_loop(0, blocks, lbody, jnp.zeros((2 * mine, LANES), F32), unroll=2)
    lossb[0, pos[0]] = jnp.sum(part.reshape(2 * mine // 8, 8, LANES), axis=0)

    def loss_send(st):
        ref = lossb.at[st, pos[st]]
        for d in DISTS:
            i = st * AXES + d - 1
            remote(ref, ref, l_ssem.at[i], l_rsem.at[i], env.peer(st, d))

    def loss_recv(st):
        for d in DISTS:
            env.arrived(lossb.at[st, env.p(st, LINE - d)], l_rsem.at[st * AXES + d - 1])
        return (lossb[st, 0] + lossb[st, 1]) + (lossb[st, 2] + lossb[st, 3])

    own.wait()
    gg.run('sA10A11A12A13')
    loss_send(0)
    gg.run('A20')
    columns(0)
    gg.run('a10B10a11B11a12B12a13B13A21A23')
    lossb[1, pos[1]] = loss_recv(0)
    loss_send(1)
    columns(1)
    gg.run('b10b11b12b13A22a20B20')
    lossb[2, pos[2]] = loss_recv(1)
    loss_send(2)
    columns(2)
    gg.run('a21B21a23B23')
    columns(3)
    losst[0] = loss_recv(2)
    lcp = remote(losst.at[0], losst.at[1], l_ssem.at[9], l_rsem.at[9], partner)
    dcp = remote(dacc, drecv, l_ssem.at[10], l_rsem.at[10], partner)
    gg.run('a22B22')
    lcp.wait_recv()
    loss_out[...] = jnp.sum(losst[0] + losst[1], keepdims=True) * (-1.0 / (2 * total_rows))
    dcp.wait_recv()
    drecv[...] = dacc[...] + drecv[...]
    gpc = pltpu.make_async_copy(drecv, gp_out, o_sem.at[1])
    gpc.start()
    gg.run('b20b21b23b22')
    gpc.wait()
    for view in range(2):
        for i in range(chunks):
            out_copy(view, i).wait()
    env.drain()


def solution(mesh):
    proto_size = mesh.shape['proto']
    data_size = mesh.shape['data']

    def local_step(emb_one, emb_two, protos):
        rows, dim = emb_one.shape
        cols = protos.shape[0]
        total_rows = rows * data_size
        total_protos = cols * proto_size
        mine = rows // proto_size
        vm = pl.BlockSpec(memory_space=pltpu.VMEM)
        hbm = pl.BlockSpec(memory_space=pltpu.HBM)
        free = pl.BlockSpec(memory_space=pl.ANY)
        nsem = ITERS * AXES * AXES * (LINE - 1)
        dma = lambda n: pltpu.SemaphoreType.DMA((n,))
        grid3 = (LINE,) * AXES
        sds = jax.ShapeDtypeStruct
        code = sds((rows, cols), F32)
        zbuf = pltpu.VMEM((rows, dim), BF16)
        square = pltpu.VMEM((cols, dim), F32)
        rowbuf = pltpu.VMEM((proto_size, 2 * mine, cols), F32)
        small = pltpu.VMEM((ITERS, 4, LANES), F32)
        spread = pltpu.VMEM((2, cols, LANES), F32)
        args = [pltpu.with_memory_space_constraint(a, pltpu.HBM) for a in (emb_one, emb_two, protos)]
        code1, code2, loss, gall, gp = pl.pallas_call(
            functools.partial(step_kernel, total_rows, total_protos),
            out_shape=(code, code, sds((1, 1), F32),
                       sds(grid3 + (2 * mine, dim), F32), sds((cols, dim), F32)),
            in_specs=[hbm] * 3,
            out_specs=(free, free, vm, free, free),
            scratch_shapes=[
                zbuf, zbuf, zbuf, zbuf, pltpu.VMEM((cols, dim), BF16),
                pltpu.VMEM((2, cols, rows), F32),
                pltpu.VMEM((2, cols, 2 * rows), F32),
                pltpu.VMEM(grid3 + (cols, dim), BF16),
                rowbuf, rowbuf,
                pltpu.VMEM(grid3 + (4, LANES), F32),
                pltpu.VMEM((2 * mine, dim), BF16),
                pltpu.VMEM((4, total_rows), F32),
                spread, spread,
                pltpu.VMEM((2, 8, total_rows), F32),
                pltpu.VMEM((ITERS, 4, total_rows), F32),
                small, small,
                pltpu.VMEM((AXES, LINE, 4, total_rows), F32),
                pltpu.VMEM((ITERS - 1, AXES, LINE, 2, total_rows), F32),
                pltpu.VMEM((AXES, LINE, 8, LANES), F32),
                pltpu.VMEM((2, 8, LANES), F32),
                square, square,
                pltpu.VMEM((2 * mine, dim), F32),
                pltpu.VMEM((2, rows, cols), F32),
                dma(4), dma(ITERS), dma(ITERS), dma(nsem), dma(nsem),
                dma(AXES * AG_SEMS), dma(AXES * AG_SEMS), dma(48), dma(48),
                dma(9), dma(9), dma(AXES * AG_SEMS), dma(AXES * AG_SEMS), dma(11), dma(11),
                dma(5), dma(5), dma(2 + 2 * rows // cols),
            ],
            compiler_params=pltpu.CompilerParams(collective_id=0, has_side_effects=True,
                                                 vmem_limit_bytes=44 * 2 ** 20),
        )(*args)
        blocked = sds((proto_size, mine, dim), F32)
        o1, o2, g1, g2, og = pl.pallas_call(
            functools.partial(write_kernel, mine),
            out_shape=(code, code, blocked, blocked, sds((cols, dim), F32)),
            in_specs=[vm] * 4,
            out_specs=(hbm,) * 5,
            scratch_shapes=[dma(5)],
            compiler_params=pltpu.CompilerParams(vmem_limit_bytes=2 ** 20),
        )(code1, code2, gall.reshape(proto_size, 2 * mine, dim), gp)
        return o1, o2, loss[0, 0], g1.reshape(rows, dim), g2.reshape(rows, dim), og

    return jax.shard_map(
        local_step, mesh=mesh,
        in_specs=(P('data', None), P('data', None), P('proto', None)),
        out_specs=(P('data', 'proto'), P('data', 'proto'), P(), P('data', None), P('data', None), P('proto', None)),
        check_vma=False)
```

```python
import functools
import re

import jax
import jax.numpy as jnp
from jax import lax
from jax.experimental import pallas as pl
from jax.experimental.pallas import tpu as pltpu
from jax.sharding import PartitionSpec as P

EPSILON = 0.05
TEMP_TAU = 0.1
ITERS = 3
LINE = 4
AXES = 3
MESH = pl.DeviceIdType.MESH
F32 = jnp.float32
BF16 = jnp.bfloat16
LANES = 128
SUM_CUTS = (0, 1408, 2816, 4096)
C_CUTS = (0, 80, 160, 256)
G_CUTS = (0, 24, 48, 64)
AG_SEMS = 19
DISTS = (2, 1, 3)


def _nt(a, b):
    return lax.dot_general(a, b, (((1,), (1,)), ((), ())), preferred_element_type=F32)


def _nn(a, b):
    return jnp.dot(a, b, preferred_element_type=F32)


def _col_to_row(s):
    r = lax.broadcasted_iota(jnp.int32, (LANES, LANES), 0)
    c = lax.broadcasted_iota(jnp.int32, (LANES, LANES), 1)
    return jnp.sum(jnp.where(r == c, s, 0.0), axis=0, keepdims=True)


def _row_to_col(row, n=LANES, shift=0):
    r = lax.broadcasted_iota(jnp.int32, (n, LANES), 0)
    c = lax.broadcasted_iota(jnp.int32, (n, LANES), 1)
    return jnp.sum(jnp.where(c == r + shift, row, 0.0), axis=1, keepdims=True)


def _parts(cuts):
    return tuple(zip(cuts[:-1], cuts[1:]))


class _Env:
    def __init__(self):
        self.me = lax.axis_index('proto')
        self.core = lax.axis_index('data')
        me = self.me
        self.pos = [lax.rem(me, LINE), lax.rem(lax.div(me, LINE), LINE), lax.div(me, LINE * LINE)]
        self.stride = [1, LINE, LINE * LINE]
        self.pending = []
        self.partner = (me, 1 - self.core)

    def p(self, axis, d):
        return self.pos[axis] if d == 0 else lax.rem(self.pos[axis] + d, LINE)

    def peer(self, axis, d):
        return (self.me + (self.p(axis, d) - self.pos[axis]) * self.stride[axis], self.core)

    def remote(self, src, dst, ss, rs, dev):
        cp = pltpu.make_async_remote_copy(src, dst, ss, rs, device_id=dev, device_id_type=MESH)
        cp.start()
        return cp

    def sent(self, ref, ss):
        self.pending.append(pltpu.make_async_remote_copy(ref, ref, ss, ss, device_id=self.partner,
                                                         device_id_type=MESH))

    def arrived(self, ref, rs):
        pltpu.make_async_remote_copy(ref, ref, rs, rs, device_id=self.partner, device_id_type=MESH).wait_recv()

    def drain(self):
        for cp in self.pending:
            cp.wait_send()
        self.pending.clear()


class _Gather:
    def __init__(self, env, buf, cuts, ssem, rsem, twin=None):
        self.env, self.buf, self.parts = env, buf, _parts(cuts)
        self.ssem, self.rsem, self.twin = ssem, rsem, twin

    def at(self, j, i0, i1, i2):
        ids = [None] * AXES
        for axis, i in zip((j, j + 1, j + 2), (i0, i1, i2)):
            ids[axis % AXES] = slice(None) if i is None else i
        r0, r1 = self.parts[j]
        return self.buf.at[ids[2], ids[1], ids[0], r0:r1, :]

    def p(self, j, level, d):
        return self.env.p((j + level) % AXES, d)

    def send(self, j, group, k, ref, level, d, src=None):
        self.env.remote(ref if src is None else src, ref, self.ssem.at[group], self.rsem.at[k],
                        self.env.peer((j + level) % AXES, d))

    def some(self, blocks):
        for level in range(AXES):
            width = LINE ** level
            if blocks <= width * (LINE - 1):
                lead = (0,) * (AXES - 1 - level)
                return self.buf.at[lead + (pl.ds(0, blocks // width),)]

    def recv(self, k, blocks):
        self.env.arrived(self.some(blocks), self.rsem.at[k])

    def all_sent(self):
        for group, blocks in enumerate((3, 8, 4, 32, 16)):
            self.env.sent(self.some(blocks), self.ssem.at[group])

    def s1_send(self, src=None):
        for d in DISTS:
            for j, (r0, r1) in enumerate(self.parts):
                ref = self.at(j, self.p(j, 0, 0), self.p(j, 1, 0), self.p(j, 2, 0))
                self.send(j, 0, d - 1, ref, 0, d, None if src is None else src.at[r0:r1, :])

    def s1_recv(self):
        for d in (1, 3, 2):
            self.recv(d - 1, 1)

    def chunk(self, j, level, k, m):
        if level == 1:
            return self.at(j, self.p(j, 0, k), self.p(j, 1, m), self.p(j, 2, 0))
        return self.at(j, None, self.p(j, 1, k), self.p(j, 2, m))

    def a_send(self, level, k):
        for j in range(AXES):
            ref = self.chunk(j, level, k, 0)
            for d in (1, 3):
                self.send(j, 2 * level - 1, 8 * level - 5 + k, ref, level, d)

    def a_recv(self, level, k):
        self.recv(8 * level - 5 + k, 2 * LINE ** (level - 1))

    def b_send(self, level, k):
        d = 1 if k < 2 else 3
        for j in range(AXES):
            self.send(j, 2 * level, 8 * level - 1 + k, self.chunk(j, level, k, LINE - d), level, d)

    def b_recv(self, level, k):
        self.recv(8 * level - 1 + k, LINE ** (level - 1))

    def t_send(self, k, m):
        ts, tr = self.twin
        for j in range(AXES):
            ref = self.chunk(j, 2, k, m)
            self.env.remote(ref, ref, ts.at[0], tr.at[0], self.env.partner)

    def t_recv(self):
        self.env.arrived(self.buf, self.twin[1].at[0])

    def run(self, ops):
        for op in re.findall('[a-zA-Z][0-9]*', ops):
            args = [int(c) for c in op[1:]]
            {'S': self.s1_send, 's': self.s1_recv, 'A': self.a_send, 'a': self.a_recv,
             'B': self.b_send, 'b': self.b_recv, 'T': self.t_send, 'U': self.t_recv}[op[0]](*args)


def write_kernel(mine, code1, code2, gfull, gp, o1, o2, g1, g2, og, sem):
    pairs = [(code1, o1), (code2, o2), (gp, og)]
    for view, out in enumerate((g1, g2)):
        pairs.append((gfull.at[:, view * mine:(view + 1) * mine, :], out))
    copies = [pltpu.make_async_copy(src, dst, sem.at[i]) for i, (src, dst) in enumerate(pairs)]
    for cp in copies:
        cp.start()
    for cp in copies:
        cp.wait()


def step_kernel(total_rows, total_protos, z1h, z2h, ch,
                code1, code2, loss_out, gfull, gp_out,
                z1, z2, y1, y2, c_ref, f_scr, e_scr, cfull, lrow, frow, vall, zr, dall,
                cacc, vb, ub, stage, csend, crecv, first, later, lossb, losst, dacc, drecv, dz, cst,
                lsem, c_ssem, c_rsem, s_ssem, s_rsem, a_ssem, a_rsem, t_ssem, t_rsem,
                v_ssem, v_rsem, g_ssem, g_rsem, l_ssem, l_rsem, x_ssem, x_rsem, o_sem):
    env = _Env()
    me, core, pos, partner = env.me, env.core, env.pos, env.partner
    remote = env.remote
    rows, cols = z1.shape[0], c_ref.shape[0]
    mine = zr.shape[0] // 2
    blocks = LINE ** AXES
    fscale = 1.0 / (2 * total_rows * TEMP_TAU)
    zs, ys = (z1, z2), (y1, y2)
    chunks = rows // cols

    barrier = pltpu.get_barrier_semaphore()
    pl.semaphore_signal(barrier, inc=1, device_id=partner, device_id_type=MESH)
    for axis in range(AXES):
        for d in DISTS:
            pl.semaphore_signal(barrier, inc=1, device_id=env.peer(axis, d), device_id_type=MESH)
    loads = [pltpu.make_async_copy(src, dst, lsem.at[i]) for i, (src, dst) in enumerate(
        ((ch, c_ref), (z1h, z1), (z2h, z2), (ch, cfull.at[pos[2], pos[1], pos[0]])))]
    gc = _Gather(env, cfull, C_CUTS, a_ssem, a_rsem, (t_ssem, t_rsem))
    gg = _Gather(env, gfull, G_CUTS, g_ssem, g_rsem)
    for cp in loads[:3]:
        cp.start()

    def scores(view):
        cacc[view] = jnp.zeros((cols, LANES), F32)

        def body(i, _):
            n0 = pl.multiple_of(i * cols, cols)
            s = _nt(c_ref[...], zs[view][pl.ds(n0, cols), :])
            f = jnp.exp(s * (1.0 / TEMP_TAU))
            stage[0, 2 + view:3 + view, pl.ds(n0, cols)] = jnp.sum(f, axis=0, keepdims=True)
            e = f * f
            f_scr[view, :, pl.ds(n0, cols)] = f
            e_scr[view, :, pl.ds(n0, cols)] = e
            cacc[view] += e[:, :LANES] + e[:, LANES:]
            return 0
        lax.fori_loop(0, chunks, body, 0, unroll=2)
        zr[view * mine:(view + 1) * mine, :] = zs[view][pl.ds(pl.multiple_of(me * mine, mine), mine), :]

    def other_scores(view):
        def body(i, _):
            n0 = pl.multiple_of(i * cols, cols)
            f = jnp.exp(_nt(c_ref[...], ys[view][pl.ds(n0, cols), :]) * (1.0 / TEMP_TAU))
            e_scr[view, :, pl.ds(rows + n0, cols)] = f * f
            return 0
        lax.fori_loop(0, chunks, body, 0, unroll=2)

    def row_scores(lo, hi):
        def body(q, _):
            z_, y_, x_ = block(q)
            l = _nt(zr[...], cfull[z_, y_, x_]) * (1.0 / TEMP_TAU)
            lrow[q] = l
            frow[q] = jnp.exp(l)
            return 0
        lax.fori_loop(lo, hi, body, 0, unroll=2)

    def block(q):
        return lax.div(q, LINE * LINE), lax.rem(lax.div(q, LINE), LINE), lax.rem(q, LINE)

    def column_sums(it):
        for view in range(2):
            for h in range(2):
                k = 2 * view + h
                s = jnp.sum(cacc[view, h * LANES:(h + 1) * LANES, :], axis=1, keepdims=True)
                csend[it, k:k + 1, :] = _col_to_row(s)

    def spread(vrow):
        for view in range(2):
            for h in range(2):
                k = 2 * view + h
                vb[view, h * LANES:(h + 1) * LANES, :] = jnp.broadcast_to(
                    _row_to_col(vrow[k:k + 1, :]), (LANES, LANES))

    def exchange():
        cp = remote(csend.at[0], crecv.at[0], c_ssem.at[0], c_rsem.at[0], partner)
        cp.wait()
        return csend[0] + crecv[0]

    def row_sums(it, width):
        wide = 8
        step = wide * LANES
        for view in range(2):
            def body(j, _, view=view):
                acc = [jnp.zeros((8, LANES), F32) for _ in range(wide)]
                offs = [pl.multiple_of(j * step + t * LANES, LANES) for t in range(wide)]
                for g in range(0, cols, 8):
                    w = vb[view, g:g + 8, :]
                    for t, l0 in enumerate(offs):
                        acc[t] = acc[t] + e_scr[view, g:g + 8, pl.ds(l0, LANES)] * w
                for t, l0 in enumerate(offs):
                    stage[it, view:view + 1, pl.ds(l0, LANES)] = jnp.sum(acc[t], axis=0, keepdims=True)
                return 0
            lax.fori_loop(0, width // step, body, 0)

    def weighted_columns():
        for view in range(2):
            def body(g, _, view=view):
                for gi in range(2):
                    k0 = pl.multiple_of(g * 16 + gi * 8, 8)
                    acc = [None] * 4
                    for t in range(2 * rows // LANES):
                        ls = slice(t * LANES, (t + 1) * LANES)
                        x = e_scr[view, pl.ds(k0, 8), ls] * ub[view, :, ls]
                        acc[t % 4] = x if acc[t % 4] is None else acc[t % 4] + x
                    cacc[view, pl.ds(k0, 8), :] = (acc[0] + acc[1]) + (acc[2] + acc[3])
                return 0
            lax.fori_loop(0, cols // 16, body, 0)

    def vsend(st):
        ref = vall.at[(pos[2], pos[1], pos[0])[:AXES - st]]
        for d in DISTS:
            remote(ref, ref, v_ssem.at[st], v_rsem.at[st], env.peer(st, d))

    def v_some(st):
        return vall.at[(0,) * (AXES - 1 - st) + (pl.ds(0, LINE - 1),)]

    def vrecv(st):
        env.arrived(v_some(st), v_rsem.at[st])

    def hidden(slot):
        if slot in (0, 1):
            env.arrived(ys[slot], x_rsem.at[slot])
            other_scores(slot)
        elif slot == 6:
            gc.t_recv()
            row_scores(0, 20)
        elif slot == 7:
            row_scores(20, 42)
        elif slot == 8:
            row_scores(42, blocks)

    @pl.when(core == 1)
    def _():
        loads[0].wait()
        for view in range(2):
            loads[1 + view].wait()
            scores(view)
        pl.semaphore_wait(barrier, 1 + AXES * (LINE - 1))
        column_sums(0)
        total = exchange()
        for it in range(ITERS):
            last = it == ITERS - 1
            vrow = 1.0 / (float(total_protos) * total)
            if last:
                vall[pos[2], pos[1], pos[0]] = vrow
                vsend(0)
            spread(vrow)
            row_sums(it, rows if it == 0 else 2 * rows)
            buf = first if it == 0 else later.at[it - 1]
            if it == 0:
                env.arrived(stage.at[0, :, rows:], x_rsem.at[2])
            for j, (l0, l1) in enumerate(_parts(SUM_CUTS)):
                buf[0, pos[j], :, l0:l1] = stage[it, :buf.shape[2], l0:l1]
            for st in range(AXES):
                i = it * AXES + st
                for d in DISTS:
                    for j, (l0, l1) in enumerate(_parts(SUM_CUTS)):
                        ax = (st + j) % AXES
                        src = buf.at[st, pos[ax], :, l0:l1]
                        remote(src, src, s_ssem.at[i], s_rsem.at[i], env.peer(ax, d))
                hidden(i)
                if last:
                    vrecv(st)
                    if st < AXES - 1:
                        vsend(st + 1)
                env.arrived(buf.at[st, :LINE - 1], s_rsem.at[i])
                for j, (l0, l1) in enumerate(_parts(SUM_CUTS)):
                    tot = (buf[st, 0, :, l0:l1] + buf[st, 1, :, l0:l1]) + (buf[st, 2, :, l0:l1] + buf[st, 3, :, l0:l1])
                    if st < AXES - 1:
                        buf[st + 1, pos[(st + 1 + j) % AXES], :, l0:l1] = tot
                        continue
                    if it == 0:
                        dall[2:4, l0:l1] = tot[2:4]
                    if last:
                        dall[0:2, l0:l1] = tot
                    else:
                        u = 1.0 / (float(total_rows) * tot)
                        for view in range(2):
                            ub[view, :, l0:l1] = jnp.broadcast_to(u[view:view + 1], (8, l1 - l0))
            if not last:
                weighted_columns()
                column_sums(it + 1)
                total = csend[it + 1]
        remote(dall.at[:, rows:], dall.at[:, :rows], x_ssem.at[3], x_rsem.at[3], partner)
        remote(vall, vall, x_ssem.at[4], x_rsem.at[4], partner)

    @pl.when(core == 0)
    def _():
        loads[3].start()
        loads[0].wait()
        loads[3].wait()
        pl.semaphore_wait(barrier, 1 + AXES * (LINE - 1))
        gc.run('S')
        loads[1].wait()
        remote(z1, y1, x_ssem.at[0], x_rsem.at[0], partner)
        scores(0)
        loads[2].wait()
        scores(1)
        column_sums(0)
        vrow = 1.0 / (float(total_protos) * exchange())
        spread(vrow)
        row_sums(0, rows)
        remote(stage.at[0, :, :rows], stage.at[0, :, rows:], x_ssem.at[2], x_rsem.at[2], partner)
        remote(z2, y2, x_ssem.at[1], x_rsem.at[1], partner)
        gc.run('A10sA11A12A13A20T00')
        gc.run('a10B10a11B11a12B12a13B13A21A23T10T30')
        gc.run('a20B20T01T03b10b11b12b13A22T20')
        gc.run('a21B21T11T13a23B23T31T33')
        gc.run('b20T02b21T12b23T32')
        gc.run('a22B22T21T23b22T22')
        row_scores(0, blocks)
        env.arrived(dall.at[:, :rows], x_rsem.at[3])
        env.arrived(vall, x_rsem.at[4])
        gc.all_sent()
        for i, ref in enumerate((z1, z2, stage.at[0, :, :rows])):
            env.sent(ref, x_ssem.at[i])
        env.sent(cfull, t_ssem.at[0])
        env.drain()

    tile = pl.multiple_of(lax.div(me * mine, LANES) * LANES, LANES)
    shift = lax.rem(me * mine, LANES)
    dv = dall[:, pl.ds(tile, LANES)]
    col = [_row_to_col(dv[i:i + 1, :], mine, shift) for i in range(4)]
    rc = jnp.broadcast_to(1.0 / jnp.concatenate(col[0:2], axis=0), (2 * mine, LANES))
    den = jnp.concatenate(col[2:4], axis=0)
    dc = jnp.broadcast_to(1.0 / den, (2 * mine, LANES))
    ld = jnp.broadcast_to(jnp.log(den), (2 * mine, LANES))

    def code_rows(q, h):
        z_, y_, x_ = block(q)
        f = frow[q, :, h * LANES:(h + 1) * LANES]
        v0 = jnp.broadcast_to(vall[z_, y_, x_, h:h + 1, :], (mine, LANES))
        v1 = jnp.broadcast_to(vall[z_, y_, x_, 2 + h:3 + h, :], (mine, LANES))
        return f, f * f * (rc * jnp.concatenate([v0, v1], axis=0))

    def dzbody(i, acc):
        hs = []
        for x_ in range(LINE):
            for h in range(2):
                f, code = code_rows(i * LINE + x_, h)
                other = jnp.concatenate([code[mine:], code[:mine]], axis=0)
                hs.append(((f * dc - other) * fscale).astype(BF16))
        cl = cfull[lax.div(i, LINE), lax.rem(i, LINE)].reshape(LINE * cols, cols)
        return acc + _nn(jnp.concatenate(hs, axis=1), cl)

    dz[...] = lax.fori_loop(0, LINE * LINE, dzbody, jnp.zeros((2 * mine, cols), F32), unroll=2)

    own = pltpu.make_async_copy(dz, gfull.at[pos[2], pos[1], pos[0]], o_sem.at[0])
    own.start()
    gg.s1_send(dz)
    own.wait()
    gg.run('A10')
    spread(vall[pos[2], pos[1], pos[0]])
    dacc[...] = jnp.zeros((cols, cols), F32)

    def out_copy(view, i):
        n0 = pl.multiple_of(i * cols, cols)
        return pltpu.make_async_copy(cst.at[view, pl.ds(n0, cols), :], (code1, code2)[view].at[pl.ds(n0, cols), :],
                                     o_sem.at[2 + view])

    def columns(i):
        def body(i, _):
            n0 = pl.multiple_of(i * cols, cols)
            inv = 1.0 / dall[:, pl.ds(n0, cols)]
            code, prob = [], []
            for view in range(2):
                w = jnp.concatenate([vb[view], vb[view]], axis=1)
                code.append(e_scr[view, :, pl.ds(n0, cols)] * w * inv[view:view + 1, :])
                prob.append(f_scr[view, :, pl.ds(n0, cols)] * inv[2 + view:3 + view, :])
            for view in range(2):
                h = ((prob[view] - code[1 - view]) * fscale).astype(BF16)
                dacc[...] += _nn(h, zs[view][pl.ds(n0, cols), :])
                cst[view, pl.ds(n0, cols), :] = code[view].T
                out_copy(view, i).start()
            return 0
        lax.fori_loop(i * 2, i * 2 + 2, body, 0)

    def lbody(q, acc):
        for h in range(2):
            f, code = code_rows(q, h)
            lp = lrow[q, :, h * LANES:(h + 1) * LANES] - ld
            other = jnp.concatenate([code[mine:], code[:mine]], axis=0)
            acc = acc + other * lp
        return acc
    part = lax.fori_loop(0, blocks, lbody, jnp.zeros((2 * mine, LANES), F32), unroll=2)
    lossb[0, pos[0]] = jnp.sum(part.reshape(2 * mine // 8, 8, LANES), axis=0)

    def loss_send(st):
        ref = lossb.at[st, pos[st]]
        for d in DISTS:
            remote(ref, ref, l_ssem.at[st], l_rsem.at[st], env.peer(st, d))
        env.sent(lossb.at[st, :LINE - 1], l_ssem.at[st])

    def loss_recv(st):
        env.arrived(lossb.at[st, :LINE - 1], l_rsem.at[st])
        return (lossb[st, 0] + lossb[st, 1]) + (lossb[st, 2] + lossb[st, 3])

    gg.run('sA11A12A13')
    loss_send(0)
    gg.run('A20')
    columns(0)
    gg.run('a10B10a11B11a12B12a13B13A21A23')
    lossb[1, pos[1]] = loss_recv(0)
    loss_send(1)
    columns(1)
    gg.run('b10b11b12b13A22a20B20')
    lossb[2, pos[2]] = loss_recv(1)
    loss_send(2)
    columns(2)
    gg.run('a21B21a23B23')
    columns(3)
    losst[0] = loss_recv(2)
    lcp = remote(losst.at[0], losst.at[1], l_ssem.at[3], l_rsem.at[3], partner)
    dcp = remote(dacc, drecv, l_ssem.at[4], l_rsem.at[4], partner)
    gg.run('a22B22')
    lcp.wait_recv()
    loss_out[...] = jnp.sum(losst[0] + losst[1], keepdims=True) * (-1.0 / (2 * total_rows))
    dcp.wait_recv()
    drecv[...] = dacc[...] + drecv[...]
    gpc = pltpu.make_async_copy(drecv, gp_out, o_sem.at[1])
    gpc.start()
    gg.run('b20b21b23b22')
    gpc.wait()
    for view, out in enumerate((code1, code2)):
        pltpu.make_async_copy(cst.at[view], out, o_sem.at[2 + view]).wait()
    gg.all_sent()
    env.sent(losst.at[0], l_ssem.at[3])
    env.sent(dacc, l_ssem.at[4])
    env.drain()

    @pl.when(core == 1)
    def _():
        for it in range(ITERS):
            for st in range(AXES):
                buf = first if it == 0 else later.at[it - 1]
                env.sent(buf.at[st, :LINE - 1], s_ssem.at[it * AXES + st])
        for st in range(AXES):
            env.sent(v_some(st), v_ssem.at[st])
        env.sent(dall.at[:, rows:], x_ssem.at[3])
        env.sent(vall, x_ssem.at[4])
        env.drain()


def solution(mesh):
    proto_size = mesh.shape['proto']
    data_size = mesh.shape['data']

    def local_step(emb_one, emb_two, protos):
        rows, dim = emb_one.shape
        cols = protos.shape[0]
        total_rows = rows * data_size
        total_protos = cols * proto_size
        mine = rows // proto_size
        vm = pl.BlockSpec(memory_space=pltpu.VMEM)
        hbm = pl.BlockSpec(memory_space=pltpu.HBM)
        free = pl.BlockSpec(memory_space=pl.ANY)
        nsem = ITERS * AXES
        dma = lambda n: pltpu.SemaphoreType.DMA((n,))
        grid3 = (LINE,) * AXES
        sds = jax.ShapeDtypeStruct
        code = sds((rows, cols), F32)
        zbuf = pltpu.VMEM((rows, dim), BF16)
        square = pltpu.VMEM((cols, dim), F32)
        rowbuf = pltpu.VMEM((proto_size, 2 * mine, cols), F32)
        small = pltpu.VMEM((ITERS, 4, LANES), F32)
        spread = pltpu.VMEM((2, cols, LANES), F32)
        args = [pltpu.with_memory_space_constraint(a, pltpu.HBM) for a in (emb_one, emb_two, protos)]
        code1, code2, loss, gall, gp = pl.pallas_call(
            functools.partial(step_kernel, total_rows, total_protos),
            out_shape=(code, code, sds((1, 1), F32),
                       sds(grid3 + (2 * mine, dim), F32), sds((cols, dim), F32)),
            in_specs=[hbm] * 3,
            out_specs=(free, free, vm, free, free),
            scratch_shapes=[
                zbuf, zbuf, zbuf, zbuf, pltpu.VMEM((cols, dim), BF16),
                pltpu.VMEM((2, cols, rows), F32),
                pltpu.VMEM((2, cols, 2 * rows), F32),
                pltpu.VMEM(grid3 + (cols, dim), BF16),
                rowbuf, rowbuf,
                pltpu.VMEM(grid3 + (4, LANES), F32),
                pltpu.VMEM((2 * mine, dim), BF16),
                pltpu.VMEM((4, total_rows), F32),
                spread, spread,
                pltpu.VMEM((2, 8, total_rows), F32),
                pltpu.VMEM((ITERS, 4, total_rows), F32),
                small, small,
                pltpu.VMEM((AXES, LINE, 4, total_rows), F32),
                pltpu.VMEM((ITERS - 1, AXES, LINE, 2, total_rows), F32),
                pltpu.VMEM((AXES, LINE, 8, LANES), F32),
                pltpu.VMEM((2, 8, LANES), F32),
                square, square,
                pltpu.VMEM((2 * mine, dim), F32),
                pltpu.VMEM((2, rows, cols), F32),
                dma(4), dma(1), dma(1), dma(nsem), dma(nsem),
                dma(5), dma(AG_SEMS), dma(1), dma(1),
                dma(AXES), dma(AXES), dma(5), dma(AG_SEMS), dma(5), dma(5),
                dma(5), dma(5), dma(4),
            ],
            compiler_params=pltpu.CompilerParams(collective_id=0, has_side_effects=True,
                                                 vmem_limit_bytes=44 * 2 ** 20),
        )(*args)
        blocked = sds((proto_size, mine, dim), F32)
        o1, o2, g1, g2, og = pl.pallas_call(
            functools.partial(write_kernel, mine),
            out_shape=(code, code, blocked, blocked, sds((cols, dim), F32)),
            in_specs=[vm] * 4,
            out_specs=(hbm,) * 5,
            scratch_shapes=[dma(5)],
            compiler_params=pltpu.CompilerParams(vmem_limit_bytes=2 ** 20),
        )(code1, code2, gall.reshape(proto_size, 2 * mine, dim), gp)
        return o1, o2, loss[0, 0], g1.reshape(rows, dim), g2.reshape(rows, dim), og

    return jax.shard_map(
        local_step, mesh=mesh,
        in_specs=(P('data', None), P('data', None), P('proto', None)),
        out_specs=(P('data', 'proto'), P('data', 'proto'), P(), P('data', None), P('data', None), P('proto', None)),
        check_vma=False)
```

```python
import functools
import re

import jax
import jax.numpy as jnp
from jax import lax
from jax.experimental import pallas as pl
from jax.experimental.pallas import tpu as pltpu
from jax.sharding import PartitionSpec as P

EPSILON = 0.05
TEMP_TAU = 0.1
ITERS = 3
LINE = 4
AXES = 3
MESH = pl.DeviceIdType.MESH
F32 = jnp.float32
BF16 = jnp.bfloat16
LANES = 128
SUM_CUTS = (0, 1408, 2816, 4096)
C_CUTS = (0, 80, 160, 256)
G_CUTS = (0, 24, 48, 64)
AG_SEMS = 19
DISTS = (2, 1, 3)


def _nt(a, b):
    return lax.dot_general(a, b, (((1,), (1,)), ((), ())), preferred_element_type=F32)


def _nn(a, b):
    return jnp.dot(a, b, preferred_element_type=F32)


def _col_to_row(s):
    r = lax.broadcasted_iota(jnp.int32, (LANES, LANES), 0)
    c = lax.broadcasted_iota(jnp.int32, (LANES, LANES), 1)
    return jnp.sum(jnp.where(r == c, s, 0.0), axis=0, keepdims=True)


def _row_to_col(row, n=LANES, shift=0):
    r = lax.broadcasted_iota(jnp.int32, (n, LANES), 0)
    c = lax.broadcasted_iota(jnp.int32, (n, LANES), 1)
    return jnp.sum(jnp.where(c == r + shift, row, 0.0), axis=1, keepdims=True)


def _parts(cuts):
    return tuple(zip(cuts[:-1], cuts[1:]))


class _Env:
    def __init__(self):
        self.me = lax.axis_index('proto')
        self.core = lax.axis_index('data')
        me = self.me
        self.pos = [lax.rem(me, LINE), lax.rem(lax.div(me, LINE), LINE), lax.div(me, LINE * LINE)]
        self.stride = [1, LINE, LINE * LINE]
        self.pending = []
        self.partner = (me, 1 - self.core)

    def p(self, axis, d):
        return self.pos[axis] if d == 0 else lax.rem(self.pos[axis] + d, LINE)

    def peer(self, axis, d):
        return (self.me + (self.p(axis, d) - self.pos[axis]) * self.stride[axis], self.core)

    def remote(self, src, dst, ss, rs, dev):
        cp = pltpu.make_async_remote_copy(src, dst, ss, rs, device_id=dev, device_id_type=MESH)
        cp.start()
        return cp

    def sent(self, ref, ss):
        self.pending.append(pltpu.make_async_remote_copy(ref, ref, ss, ss, device_id=self.partner,
                                                         device_id_type=MESH))

    def arrived(self, ref, rs):
        pltpu.make_async_remote_copy(ref, ref, rs, rs, device_id=self.partner, device_id_type=MESH).wait_recv()

    def drain(self):
        for cp in self.pending:
            cp.wait_send()
        self.pending.clear()


class _Gather:
    def __init__(self, env, buf, cuts, ssem, rsem, twin=None):
        self.env, self.buf, self.parts = env, buf, _parts(cuts)
        self.ssem, self.rsem, self.twin = ssem, rsem, twin

    def at(self, j, i0, i1, i2):
        ids = [None] * AXES
        for axis, i in zip((j, j + 1, j + 2), (i0, i1, i2)):
            ids[axis % AXES] = slice(None) if i is None else i
        r0, r1 = self.parts[j]
        return self.buf.at[ids[2], ids[1], ids[0], r0:r1, :]

    def p(self, j, level, d):
        return self.env.p((j + level) % AXES, d)

    def send(self, j, group, k, ref, level, d, src=None):
        self.env.remote(ref if src is None else src, ref, self.ssem.at[group], self.rsem.at[k],
                        self.env.peer((j + level) % AXES, d))

    def some(self, blocks):
        for level in range(AXES):
            width = LINE ** level
            if blocks <= width * (LINE - 1):
                lead = (0,) * (AXES - 1 - level)
                return self.buf.at[lead + (pl.ds(0, blocks // width),)]

    def recv(self, k, blocks):
        self.env.arrived(self.some(blocks), self.rsem.at[k])

    def all_sent(self):
        for group, blocks in enumerate((3, 8, 4, 32, 16)):
            self.env.sent(self.some(blocks), self.ssem.at[group])

    def s1_send(self, src=None):
        for d in DISTS:
            for j, (r0, r1) in enumerate(self.parts):
                ref = self.at(j, self.p(j, 0, 0), self.p(j, 1, 0), self.p(j, 2, 0))
                self.send(j, 0, d - 1, ref, 0, d, None if src is None else src.at[r0:r1, :])

    def s1_recv(self):
        for d in (1, 3, 2):
            self.recv(d - 1, 1)

    def chunk(self, j, level, k, m):
        if level == 1:
            return self.at(j, self.p(j, 0, k), self.p(j, 1, m), self.p(j, 2, 0))
        return self.at(j, None, self.p(j, 1, k), self.p(j, 2, m))

    def a_send(self, level, k):
        for j in range(AXES):
            ref = self.chunk(j, level, k, 0)
            for d in (1, 3):
                self.send(j, 2 * level - 1, 8 * level - 5 + k, ref, level, d)

    def piece_send(self, *offsets):
        for k in offsets:
            for j in range(AXES):
                ref = self.chunk(j, 1, k, 0)
                for d in (1, 3):
                    self.send(j, 3, 11, ref, 2, d)

    def own_piece(self):
        self.piece_send(0)

    def other_pieces(self):
        self.piece_send(1, 3, 2)

    def a_recv(self, level, k):
        self.recv(8 * level - 5 + k, 2 * LINE ** (level - 1))

    def b_send(self, level, k):
        d = 1 if k < 2 else 3
        for j in range(AXES):
            self.send(j, 2 * level, 8 * level - 1 + k, self.chunk(j, level, k, LINE - d), level, d)

    def b_recv(self, level, k):
        self.recv(8 * level - 1 + k, LINE ** (level - 1))

    def t_send(self, k, m):
        ts, tr = self.twin
        for j in range(AXES):
            ref = self.chunk(j, 2, k, m)
            self.env.remote(ref, ref, ts.at[0], tr.at[0], self.env.partner)

    def t_recv(self):
        self.env.arrived(self.buf, self.twin[1].at[0])

    def run(self, ops):
        for op in re.findall('[a-zA-Z][0-9]*', ops):
            args = [int(c) for c in op[1:]]
            {'S': self.s1_send, 's': self.s1_recv, 'A': self.a_send, 'a': self.a_recv,
             'B': self.b_send, 'b': self.b_recv, 'T': self.t_send, 'P': self.own_piece, 'Q': self.other_pieces}[op[0]](*args)


def write_kernel(mine, code1, code2, gfull, gp, o1, o2, g1, g2, og, sem):
    pairs = [(code1, o1), (code2, o2), (gp, og)]
    for view, out in enumerate((g1, g2)):
        pairs.append((gfull.at[:, view * mine:(view + 1) * mine, :], out))
    copies = [pltpu.make_async_copy(src, dst, sem.at[i]) for i, (src, dst) in enumerate(pairs)]
    for cp in copies:
        cp.start()
    for cp in copies:
        cp.wait()


def step_kernel(total_rows, total_protos, z1h, z2h, ch,
                code1, code2, loss_out, gfull, gp_out,
                z1, z2, y1, y2, c_ref, f_scr, e_scr, cfull, lrow, frow, vall, zr, dall,
                cacc, vb, ub, stage, csend, crecv, first, later, lossb, losst, dacc, drecv, dz, cst,
                lsem, c_ssem, c_rsem, s_ssem, s_rsem, a_ssem, a_rsem, t_ssem, t_rsem,
                v_ssem, v_rsem, g_ssem, g_rsem, l_ssem, l_rsem, x_ssem, x_rsem, o_sem):
    env = _Env()
    me, core, pos, partner = env.me, env.core, env.pos, env.partner
    remote = env.remote
    rows, cols = z1.shape[0], c_ref.shape[0]
    mine = zr.shape[0] // 2
    blocks = LINE ** AXES
    fscale = 1.0 / (2 * total_rows * TEMP_TAU)
    zs, ys = (z1, z2), (y1, y2)
    chunks, groups = rows // cols, cols // 8

    barrier = pltpu.get_barrier_semaphore()
    pl.semaphore_signal(barrier, inc=1, device_id=partner, device_id_type=MESH)
    for axis in range(AXES):
        for d in DISTS:
            pl.semaphore_signal(barrier, inc=1, device_id=env.peer(axis, d), device_id_type=MESH)
    loads = [pltpu.make_async_copy(src, dst, lsem.at[i]) for i, (src, dst) in enumerate(
        ((ch, c_ref), (z1h, z1), (z2h, z2), (ch, cfull.at[pos[2], pos[1], pos[0]])))]
    gc = _Gather(env, cfull, C_CUTS, a_ssem, a_rsem, (t_ssem, t_rsem))
    gg = _Gather(env, gfull, G_CUTS, g_ssem, g_rsem)
    for cp in loads[:3]:
        cp.start()

    def scores(view):
        cacc[view] = jnp.zeros((cols, LANES), F32)

        def body(i, _):
            n0 = pl.multiple_of(i * cols, cols)
            s = _nt(c_ref[...], zs[view][pl.ds(n0, cols), :])
            f = jnp.exp(s * (1.0 / TEMP_TAU))
            stage[0, 2 + view:3 + view, pl.ds(n0, cols)] = jnp.sum(f, axis=0, keepdims=True)
            e = f * f
            f_scr[view, :, pl.ds(n0, cols)] = f
            e_scr[view, :, :, pl.ds(n0, cols)] = e.reshape(groups, 8, cols)
            cacc[view] += e[:, :LANES] + e[:, LANES:]
            return 0
        lax.fori_loop(0, chunks, body, 0, unroll=4)
        zr[view * mine:(view + 1) * mine, :] = zs[view][pl.ds(pl.multiple_of(me * mine, mine), mine), :]

    def other_scores(view):
        def body(i, _):
            n0 = pl.multiple_of(i * cols, cols)
            f = jnp.exp(_nt(c_ref[...], ys[view][pl.ds(n0, cols), :]) * (1.0 / TEMP_TAU))
            e_scr[view, :, :, pl.ds(rows + n0, cols)] = (f * f).reshape(groups, 8, cols)
            return 0
        lax.fori_loop(0, chunks, body, 0, unroll=2)

    def row_scores(lo, hi):
        def body(q, _):
            z_, y_, x_ = block(q)
            l = _nt(zr[...], cfull[z_, y_, x_]) * (1.0 / TEMP_TAU)
            lrow[q] = l
            frow[q] = jnp.exp(l)
            return 0
        lax.fori_loop(lo, hi, body, 0, unroll=4)

    def block(q):
        return lax.div(q, LINE * LINE), lax.rem(lax.div(q, LINE), LINE), lax.rem(q, LINE)

    def column_sums(it):
        for view in range(2):
            for h in range(2):
                k = 2 * view + h
                s = jnp.sum(cacc[view, h * LANES:(h + 1) * LANES, :], axis=1, keepdims=True)
                csend[it, k:k + 1, :] = _col_to_row(s)

    def spread(vrow):
        for view in range(2):
            for h in range(2):
                k = 2 * view + h
                vb[view, h * LANES:(h + 1) * LANES, :] = jnp.broadcast_to(
                    _row_to_col(vrow[k:k + 1, :]), (LANES, LANES))

    def exchange():
        cp = remote(csend.at[0], crecv.at[0], c_ssem.at[0], c_rsem.at[0], partner)
        cp.wait()
        return csend[0] + crecv[0]

    def row_sums(it, width):
        tiles = [slice(l, l + LANES) for l in range(0, width, LANES)]
        for view in range(2):
            def body(g, acc, view=view):
                w = vb[view, pl.ds(pl.multiple_of(g * 8, 8), 8), :]
                return tuple(a + e_scr[view, g, :, ls] * w for a, ls in zip(acc, tiles))
            acc = lax.fori_loop(0, groups, body, tuple(jnp.zeros((8, LANES), F32) for _ in tiles), unroll=4)
            for a, ls in zip(acc, tiles):
                stage[it, view:view + 1, ls] = jnp.sum(a, axis=0, keepdims=True)

    def weighted_columns():
        tiles = [slice(l, l + LANES) for l in range(0, 2 * rows, LANES)]
        for view in range(2):
            us = [ub[view, :, ls] for ls in tiles]

            def body(g, _, view=view, us=us):
                acc = [None] * 4
                for t, ls in enumerate(tiles):
                    x = e_scr[view, g, :, ls] * us[t]
                    acc[t % 4] = x if acc[t % 4] is None else acc[t % 4] + x
                cacc[view, pl.ds(pl.multiple_of(g * 8, 8), 8), :] = (acc[0] + acc[1]) + (acc[2] + acc[3])
                return 0
            lax.fori_loop(0, groups, body, 0, unroll=4)

    def vsend(st):
        ref = vall.at[(pos[2], pos[1], pos[0])[:AXES - st]]
        for d in DISTS:
            remote(ref, ref, v_ssem.at[st], v_rsem.at[st], env.peer(st, d))

    def v_some(st):
        return vall.at[(0,) * (AXES - 1 - st) + (pl.ds(0, LINE - 1),)]

    def vrecv(st):
        env.arrived(v_some(st), v_rsem.at[st])

    def hidden(slot):
        if slot in (1, 2):
            env.arrived(ys[slot - 1], x_rsem.at[slot - 1])
            other_scores(slot - 1)
        elif slot == 6:
            gc.t_recv()
            row_scores(0, 20)
        elif slot == 7:
            row_scores(20, 44)
        elif slot == 8:
            row_scores(44, blocks)

    @pl.when(core == 1)
    def _():
        loads[0].wait()
        for view in range(2):
            loads[1 + view].wait()
            scores(view)
        pl.semaphore_wait(barrier, 1 + AXES * (LINE - 1))
        column_sums(0)
        total = exchange()
        for it in range(ITERS):
            last = it == ITERS - 1
            vrow = 1.0 / (float(total_protos) * total)
            if last:
                vall[pos[2], pos[1], pos[0]] = vrow
                vsend(0)
            spread(vrow)
            row_sums(it, rows if it == 0 else 2 * rows)
            buf = first if it == 0 else later.at[it - 1]
            if it == 0:
                env.arrived(stage.at[0, :, rows:], x_rsem.at[2])
            for j, (l0, l1) in enumerate(_parts(SUM_CUTS)):
                buf[0, pos[j], :, l0:l1] = stage[it, :buf.shape[2], l0:l1]
            for st in range(AXES):
                i = it * AXES + st
                for d in DISTS:
                    for j, (l0, l1) in enumerate(_parts(SUM_CUTS)):
                        ax = (st + j) % AXES
                        src = buf.at[st, pos[ax], :, l0:l1]
                        remote(src, src, s_ssem.at[i], s_rsem.at[i], env.peer(ax, d))
                hidden(i)
                if last:
                    vrecv(st)
                    if st < AXES - 1:
                        vsend(st + 1)
                env.arrived(buf.at[st, :LINE - 1], s_rsem.at[i])
                for j, (l0, l1) in enumerate(_parts(SUM_CUTS)):
                    tot = (buf[st, 0, :, l0:l1] + buf[st, 1, :, l0:l1]) + (buf[st, 2, :, l0:l1] + buf[st, 3, :, l0:l1])
                    if st < AXES - 1:
                        buf[st + 1, pos[(st + 1 + j) % AXES], :, l0:l1] = tot
                        continue
                    if it == 0:
                        dall[2:4, l0:l1] = tot[2:4]
                    if last:
                        dall[0:2, l0:l1] = tot
                    else:
                        u = 1.0 / (float(total_rows) * tot)
                        for view in range(2):
                            ub[view, :, l0:l1] = jnp.broadcast_to(u[view:view + 1], (8, l1 - l0))
            if not last:
                weighted_columns()
                column_sums(it + 1)
                total = csend[it + 1]
        remote(dall.at[:, rows:], dall.at[:, :rows], x_ssem.at[3], x_rsem.at[3], partner)
        remote(vall, vall, x_ssem.at[4], x_rsem.at[4], partner)

    @pl.when(core == 0)
    def _():
        loads[3].start()
        loads[0].wait()
        loads[1].wait()
        scores(0)
        loads[3].wait()
        pl.semaphore_wait(barrier, 1 + AXES * (LINE - 1))
        gc.run('SA10P')
        loads[2].wait()
        scores(1)
        column_sums(0)
        vrow = 1.0 / (float(total_protos) * exchange())
        spread(vrow)
        row_sums(0, rows)
        remote(stage.at[0, :, :rows], stage.at[0, :, rows:], x_ssem.at[2], x_rsem.at[2], partner)
        for i in range(2):
            remote(zs[i], ys[i], x_ssem.at[i], x_rsem.at[i], partner)
        gc.run('sA11A13A12QT00')
        gc.run('a10B10a11B11a13B13a12B12A21A23')
        gc.run('a20B20b10b11b13b12A22T10T30T20')
        gc.run('a21B21a23B23T01T03T11T13T31T33')
        gc.run('a22B22T21T23b20T02b21T12b23T32b22T22')
        row_scores(0, blocks)
        env.arrived(dall.at[:, :rows], x_rsem.at[3])
        env.arrived(vall, x_rsem.at[4])
        gc.all_sent()
        for i, ref in enumerate((z1, z2, stage.at[0, :, :rows])):
            env.sent(ref, x_ssem.at[i])
        env.sent(cfull, t_ssem.at[0])
        env.drain()

    tile = pl.multiple_of(lax.div(me * mine, LANES) * LANES, LANES)
    shift = lax.rem(me * mine, LANES)
    dv = dall[:, pl.ds(tile, LANES)]
    col = [_row_to_col(dv[i:i + 1, :], mine, shift) for i in range(4)]
    rc = jnp.broadcast_to(1.0 / jnp.concatenate(col[0:2], axis=0), (2 * mine, LANES))
    den = jnp.concatenate(col[2:4], axis=0)
    dc = jnp.broadcast_to(1.0 / den, (2 * mine, LANES))
    ld = jnp.broadcast_to(jnp.log(den), (2 * mine, LANES))

    def code_rows(q, h):
        z_, y_, x_ = block(q)
        f = frow[q, :, h * LANES:(h + 1) * LANES]
        v0 = jnp.broadcast_to(vall[z_, y_, x_, h:h + 1, :], (mine, LANES))
        v1 = jnp.broadcast_to(vall[z_, y_, x_, 2 + h:3 + h, :], (mine, LANES))
        return f, f * f * (rc * jnp.concatenate([v0, v1], axis=0))

    def dzbody(i, acc):
        hs = []
        for x_ in range(LINE):
            for h in range(2):
                f, code = code_rows(i * LINE + x_, h)
                other = jnp.concatenate([code[mine:], code[:mine]], axis=0)
                hs.append(((f * dc - other) * fscale).astype(BF16))
        cl = cfull[lax.div(i, LINE), lax.rem(i, LINE)].reshape(LINE * cols, cols)
        return acc + _nn(jnp.concatenate(hs, axis=1), cl)

    dz[...] = lax.fori_loop(0, LINE * LINE, dzbody, jnp.zeros((2 * mine, cols), F32), unroll=4)

    own = pltpu.make_async_copy(dz, gfull.at[pos[2], pos[1], pos[0]], o_sem.at[0])
    own.start()
    gg.s1_send(dz)
    own.wait()
    gg.run('A10P')
    spread(vall[pos[2], pos[1], pos[0]])
    dacc[...] = jnp.zeros((cols, cols), F32)

    def out_copy(view, i):
        n0 = pl.multiple_of(i * cols, cols)
        return pltpu.make_async_copy(cst.at[view, pl.ds(n0, cols), :], (code1, code2)[view].at[pl.ds(n0, cols), :],
                                     o_sem.at[2 + view])

    def columns(i):
        def body(i, _):
            n0 = pl.multiple_of(i * cols, cols)
            inv = 1.0 / dall[:, pl.ds(n0, cols)]
            code, prob = [], []
            for view in range(2):
                w = jnp.concatenate([vb[view], vb[view]], axis=1)
                code.append(e_scr[view, :, :, pl.ds(n0, cols)].reshape(cols, cols) * w * inv[view:view + 1, :])
                prob.append(f_scr[view, :, pl.ds(n0, cols)] * inv[2 + view:3 + view, :])
            for view in range(2):
                h = ((prob[view] - code[1 - view]) * fscale).astype(BF16)
                dacc[...] += _nn(h, zs[view][pl.ds(n0, cols), :])
                cst[view, pl.ds(n0, cols), :] = code[view].T
                out_copy(view, i).start()
            return 0
        lax.fori_loop(i * 2, i * 2 + 2, body, 0, unroll=True)

    def lbody(q, acc):
        for h in range(2):
            f, code = code_rows(q, h)
            lp = lrow[q, :, h * LANES:(h + 1) * LANES] - ld
            other = jnp.concatenate([code[mine:], code[:mine]], axis=0)
            acc = acc + other * lp
        return acc
    part = lax.fori_loop(0, blocks, lbody, jnp.zeros((2 * mine, LANES), F32), unroll=4)
    lossb[0, pos[0]] = jnp.sum(part.reshape(2 * mine // 8, 8, LANES), axis=0)

    def loss_send(st):
        ref = lossb.at[st, pos[st]]
        for d in DISTS:
            remote(ref, ref, l_ssem.at[st], l_rsem.at[st], env.peer(st, d))
        env.sent(lossb.at[st, :LINE - 1], l_ssem.at[st])

    def loss_recv(st):
        env.arrived(lossb.at[st, :LINE - 1], l_rsem.at[st])
        return (lossb[st, 0] + lossb[st, 1]) + (lossb[st, 2] + lossb[st, 3])

    gg.run('sA11A13A12Q')
    loss_send(0)
    columns(0)
    gg.run('a10B10a11B11a13B13a12B12A21A23')
    lossb[1, pos[1]] = loss_recv(0)
    loss_send(1)
    columns(1)
    gg.run('a20B20b10b11b13b12A22')
    lossb[2, pos[2]] = loss_recv(1)
    loss_send(2)
    columns(2)
    gg.run('a21B21a23B23')
    columns(3)
    losst[0] = loss_recv(2)
    lcp = remote(losst.at[0], losst.at[1], l_ssem.at[3], l_rsem.at[3], partner)
    dcp = remote(dacc, drecv, l_ssem.at[4], l_rsem.at[4], partner)
    gg.run('a22B22')
    lcp.wait_recv()
    loss_out[...] = jnp.sum(losst[0] + losst[1], keepdims=True) * (-1.0 / (2 * total_rows))
    dcp.wait_recv()
    drecv[...] = dacc[...] + drecv[...]
    gpc = pltpu.make_async_copy(drecv, gp_out, o_sem.at[1])
    gpc.start()
    gg.run('b20b21b23b22')
    gpc.wait()
    for view, out in enumerate((code1, code2)):
        pltpu.make_async_copy(cst.at[view], out, o_sem.at[2 + view]).wait()
    gg.all_sent()
    env.sent(losst.at[0], l_ssem.at[3])
    env.sent(dacc, l_ssem.at[4])
    env.drain()

    @pl.when(core == 1)
    def _():
        for it in range(ITERS):
            for st in range(AXES):
                buf = first if it == 0 else later.at[it - 1]
                env.sent(buf.at[st, :LINE - 1], s_ssem.at[it * AXES + st])
        for st in range(AXES):
            env.sent(v_some(st), v_ssem.at[st])
        env.sent(dall.at[:, rows:], x_ssem.at[3])
        env.sent(vall, x_ssem.at[4])
        env.drain()


def solution(mesh):
    proto_size = mesh.shape['proto']
    data_size = mesh.shape['data']

    def local_step(emb_one, emb_two, protos):
        rows, dim = emb_one.shape
        cols = protos.shape[0]
        total_rows = rows * data_size
        total_protos = cols * proto_size
        mine = rows // proto_size
        vm = pl.BlockSpec(memory_space=pltpu.VMEM)
        hbm = pl.BlockSpec(memory_space=pltpu.HBM)
        free = pl.BlockSpec(memory_space=pl.ANY)
        nsem = ITERS * AXES
        dma = lambda n: pltpu.SemaphoreType.DMA((n,))
        grid3 = (LINE,) * AXES
        sds = jax.ShapeDtypeStruct
        code = sds((rows, cols), F32)
        zbuf = pltpu.VMEM((rows, dim), BF16)
        square = pltpu.VMEM((cols, dim), F32)
        rowbuf = pltpu.VMEM((proto_size, 2 * mine, cols), F32)
        small = pltpu.VMEM((ITERS, 4, LANES), F32)
        spread = pltpu.VMEM((2, cols, LANES), F32)
        args = [pltpu.with_memory_space_constraint(a, pltpu.HBM) for a in (emb_one, emb_two, protos)]
        code1, code2, loss, gall, gp = pl.pallas_call(
            functools.partial(step_kernel, total_rows, total_protos),
            out_shape=(code, code, sds((1, 1), F32),
                       sds(grid3 + (2 * mine, dim), F32), sds((cols, dim), F32)),
            in_specs=[hbm] * 3,
            out_specs=(free, free, vm, free, free),
            scratch_shapes=[
                zbuf, zbuf, zbuf, zbuf, pltpu.VMEM((cols, dim), BF16),
                pltpu.VMEM((2, cols, rows), F32),
                pltpu.VMEM((2, cols // 8, 8, total_rows), F32),
                pltpu.VMEM(grid3 + (cols, dim), BF16),
                rowbuf, rowbuf,
                pltpu.VMEM(grid3 + (4, LANES), F32),
                pltpu.VMEM((2 * mine, dim), BF16),
                pltpu.VMEM((4, total_rows), F32),
                spread, spread,
                pltpu.VMEM((2, 8, total_rows), F32),
                pltpu.VMEM((ITERS, 4, total_rows), F32),
                small, small,
                pltpu.VMEM((AXES, LINE, 4, total_rows), F32),
                pltpu.VMEM((ITERS - 1, AXES, LINE, 2, total_rows), F32),
                pltpu.VMEM((AXES, LINE, 8, LANES), F32),
                pltpu.VMEM((2, 8, LANES), F32),
                square, square,
                pltpu.VMEM((2 * mine, dim), F32),
                pltpu.VMEM((2, rows, cols), F32),
                dma(4), dma(1), dma(1), dma(nsem), dma(nsem),
                dma(5), dma(AG_SEMS), dma(1), dma(1),
                dma(AXES), dma(AXES), dma(5), dma(AG_SEMS), dma(5), dma(5),
                dma(5), dma(5), dma(4),
            ],
            compiler_params=pltpu.CompilerParams(collective_id=0, has_side_effects=True,
                                                 vmem_limit_bytes=44 * 2 ** 20),
        )(*args)
        blocked = sds((proto_size, mine, dim), F32)
        o1, o2, g1, g2, og = pl.pallas_call(
            functools.partial(write_kernel, mine),
            out_shape=(code, code, blocked, blocked, sds((cols, dim), F32)),
            in_specs=[vm] * 4,
            out_specs=(hbm,) * 5,
            scratch_shapes=[dma(5)],
            compiler_params=pltpu.CompilerParams(vmem_limit_bytes=2 ** 20),
        )(code1, code2, gall.reshape(proto_size, 2 * mine, dim), gp)
        return o1, o2, loss[0, 0], g1.reshape(rows, dim), g2.reshape(rows, dim), og

    return jax.shard_map(
        local_step, mesh=mesh,
        in_specs=(P('data', None), P('data', None), P('proto', None)),
        out_specs=(P('data', 'proto'), P('data', 'proto'), P(), P('data', None), P('data', None), P('proto', None)),
        check_vma=False)
```

```python
import functools
import re

import jax
import jax.numpy as jnp
from jax import lax
from jax.experimental import pallas as pl
from jax.experimental.pallas import tpu as pltpu
from jax.sharding import PartitionSpec as P

EPSILON = 0.05
TEMP_TAU = 0.1
ITERS = 3
LINE = 4
AXES = 3
MESH = pl.DeviceIdType.MESH
F32 = jnp.float32
BF16 = jnp.bfloat16
LANES = 128
SUM_CUTS = (0, 1408, 2816, 4096)
C_CUTS = (0, 80, 160, 256)
G_CUTS = (0, 24, 48, 64)
AG_SEMS = 27
DISTS = (2, 1, 3)


def _nt(a, b):
    return lax.dot_general(a, b, (((1,), (1,)), ((), ())), preferred_element_type=F32)


def _nn(a, b):
    return jnp.dot(a, b, preferred_element_type=F32)


def _col_to_row(s):
    r = lax.broadcasted_iota(jnp.int32, (LANES, LANES), 0)
    c = lax.broadcasted_iota(jnp.int32, (LANES, LANES), 1)
    return jnp.sum(jnp.where(r == c, s, 0.0), axis=0, keepdims=True)


def _row_to_col(row, n=LANES, shift=0):
    r = lax.broadcasted_iota(jnp.int32, (n, LANES), 0)
    c = lax.broadcasted_iota(jnp.int32, (n, LANES), 1)
    return jnp.sum(jnp.where(c == r + shift, row, 0.0), axis=1, keepdims=True)


def _parts(cuts):
    return tuple(zip(cuts[:-1], cuts[1:]))


class _Env:
    def __init__(self):
        self.me = lax.axis_index('proto')
        self.core = lax.axis_index('data')
        me = self.me
        self.pos = [lax.rem(me, LINE), lax.rem(lax.div(me, LINE), LINE), lax.div(me, LINE * LINE)]
        self.stride = [1, LINE, LINE * LINE]
        self.pending = []
        self.partner = (me, 1 - self.core)

    def p(self, axis, d):
        return self.pos[axis] if d == 0 else lax.rem(self.pos[axis] + d, LINE)

    def peer(self, axis, d):
        return (self.me + (self.p(axis, d) - self.pos[axis]) * self.stride[axis], self.core)

    def remote(self, src, dst, ss, rs, dev):
        cp = pltpu.make_async_remote_copy(src, dst, ss, rs, device_id=dev, device_id_type=MESH)
        cp.start()
        return cp

    def sent(self, ref, ss):
        self.pending.append(pltpu.make_async_remote_copy(ref, ref, ss, ss, device_id=self.partner,
                                                         device_id_type=MESH))

    def arrived(self, ref, rs):
        pltpu.make_async_remote_copy(ref, ref, rs, rs, device_id=self.partner, device_id_type=MESH).wait_recv()

    def drain(self):
        for cp in self.pending:
            cp.wait_send()
        self.pending.clear()


class _Gather:
    def __init__(self, env, buf, cuts, ssem, rsem, twin=None):
        self.env, self.buf, self.parts = env, buf, _parts(cuts)
        self.ssem, self.rsem, self.twin = ssem, rsem, twin

    def at(self, j, i0, i1, i2):
        ids = [None] * AXES
        for axis, i in zip((j, j + 1, j + 2), (i0, i1, i2)):
            ids[axis % AXES] = slice(None) if i is None else i
        r0, r1 = self.parts[j]
        return self.buf.at[ids[2], ids[1], ids[0], r0:r1, :]

    def p(self, j, level, d):
        return self.env.p((j + level) % AXES, d)

    def send(self, j, group, k, ref, level, d, src=None):
        self.env.remote(ref if src is None else src, ref, self.ssem.at[group], self.rsem.at[k],
                        self.env.peer((j + level) % AXES, d))

    def some(self, blocks):
        for level in range(AXES):
            width = LINE ** level
            if blocks <= width * (LINE - 1):
                lead = (0,) * (AXES - 1 - level)
                return self.buf.at[lead + (pl.ds(0, blocks // width),)]

    def recv(self, k, blocks):
        self.env.arrived(self.some(blocks), self.rsem.at[k])

    def all_sent(self):
        for group, blocks in enumerate((3, 8, 4, 32, 16)):
            self.env.sent(self.some(blocks), self.ssem.at[group])

    def s1_send(self, src=None):
        for d in DISTS:
            for j, (r0, r1) in enumerate(self.parts):
                ref = self.at(j, self.p(j, 0, 0), self.p(j, 1, 0), self.p(j, 2, 0))
                self.send(j, 0, d - 1, ref, 0, d, None if src is None else src.at[r0:r1, :])

    def s1_recv(self):
        for d in (1, 3, 2):
            self.recv(d - 1, 1)

    def chunk(self, j, level, k, m):
        if level == 1:
            return self.at(j, self.p(j, 0, k), self.p(j, 1, m), self.p(j, 2, 0))
        return self.at(j, None, self.p(j, 1, k), self.p(j, 2, m))

    def slot(self, level, k, d):
        return 12 * level - 9 + k + LINE * (d // 2)

    def a_send(self, level, k):
        for j in range(AXES):
            ref = self.chunk(j, level, k, 0)
            for d in (1, 3):
                self.send(j, 2 * level - 1, self.slot(level, k, d), ref, level, d)

    def way(self, k):
        return 1 if k < 2 else 3

    def f_recv(self, level, k):
        self.recv(self.slot(level, k, self.way(k)), LINE ** (level - 1))

    def g_recv(self, level, k):
        self.recv(self.slot(level, k, LINE - self.way(k)), LINE ** (level - 1))

    def piece_send(self, *offsets):
        for k in offsets:
            for j in range(AXES):
                ref = self.chunk(j, 1, k, 0)
                for d in (1, 3):
                    self.send(j, 3, self.slot(2, 0, d), ref, 2, d)

    def own_piece(self):
        self.piece_send(0)

    def other_pieces(self):
        self.piece_send(1, 3, 2)

    def b_send(self, level, k):
        d = self.way(k)
        for j in range(AXES):
            self.send(j, 2 * level, self.slot(level, k, 5), self.chunk(j, level, k, LINE - d), level, d)

    def b_recv(self, level, k):
        self.recv(self.slot(level, k, 5), LINE ** (level - 1))

    def t_send(self, k, m):
        ts, tr = self.twin
        for j in range(AXES):
            ref = self.chunk(j, 2, k, m)
            self.env.remote(ref, ref, ts.at[0], tr.at[0], self.env.partner)

    def t_recv(self):
        self.env.arrived(self.buf, self.twin[1].at[0])

    def run(self, ops):
        for op in re.findall('[a-zA-Z][0-9]*', ops):
            args = [int(c) for c in op[1:]]
            {'S': self.s1_send, 's': self.s1_recv, 'A': self.a_send, 'f': self.f_recv, 'g': self.g_recv,
             'B': self.b_send, 'b': self.b_recv, 'T': self.t_send, 'P': self.own_piece, 'Q': self.other_pieces}[op[0]](*args)


def write_kernel(mine, code1, code2, gfull, gp, o1, o2, g1, g2, og, sem):
    pairs = [(code1, o1), (code2, o2), (gp, og)]
    for view, out in enumerate((g1, g2)):
        pairs.append((gfull.at[:, view * mine:(view + 1) * mine, :], out))
    copies = [pltpu.make_async_copy(src, dst, sem.at[i]) for i, (src, dst) in enumerate(pairs)]
    for cp in copies:
        cp.start()
    for cp in copies:
        cp.wait()


def step_kernel(total_rows, total_protos, z1h, z2h, ch,
                code1, code2, loss_out, gfull, gp_out,
                z1, z2, y1, y2, c_ref, f_scr, e_scr, cfull, lrow, frow, vall, zr, dall,
                cacc, vb, ub, stage, csend, crecv, sums, lossb, losst, dacc, drecv, dz, cst,
                lsem, c_ssem, c_rsem, s_ssem, s_rsem, a_ssem, a_rsem, t_ssem, t_rsem,
                v_ssem, v_rsem, g_ssem, g_rsem, l_ssem, l_rsem, x_ssem, x_rsem, o_sem):
    env = _Env()
    me, core, pos, partner = env.me, env.core, env.pos, env.partner
    remote = env.remote
    rows, cols = z1.shape[0], c_ref.shape[0]
    mine = zr.shape[0] // 2
    blocks = LINE ** AXES
    fscale = 1.0 / (2 * total_rows * TEMP_TAU)
    zs, ys = (z1, z2), (y1, y2)
    chunks, groups = rows // cols, cols // 8

    barrier = pltpu.get_barrier_semaphore()
    pl.semaphore_signal(barrier, inc=1, device_id=partner, device_id_type=MESH)
    for axis in range(AXES):
        for d in DISTS:
            pl.semaphore_signal(barrier, inc=1, device_id=env.peer(axis, d), device_id_type=MESH)
    loads = [pltpu.make_async_copy(src, dst, lsem.at[i]) for i, (src, dst) in enumerate(
        ((ch, c_ref), (z1h, z1), (z2h, z2), (ch, cfull.at[pos[2], pos[1], pos[0]])))]
    gc = _Gather(env, cfull, C_CUTS, a_ssem, a_rsem, (t_ssem, t_rsem))
    gg = _Gather(env, gfull, G_CUTS, g_ssem, g_rsem)
    for cp in loads[:3]:
        cp.start()

    def scores(view):
        cacc[view] = jnp.zeros((cols, LANES), F32)

        def body(i, _):
            n0 = pl.multiple_of(i * cols, cols)
            s = _nt(c_ref[...], zs[view][pl.ds(n0, cols), :])
            f = jnp.exp(s * (1.0 / TEMP_TAU))
            stage[0, 2 + view:3 + view, pl.ds(n0, cols)] = jnp.sum(f, axis=0, keepdims=True)
            e = f * f
            f_scr[view, :, pl.ds(n0, cols)] = f
            e_scr[view, :, :, pl.ds(n0, cols)] = e.reshape(groups, 8, cols)
            cacc[view] += e[:, :LANES] + e[:, LANES:]
            return 0
        lax.fori_loop(0, chunks, body, 0, unroll=8)
        zr[view * mine:(view + 1) * mine, :] = zs[view][pl.ds(pl.multiple_of(me * mine, mine), mine), :]

    def other_scores(view):
        def body(i, _):
            n0 = pl.multiple_of(i * cols, cols)
            f = jnp.exp(_nt(c_ref[...], ys[view][pl.ds(n0, cols), :]) * (1.0 / TEMP_TAU))
            e_scr[view, :, :, pl.ds(rows + n0, cols)] = (f * f).reshape(groups, 8, cols)
            return 0
        lax.fori_loop(0, chunks, body, 0, unroll=2)

    def row_scores(lo, hi):
        def body(q, _):
            z_, y_, x_ = block(q)
            l = _nt(zr[...], cfull[z_, y_, x_]) * (1.0 / TEMP_TAU)
            lrow[q] = l
            frow[q] = jnp.exp(l)
            return 0
        lax.fori_loop(lo, hi, body, 0, unroll=4)

    def block(q):
        return lax.div(q, LINE * LINE), lax.rem(lax.div(q, LINE), LINE), lax.rem(q, LINE)

    def column_sums(it):
        for view in range(2):
            for h in range(2):
                k = 2 * view + h
                s = jnp.sum(cacc[view, h * LANES:(h + 1) * LANES, :], axis=1, keepdims=True)
                csend[it, k:k + 1, :] = _col_to_row(s)

    def spread(vrow):
        for view in range(2):
            for h in range(2):
                k = 2 * view + h
                vb[view, h * LANES:(h + 1) * LANES, :] = jnp.broadcast_to(
                    _row_to_col(vrow[k:k + 1, :]), (LANES, LANES))

    def exchange():
        return remote(csend.at[0], crecv.at[0], c_ssem.at[0], c_rsem.at[0], partner)

    def row_sums(it, width):
        tiles = [slice(l, l + LANES) for l in range(0, width, LANES)]
        for view in range(2):
            def body(g, acc, view=view):
                w = vb[view, pl.ds(pl.multiple_of(g * 8, 8), 8), :]
                return tuple(a + e_scr[view, g, :, ls] * w for a, ls in zip(acc, tiles))
            acc = lax.fori_loop(0, groups, body, tuple(jnp.zeros((8, LANES), F32) for _ in tiles), unroll=4)
            for a, ls in zip(acc, tiles):
                stage[it, view:view + 1, ls] = jnp.sum(a, axis=0, keepdims=True)

    def weighted_columns():
        tiles = [slice(l, l + LANES) for l in range(0, 2 * rows, LANES)]
        for view in range(2):
            us = [ub[view, :, ls] for ls in tiles]

            def body(g, _, view=view, us=us):
                acc = [None] * 4
                for t, ls in enumerate(tiles):
                    x = e_scr[view, g, :, ls] * us[t]
                    acc[t % 4] = x if acc[t % 4] is None else acc[t % 4] + x
                cacc[view, pl.ds(pl.multiple_of(g * 8, 8), 8), :] = (acc[0] + acc[1]) + (acc[2] + acc[3])
                return 0
            lax.fori_loop(0, groups, body, 0, unroll=4)

    def vsend(st):
        ref = vall.at[(pos[2], pos[1], pos[0])[:AXES - st]]
        for d in DISTS:
            remote(ref, ref, v_ssem.at[st], v_rsem.at[st], env.peer(st, d))

    def v_some(st):
        return vall.at[(0,) * (AXES - 1 - st) + (pl.ds(0, LINE - 1),)]

    def vrecv(st):
        env.arrived(v_some(st), v_rsem.at[st])

    def load_sums(it, value):
        for j, (l0, l1) in enumerate(_parts(SUM_CUTS)):
            sums[it, 0, pos[j], :, l0:l1] = value[:, l0:l1]

    def send_sums(it, st):
        for d in DISTS:
            for j, (l0, l1) in enumerate(_parts(SUM_CUTS)):
                ax = (st + j) % AXES
                src = sums.at[it, st, pos[ax], :, l0:l1]
                remote(src, src, s_ssem.at[it * AXES + st], s_rsem.at[it * AXES + st], env.peer(ax, d))

    def recv_sums(it, st):
        env.arrived(sums.at[it, st, :LINE - 1], s_rsem.at[it * AXES + st])
        tot = []
        for j, (l0, l1) in enumerate(_parts(SUM_CUTS)):
            s = [sums[it, st, i, :, l0:l1] for i in range(LINE)]
            t = (s[0] + s[1]) + (s[2] + s[3])
            tot.append(t)
            if st < AXES - 1:
                sums[it, st + 1, pos[(st + 1 + j) % AXES], :, l0:l1] = t
        return tot

    def denominators(st):
        if st == 0:
            load_sums(ITERS, stage[0, 2:4])
        else:
            tot = recv_sums(ITERS, st - 1)
        if st < AXES:
            send_sums(ITERS, st)
            return
        for (l0, l1), t in zip(_parts(SUM_CUTS), tot):
            dall[2:4, l0:l1] = t

    def hidden(slot):
        if slot in (1, 2):
            env.arrived(ys[slot - 1], x_rsem.at[slot - 1])
            other_scores(slot - 1)
        elif slot == 7:
            gc.t_recv()
            row_scores(0, blocks // 2)
        elif slot == 8:
            row_scores(blocks // 2, blocks)
        if slot in (3, 4, 5, 6):
            denominators(slot - 3)

    @pl.when(core == 1)
    def _():
        loads[0].wait()
        for view in range(2):
            loads[1 + view].wait()
            scores(view)
        pl.semaphore_wait(barrier, 1 + AXES * (LINE - 1))
        column_sums(0)
        exchange().wait()
        total = csend[0] + crecv[0]
        for it in range(ITERS):
            last = it == ITERS - 1
            vrow = 1.0 / (float(total_protos) * total)
            if last:
                vall[pos[2], pos[1], pos[0]] = vrow
                vsend(0)
            spread(vrow)
            row_sums(it, rows if it == 0 else 2 * rows)
            if it == 0:
                env.arrived(stage.at[0, :, rows:], x_rsem.at[2])
            load_sums(it, stage[it, 0:2])
            for st in range(AXES):
                send_sums(it, st)
                hidden(it * AXES + st)
                if last:
                    vrecv(st)
                    if st < AXES - 1:
                        vsend(st + 1)
                tot = recv_sums(it, st)
                if st < AXES - 1:
                    continue
                for (l0, l1), t in zip(_parts(SUM_CUTS), tot):
                    if last:
                        dall[0:2, l0:l1] = t
                    else:
                        u = 1.0 / (float(total_rows) * t)
                        for view in range(2):
                            ub[view, :, l0:l1] = jnp.broadcast_to(u[view:view + 1], (8, l1 - l0))
            if not last:
                weighted_columns()
                column_sums(it + 1)
                total = csend[it + 1]
        remote(dall.at[:, rows:], dall.at[:, :rows], x_ssem.at[3], x_rsem.at[3], partner)
        remote(vall, vall, x_ssem.at[4], x_rsem.at[4], partner)

    @pl.when(core == 0)
    def _():
        loads[3].start()
        loads[0].wait()
        for view in range(2):
            loads[1 + view].wait()
            scores(view)
        column_sums(0)
        loads[3].wait()
        pl.semaphore_wait(barrier, 1 + AXES * (LINE - 1))
        cp = exchange()
        gc.run('SA10P')
        cp.wait()
        vrow = 1.0 / (float(total_protos) * (csend[0] + crecv[0]))
        spread(vrow)
        row_sums(0, rows)
        remote(stage.at[0, :, :rows], stage.at[0, :, rows:], x_ssem.at[2], x_rsem.at[2], partner)
        for i in range(2):
            remote(zs[i], ys[i], x_ssem.at[i], x_rsem.at[i], partner)
        gc.run('sA11A13A12QT00')
        gc.run('f10B10f11B11f13B13f12B12g10g11A21g13g12A23')
        gc.run('f20B20b10b11b13b12A22T10T30T20')
        gc.run('f21B21f23B23g20g21g23T01T03T11T13T31T33')
        gc.run('f22B22g22T21T23b20T02b21T12b23T32b22T22')
        row_scores(0, blocks)
        env.arrived(dall.at[:, :rows], x_rsem.at[3])
        env.arrived(vall, x_rsem.at[4])
        gc.all_sent()
        for i, ref in enumerate((z1, z2, stage.at[0, :, :rows])):
            env.sent(ref, x_ssem.at[i])
        env.sent(cfull, t_ssem.at[0])
        env.drain()

    tile = pl.multiple_of(lax.div(me * mine, LANES) * LANES, LANES)
    shift = lax.rem(me * mine, LANES)
    dv = dall[:, pl.ds(tile, LANES)]
    col = [_row_to_col(dv[i:i + 1, :], mine, shift) for i in range(4)]
    rc = jnp.broadcast_to(1.0 / jnp.concatenate(col[0:2], axis=0), (2 * mine, LANES))
    den = jnp.concatenate(col[2:4], axis=0)
    dc = jnp.broadcast_to(1.0 / den, (2 * mine, LANES))
    ld = jnp.broadcast_to(jnp.log(den), (2 * mine, LANES))

    def code_rows(q, h):
        z_, y_, x_ = block(q)
        f = frow[q, :, h * LANES:(h + 1) * LANES]
        v0 = jnp.broadcast_to(vall[z_, y_, x_, h:h + 1, :], (mine, LANES))
        v1 = jnp.broadcast_to(vall[z_, y_, x_, 2 + h:3 + h, :], (mine, LANES))
        return f, f * f * (rc * jnp.concatenate([v0, v1], axis=0))

    def dzbody(i, acc):
        hs = []
        for x_ in range(LINE):
            for h in range(2):
                f, code = code_rows(i * LINE + x_, h)
                other = jnp.concatenate([code[mine:], code[:mine]], axis=0)
                hs.append(((f * dc - other) * fscale).astype(BF16))
        cl = cfull[lax.div(i, LINE), lax.rem(i, LINE)].reshape(LINE * cols, cols)
        return acc + _nn(jnp.concatenate(hs, axis=1), cl)

    dz[...] = lax.fori_loop(0, LINE * LINE, dzbody, jnp.zeros((2 * mine, cols), F32), unroll=4)

    own = pltpu.make_async_copy(dz, gfull.at[pos[2], pos[1], pos[0]], o_sem.at[0])
    own.start()
    gg.s1_send(dz)
    own.wait()
    gg.run('A10P')
    spread(vall[pos[2], pos[1], pos[0]])
    dacc[...] = jnp.zeros((cols, cols), F32)

    def out_copy(view, i):
        n0 = pl.multiple_of(i * cols, cols)
        return pltpu.make_async_copy(cst.at[view, pl.ds(n0, cols), :], (code1, code2)[view].at[pl.ds(n0, cols), :],
                                     o_sem.at[2 + view])

    def columns(i):
        def body(i, _):
            n0 = pl.multiple_of(i * cols, cols)
            inv = 1.0 / dall[:, pl.ds(n0, cols)]
            code, prob = [], []
            for view in range(2):
                w = jnp.concatenate([vb[view], vb[view]], axis=1)
                code.append(e_scr[view, :, :, pl.ds(n0, cols)].reshape(cols, cols) * w * inv[view:view + 1, :])
                prob.append(f_scr[view, :, pl.ds(n0, cols)] * inv[2 + view:3 + view, :])
            for view in range(2):
                h = ((prob[view] - code[1 - view]) * fscale).astype(BF16)
                dacc[...] += _nn(h, zs[view][pl.ds(n0, cols), :])
                cst[view, pl.ds(n0, cols), :] = code[view].T
                out_copy(view, i).start()
            return 0
        lax.fori_loop(i * 2, i * 2 + 2, body, 0, unroll=True)

    def lbody(q, acc):
        for h in range(2):
            f, code = code_rows(q, h)
            lp = lrow[q, :, h * LANES:(h + 1) * LANES] - ld
            other = jnp.concatenate([code[mine:], code[:mine]], axis=0)
            acc = acc + other * lp
        return acc
    part = lax.fori_loop(0, blocks, lbody, jnp.zeros((2 * mine, LANES), F32), unroll=4)
    lossb[0, pos[0]] = jnp.sum(part.reshape(2 * mine // 8, 8, LANES), axis=0)

    def loss_send(st):
        ref = lossb.at[st, pos[st]]
        for d in DISTS:
            remote(ref, ref, l_ssem.at[st], l_rsem.at[st], env.peer(st, d))
        env.sent(lossb.at[st, :LINE - 1], l_ssem.at[st])

    def loss_recv(st):
        env.arrived(lossb.at[st, :LINE - 1], l_rsem.at[st])
        return (lossb[st, 0] + lossb[st, 1]) + (lossb[st, 2] + lossb[st, 3])

    gg.run('sA11A13A12Q')
    loss_send(0)
    columns(0)
    gg.run('f10B10f11B11f13B13f12B12g10g11A21g13g12A23')
    lossb[1, pos[1]] = loss_recv(0)
    loss_send(1)
    columns(1)
    gg.run('f20B20b10b11b13b12A22')
    lossb[2, pos[2]] = loss_recv(1)
    loss_send(2)
    columns(2)
    gg.run('f21B21f23B23')
    columns(3)
    losst[0] = loss_recv(2)
    lcp = remote(losst.at[0], losst.at[1], l_ssem.at[3], l_rsem.at[3], partner)
    dcp = remote(dacc, drecv, l_ssem.at[4], l_rsem.at[4], partner)
    gg.run('f22B22')
    lcp.wait_recv()
    loss_out[...] = jnp.sum(losst[0] + losst[1], keepdims=True) * (-1.0 / (2 * total_rows))
    dcp.wait_recv()
    drecv[...] = dacc[...] + drecv[...]
    gpc = pltpu.make_async_copy(drecv, gp_out, o_sem.at[1])
    gpc.start()
    gg.run('g20g21g23g22b20b21b23b22')
    gpc.wait()
    for view, out in enumerate((code1, code2)):
        pltpu.make_async_copy(cst.at[view], out, o_sem.at[2 + view]).wait()
    gg.all_sent()
    env.sent(losst.at[0], l_ssem.at[3])
    env.sent(dacc, l_ssem.at[4])
    env.drain()

    @pl.when(core == 1)
    def _():
        for it in range(ITERS + 1):
            for st in range(AXES):
                env.sent(sums.at[it, st, :LINE - 1], s_ssem.at[it * AXES + st])
        for st in range(AXES):
            env.sent(v_some(st), v_ssem.at[st])
        env.sent(dall.at[:, rows:], x_ssem.at[3])
        env.sent(vall, x_ssem.at[4])
        env.drain()


def solution(mesh):
    proto_size = mesh.shape['proto']
    data_size = mesh.shape['data']

    def local_step(emb_one, emb_two, protos):
        rows, dim = emb_one.shape
        cols = protos.shape[0]
        total_rows = rows * data_size
        total_protos = cols * proto_size
        mine = rows // proto_size
        vm = pl.BlockSpec(memory_space=pltpu.VMEM)
        hbm = pl.BlockSpec(memory_space=pltpu.HBM)
        free = pl.BlockSpec(memory_space=pl.ANY)
        nsem = (ITERS + 1) * AXES
        dma = lambda n: pltpu.SemaphoreType.DMA((n,))
        grid3 = (LINE,) * AXES
        sds = jax.ShapeDtypeStruct
        code = sds((rows, cols), F32)
        zbuf = pltpu.VMEM((rows, dim), BF16)
        square = pltpu.VMEM((cols, dim), F32)
        rowbuf = pltpu.VMEM((proto_size, 2 * mine, cols), F32)
        small = pltpu.VMEM((ITERS, 4, LANES), F32)
        spread = pltpu.VMEM((2, cols, LANES), F32)
        args = [pltpu.with_memory_space_constraint(a, pltpu.HBM) for a in (emb_one, emb_two, protos)]
        code1, code2, loss, gall, gp = pl.pallas_call(
            functools.partial(step_kernel, total_rows, total_protos),
            out_shape=(code, code, sds((1, 1), F32),
                       sds(grid3 + (2 * mine, dim), F32), sds((cols, dim), F32)),
            in_specs=[hbm] * 3,
            out_specs=(free, free, vm, free, free),
            scratch_shapes=[
                zbuf, zbuf, zbuf, zbuf, pltpu.VMEM((cols, dim), BF16),
                pltpu.VMEM((2, cols, rows), F32),
                pltpu.VMEM((2, cols // 8, 8, total_rows), F32),
                pltpu.VMEM(grid3 + (cols, dim), BF16),
                rowbuf, rowbuf,
                pltpu.VMEM(grid3 + (4, LANES), F32),
                pltpu.VMEM((2 * mine, dim), BF16),
                pltpu.VMEM((4, total_rows), F32),
                spread, spread,
                pltpu.VMEM((2, 8, total_rows), F32),
                pltpu.VMEM((ITERS, 4, total_rows), F32),
                small, small,
                pltpu.VMEM((ITERS + 1, AXES, LINE, 2, total_rows), F32),
                pltpu.VMEM((AXES, LINE, 8, LANES), F32),
                pltpu.VMEM((2, 8, LANES), F32),
                square, square,
                pltpu.VMEM((2 * mine, dim), F32),
                pltpu.VMEM((2, rows, cols), F32),
                dma(4), dma(1), dma(1), dma(nsem), dma(nsem),
                dma(5), dma(AG_SEMS), dma(1), dma(1),
                dma(AXES), dma(AXES), dma(5), dma(AG_SEMS), dma(5), dma(5),
                dma(5), dma(5), dma(4),
            ],
            compiler_params=pltpu.CompilerParams(collective_id=0, has_side_effects=True,
                                                 vmem_limit_bytes=44 * 2 ** 20),
        )(*args)
        blocked = sds((proto_size, mine, dim), F32)
        o1, o2, g1, g2, og = pl.pallas_call(
            functools.partial(write_kernel, mine),
            out_shape=(code, code, blocked, blocked, sds((cols, dim), F32)),
            in_specs=[vm] * 4,
            out_specs=(hbm,) * 5,
            scratch_shapes=[dma(5)],
            compiler_params=pltpu.CompilerParams(vmem_limit_bytes=2 ** 20),
        )(code1, code2, gall.reshape(proto_size, 2 * mine, dim), gp)
        return o1, o2, loss[0, 0], g1.reshape(rows, dim), g2.reshape(rows, dim), og

    return jax.shard_map(
        local_step, mesh=mesh,
        in_specs=(P('data', None), P('data', None), P('proto', None)),
        out_specs=(P('data', 'proto'), P('data', 'proto'), P(), P('data', None), P('data', None), P('proto', None)),
        check_vma=False)
```

```python
import functools
import re

import jax
import jax.numpy as jnp
from jax import lax
from jax.experimental import pallas as pl
from jax.experimental.pallas import tpu as pltpu
from jax.sharding import PartitionSpec as P

EPSILON = 0.05
TEMP_TAU = 0.1
ITERS = 3
LINE = 4
AXES = 3
MESH = pl.DeviceIdType.MESH
F32 = jnp.float32
BF16 = jnp.bfloat16
LANES = 128
SUM_CUTS = (0, 1408, 2816, 4096)
C_CUTS = (0, 80, 160, 256)
G_CUTS = ((0, 40, 88, 128), (0, 40, 80, 128))
AG_SEMS = 27
DISTS = (2, 1, 3)


def _nt(a, b):
    return lax.dot_general(a, b, (((1,), (1,)), ((), ())), preferred_element_type=F32)


def _nn(a, b):
    return jnp.dot(a, b, preferred_element_type=F32)


def _col_to_row(s):
    r = lax.broadcasted_iota(jnp.int32, (LANES, LANES), 0)
    c = lax.broadcasted_iota(jnp.int32, (LANES, LANES), 1)
    return jnp.sum(jnp.where(r == c, s, 0.0), axis=0, keepdims=True)


def _row_to_col(row, n=LANES, shift=0):
    r = lax.broadcasted_iota(jnp.int32, (n, LANES), 0)
    c = lax.broadcasted_iota(jnp.int32, (n, LANES), 1)
    return jnp.sum(jnp.where(c == r + shift, row, 0.0), axis=1, keepdims=True)


def _parts(cuts):
    return tuple(zip(cuts[:-1], cuts[1:]))


class _Env:
    def __init__(self):
        self.me = lax.axis_index('proto')
        self.core = lax.axis_index('data')
        me = self.me
        self.pos = [lax.rem(me, LINE), lax.rem(lax.div(me, LINE), LINE), lax.div(me, LINE * LINE)]
        self.stride = [1, LINE, LINE * LINE]
        self.pending = []
        self.partner = (me, 1 - self.core)

    def p(self, axis, d):
        return self.pos[axis] if d == 0 else lax.rem(self.pos[axis] + d, LINE)

    def peer(self, axis, d):
        return (self.me + (self.p(axis, d) - self.pos[axis]) * self.stride[axis], self.core)

    def remote(self, src, dst, ss, rs, dev):
        cp = pltpu.make_async_remote_copy(src, dst, ss, rs, device_id=dev, device_id_type=MESH)
        cp.start()
        return cp

    def sent(self, ref, ss):
        self.pending.append(pltpu.make_async_remote_copy(ref, ref, ss, ss, device_id=self.partner,
                                                         device_id_type=MESH))

    def arrived(self, ref, rs):
        pltpu.make_async_remote_copy(ref, ref, rs, rs, device_id=self.partner, device_id_type=MESH).wait_recv()

    def drain(self):
        for cp in self.pending:
            cp.wait_send()
        self.pending.clear()


class _Gather:
    def __init__(self, env, buf, cuts, ssem, rsem, twin=None):
        self.env, self.buf, self.parts = env, buf, _parts(cuts)
        self.ssem, self.rsem, self.twin = ssem, rsem, twin

    def at(self, j, i0, i1, i2):
        ids = [None] * AXES
        for axis, i in zip((j, j + 1, j + 2), (i0, i1, i2)):
            ids[axis % AXES] = slice(None) if i is None else i
        r0, r1 = self.parts[j]
        return self.buf.at[ids[2], ids[1], ids[0], r0:r1, :]

    def p(self, j, level, d):
        return self.env.p((j + level) % AXES, d)

    def send(self, j, group, k, ref, level, d, src=None):
        self.env.remote(ref if src is None else src, ref, self.ssem.at[group], self.rsem.at[k],
                        self.env.peer((j + level) % AXES, d))

    def some(self, blocks):
        for level in range(AXES):
            width = LINE ** level
            if blocks <= width * (LINE - 1):
                lead = (0,) * (AXES - 1 - level)
                return self.buf.at[lead + (pl.ds(0, blocks // width),)]

    def recv(self, k, blocks):
        self.env.arrived(self.some(blocks), self.rsem.at[k])

    def all_sent(self):
        for group, blocks in enumerate((3, 8, 4, 32, 16)):
            self.env.sent(self.some(blocks), self.ssem.at[group])

    def s1_send(self, src=None):
        for d in DISTS:
            for j, (r0, r1) in enumerate(self.parts):
                ref = self.at(j, self.p(j, 0, 0), self.p(j, 1, 0), self.p(j, 2, 0))
                self.send(j, 0, d - 1, ref, 0, d, None if src is None else src.at[r0:r1, :])

    def s1_recv(self):
        for d in (1, 3, 2):
            self.recv(d - 1, 1)

    def chunk(self, j, level, k, m):
        if level == 1:
            return self.at(j, self.p(j, 0, k), self.p(j, 1, m), self.p(j, 2, 0))
        return self.at(j, None, self.p(j, 1, k), self.p(j, 2, m))

    def slot(self, level, k, d):
        return 12 * level - 9 + k + LINE * (d // 2)

    def a_send(self, level, k):
        for j in range(AXES):
            ref = self.chunk(j, level, k, 0)
            for d in (1, 3):
                self.send(j, 2 * level - 1, self.slot(level, k, d), ref, level, d)

    def way(self, k):
        return 1 if k < 2 else 3

    def f_recv(self, level, k):
        self.recv(self.slot(level, k, self.way(k)), LINE ** (level - 1))

    def g_recv(self, level, k):
        self.recv(self.slot(level, k, LINE - self.way(k)), LINE ** (level - 1))

    def piece_send(self, *offsets):
        for k in offsets:
            for j in range(AXES):
                ref = self.chunk(j, 1, k, 0)
                for d in (1, 3):
                    self.send(j, 3, self.slot(2, 0, d), ref, 2, d)

    def own_piece(self):
        self.piece_send(0)

    def other_pieces(self):
        self.piece_send(1, 3, 2)

    def b_send(self, level, k):
        d = self.way(k)
        for j in range(AXES):
            self.send(j, 2 * level, self.slot(level, k, 5), self.chunk(j, level, k, LINE - d), level, d)

    def b_recv(self, level, k):
        self.recv(self.slot(level, k, 5), LINE ** (level - 1))

    def t_send(self, k, m):
        ts, tr = self.twin
        for j in range(AXES):
            ref = self.chunk(j, 2, k, m)
            self.env.remote(ref, ref, ts.at[0], tr.at[0], self.env.partner)

    def t_recv(self):
        self.env.arrived(self.buf, self.twin[1].at[0])

    def run(self, ops):
        for op in re.findall('[a-zA-Z][0-9]*', ops):
            args = [int(c) for c in op[1:]]
            {'S': self.s1_send, 's': self.s1_recv, 'A': self.a_send, 'f': self.f_recv, 'g': self.g_recv,
             'B': self.b_send, 'b': self.b_recv, 'T': self.t_send, 'P': self.own_piece, 'Q': self.other_pieces}[op[0]](*args)


def write_kernel(mine, code1, code2, gfull, gp, o1, o2, g1, g2, og, sem):
    half = code1.shape[0] // 2
    pairs = [(gp, og)]
    for h in range(2):
        for src, dst in ((code1, o1), (code2, o2)):
            pairs.append((src.at[h * half:(h + 1) * half, :], dst.at[h * half:(h + 1) * half, :]))
        for view, dst in enumerate((g1, g2)):
            r = (2 * h + view) * mine
            pairs.append((gfull.at[:, r:r + mine, :], dst.at[:, :, h * LANES:(h + 1) * LANES]))
    copies = [pltpu.make_async_copy(src, dst, sem.at[i]) for i, (src, dst) in enumerate(pairs)]
    for cp in copies:
        cp.start()
    for cp in copies:
        cp.wait()


def step_kernel(total_rows, total_protos, z1h, z2h, ch,
                code1, code2, loss_out, gfull, gp_out,
                z1, z2, y1, y2, c_ref, f_scr, e_scr, cfull, lrow, frow, vall, zr, dall,
                cacc, vb, ub, stage, csend, crecv, sums, lossb, losst, dacc, drecv, dz, cst,
                lsem, c_ssem, c_rsem, s_ssem, s_rsem, a_ssem, a_rsem, t_ssem, t_rsem,
                v_ssem, v_rsem, l_ssem, l_rsem, x_ssem, x_rsem, o_sem):
    env = _Env()
    me, core, pos, partner = env.me, env.core, env.pos, env.partner
    remote = env.remote
    rows, cols = z1.shape[0], c_ref.shape[0]
    mine = zr.shape[0] // 2
    blocks = LINE ** AXES
    fscale = 1.0 / (2 * total_rows * TEMP_TAU)
    zs, ys = (z1, z2), (y1, y2)
    chunks, groups = rows // cols, cols // 8

    barrier = pltpu.get_barrier_semaphore()
    pl.semaphore_signal(barrier, inc=1, device_id=partner, device_id_type=MESH)
    for axis in range(AXES):
        for d in DISTS:
            pl.semaphore_signal(barrier, inc=1, device_id=env.peer(axis, d), device_id_type=MESH)
    loads = [pltpu.make_async_copy(src, dst, lsem.at[i]) for i, (src, dst) in enumerate(
        ((ch, c_ref), (z1h, z1), (z2h, z2), (ch, cfull.at[pos[2], pos[1], pos[0]])))]
    gc = _Gather(env, cfull, C_CUTS, a_ssem, a_rsem, (t_ssem, t_rsem))
    gg = [_Gather(env, gfull, cuts, a_ssem, a_rsem) for cuts in G_CUTS]

    def by_core(fn):
        for c in range(2):
            pl.when(core == c)(functools.partial(fn, c))

    def grun(ops):
        by_core(lambda c: gg[c].run(ops))

    for cp in loads[:3]:
        cp.start()

    def scores(view):
        cacc[view] = jnp.zeros((cols, LANES), F32)

        def body(i, _):
            n0 = pl.multiple_of(i * cols, cols)
            s = _nt(c_ref[...], zs[view][pl.ds(n0, cols), :])
            f = jnp.exp(s * (1.0 / TEMP_TAU))
            stage[0, 2 + view:3 + view, pl.ds(n0, cols)] = jnp.sum(f, axis=0, keepdims=True)
            e = f * f
            f_scr[view, :, pl.ds(n0, cols)] = f
            e_scr[view, :, :, pl.ds(n0, cols)] = e.reshape(groups, 8, cols)
            cacc[view] += e[:, :LANES] + e[:, LANES:]
            return 0
        lax.fori_loop(0, chunks, body, 0, unroll=8)
        zr[view * mine:(view + 1) * mine, :] = zs[view][pl.ds(pl.multiple_of(me * mine, mine), mine), :]

    def other_scores(view):
        def body(i, _):
            n0 = pl.multiple_of(i * cols, cols)
            f = jnp.exp(_nt(c_ref[...], ys[view][pl.ds(n0, cols), :]) * (1.0 / TEMP_TAU))
            e_scr[view, :, :, pl.ds(rows + n0, cols)] = (f * f).reshape(groups, 8, cols)
            return 0
        lax.fori_loop(0, chunks, body, 0, unroll=2)

    def row_scores(lo, hi):
        def body(q, _):
            z_, y_, x_ = block(q)
            l = _nt(zr[...], cfull[z_, y_, x_]) * (1.0 / TEMP_TAU)
            lrow[q] = l
            frow[q] = jnp.exp(l)
            return 0
        lax.fori_loop(lo, hi, body, 0, unroll=4)

    def block(q):
        return lax.div(q, LINE * LINE), lax.rem(lax.div(q, LINE), LINE), lax.rem(q, LINE)

    def column_sums(it):
        for view in range(2):
            for h in range(2):
                k = 2 * view + h
                s = jnp.sum(cacc[view, h * LANES:(h + 1) * LANES, :], axis=1, keepdims=True)
                csend[it, k:k + 1, :] = _col_to_row(s)

    def spread(vrow):
        for view in range(2):
            for h in range(2):
                k = 2 * view + h
                vb[view, h * LANES:(h + 1) * LANES, :] = jnp.broadcast_to(
                    _row_to_col(vrow[k:k + 1, :]), (LANES, LANES))

    def exchange():
        return remote(csend.at[0], crecv.at[0], c_ssem.at[0], c_rsem.at[0], partner)

    def row_sums(it, width):
        tiles = [slice(l, l + LANES) for l in range(0, width, LANES)]
        for view in range(2):
            def body(g, acc, view=view):
                w = vb[view, pl.ds(pl.multiple_of(g * 8, 8), 8), :]
                return tuple(a + e_scr[view, g, :, ls] * w for a, ls in zip(acc, tiles))
            acc = lax.fori_loop(0, groups, body, tuple(jnp.zeros((8, LANES), F32) for _ in tiles), unroll=4)
            for a, ls in zip(acc, tiles):
                stage[it, view:view + 1, ls] = jnp.sum(a, axis=0, keepdims=True)

    def weighted_columns():
        tiles = [slice(l, l + LANES) for l in range(0, 2 * rows, LANES)]
        for view in range(2):
            us = [ub[view, :, ls] for ls in tiles]

            def body(g, _, view=view, us=us):
                acc = [None] * 4
                for t, ls in enumerate(tiles):
                    x = e_scr[view, g, :, ls] * us[t]
                    acc[t % 4] = x if acc[t % 4] is None else acc[t % 4] + x
                cacc[view, pl.ds(pl.multiple_of(g * 8, 8), 8), :] = (acc[0] + acc[1]) + (acc[2] + acc[3])
                return 0
            lax.fori_loop(0, groups, body, 0, unroll=4)

    def vsend(st):
        ref = vall.at[(pos[2], pos[1], pos[0])[:AXES - st]]
        for d in DISTS:
            remote(ref, ref, v_ssem.at[st], v_rsem.at[st], env.peer(st, d))

    def v_some(st):
        return vall.at[(0,) * (AXES - 1 - st) + (pl.ds(0, LINE - 1),)]

    def vrecv(st):
        env.arrived(v_some(st), v_rsem.at[st])

    def load_sums(it, value):
        for j, (l0, l1) in enumerate(_parts(SUM_CUTS)):
            sums[it, 0, pos[j], :, l0:l1] = value[:, l0:l1]

    def send_sums(it, st):
        for d in DISTS:
            for j, (l0, l1) in enumerate(_parts(SUM_CUTS)):
                ax = (st + j) % AXES
                src = sums.at[it, st, pos[ax], :, l0:l1]
                remote(src, src, s_ssem.at[0], s_rsem.at[it * AXES + st], env.peer(ax, d))

    def recv_sums(it, st):
        env.arrived(sums.at[it, st, :LINE - 1], s_rsem.at[it * AXES + st])
        tot = []
        for j, (l0, l1) in enumerate(_parts(SUM_CUTS)):
            s = [sums[it, st, i, :, l0:l1] for i in range(LINE)]
            t = (s[0] + s[1]) + (s[2] + s[3])
            tot.append(t)
            if st < AXES - 1:
                sums[it, st + 1, pos[(st + 1 + j) % AXES], :, l0:l1] = t
        return tot

    def denominators(st):
        if st == 0:
            load_sums(ITERS, stage[0, 2:4])
        else:
            tot = recv_sums(ITERS, st - 1)
        if st < AXES:
            send_sums(ITERS, st)
            return
        for (l0, l1), t in zip(_parts(SUM_CUTS), tot):
            dall[2:4, l0:l1] = t

    def hidden(slot):
        if slot in (1, 2):
            env.arrived(ys[slot - 1], x_rsem.at[slot - 1])
            other_scores(slot - 1)
        elif slot == 7:
            gc.t_recv()
            row_scores(0, blocks // 2)
        elif slot == 8:
            row_scores(blocks // 2, blocks)
        if slot in (3, 4, 5, 6):
            denominators(slot - 3)

    @pl.when(core == 1)
    def _():
        loads[0].wait()
        for view in range(2):
            loads[1 + view].wait()
            scores(view)
        pl.semaphore_wait(barrier, 1 + AXES * (LINE - 1))
        column_sums(0)
        exchange().wait()
        total = csend[0] + crecv[0]
        for it in range(ITERS):
            last = it == ITERS - 1
            vrow = 1.0 / (float(total_protos) * total)
            if last:
                vall[pos[2], pos[1], pos[0]] = vrow
                vsend(0)
            spread(vrow)
            row_sums(it, rows if it == 0 else 2 * rows)
            if it == 0:
                env.arrived(stage.at[0, :, rows:], x_rsem.at[2])
            load_sums(it, stage[it, 0:2])
            for st in range(AXES):
                send_sums(it, st)
                hidden(it * AXES + st)
                if last:
                    vrecv(st)
                    if st < AXES - 1:
                        vsend(st + 1)
                tot = recv_sums(it, st)
                if st < AXES - 1:
                    continue
                for (l0, l1), t in zip(_parts(SUM_CUTS), tot):
                    if last:
                        dall[0:2, l0:l1] = t
                    else:
                        u = 1.0 / (float(total_rows) * t)
                        for view in range(2):
                            ub[view, :, l0:l1] = jnp.broadcast_to(u[view:view + 1], (8, l1 - l0))
            if not last:
                weighted_columns()
                column_sums(it + 1)
                total = csend[it + 1]
        remote(dall.at[:, rows:], dall.at[:, :rows], x_ssem.at[3], x_rsem.at[3], partner)
        remote(vall, vall, x_ssem.at[4], x_rsem.at[4], partner)

    @pl.when(core == 0)
    def _():
        loads[3].start()
        loads[0].wait()
        for view in range(2):
            loads[1 + view].wait()
            scores(view)
        column_sums(0)
        loads[3].wait()
        pl.semaphore_wait(barrier, 1 + AXES * (LINE - 1))
        cp = exchange()
        gc.run('SA10P')
        cp.wait()
        vrow = 1.0 / (float(total_protos) * (csend[0] + crecv[0]))
        spread(vrow)
        row_sums(0, rows)
        remote(stage.at[0, :, :rows], stage.at[0, :, rows:], x_ssem.at[2], x_rsem.at[2], partner)
        for i in range(2):
            remote(zs[i], ys[i], x_ssem.at[i], x_rsem.at[i], partner)
        gc.run('sA11A13A12QT00')
        gc.run('f10B10f11B11f13B13f12B12g10g11A21g13g12A23')
        gc.run('f20B20b10b11b13b12A22T10T30T20')
        gc.run('f21B21f23B23g20g21g23T01T03T11T13T31T33')
        gc.run('f22B22g22T21T23b20T02b21T12b23T32b22T22')
        row_scores(0, blocks)
        env.arrived(dall.at[:, :rows], x_rsem.at[3])
        env.arrived(vall, x_rsem.at[4])
        gc.all_sent()
        for i, ref in enumerate((z1, z2, stage.at[0, :, :rows])):
            env.sent(ref, x_ssem.at[i])
        env.sent(cfull, t_ssem.at[0])
        env.drain()

    tile = pl.multiple_of(lax.div(me * mine, LANES) * LANES, LANES)
    shift = lax.rem(me * mine, LANES)
    dv = dall[:, pl.ds(tile, LANES)]
    col = [_row_to_col(dv[i:i + 1, :], mine, shift) for i in range(4)]
    rc = jnp.broadcast_to(1.0 / jnp.concatenate(col[0:2], axis=0), (2 * mine, LANES))
    den = jnp.concatenate(col[2:4], axis=0)
    dc = jnp.broadcast_to(1.0 / den, (2 * mine, LANES))
    ld = jnp.broadcast_to(jnp.log(den), (2 * mine, LANES))

    def code_rows(q, h):
        z_, y_, x_ = block(q)
        f = frow[q, :, h * LANES:(h + 1) * LANES]
        v0 = jnp.broadcast_to(vall[z_, y_, x_, h:h + 1, :], (mine, LANES))
        v1 = jnp.broadcast_to(vall[z_, y_, x_, 2 + h:3 + h, :], (mine, LANES))
        return f, f * f * (rc * jnp.concatenate([v0, v1], axis=0))

    def dzbody(i, acc):
        hs = []
        for x_ in range(LINE):
            for h in range(2):
                f, code = code_rows(i * LINE + x_, h)
                other = jnp.concatenate([code[mine:], code[:mine]], axis=0)
                hs.append(((f * dc - other) * fscale).astype(BF16))
        cl = cfull[lax.div(i, LINE), lax.rem(i, LINE)].reshape(LINE * cols, cols)
        return acc + _nn(jnp.concatenate(hs, axis=1), cl)

    rowgrad = lax.fori_loop(0, LINE * LINE, dzbody, jnp.zeros((2 * mine, cols), F32), unroll=4)
    dz[...] = jnp.concatenate([rowgrad[:, :LANES], rowgrad[:, LANES:]], axis=0)

    own = pltpu.make_async_copy(dz, gfull.at[pos[2], pos[1], pos[0]], o_sem.at[0])
    own.start()
    by_core(lambda c: gg[c].s1_send(dz))
    own.wait()
    grun('A10P')
    spread(vall[pos[2], pos[1], pos[0]])
    dacc[...] = jnp.zeros((cols, cols), F32)

    def out_copy(view, i):
        n0 = pl.multiple_of(i * cols, cols)
        return pltpu.make_async_copy(cst.at[view, pl.ds(n0, cols), :], (code1, code2)[view].at[pl.ds(n0, cols), :],
                                     o_sem.at[2 + view])

    def columns(i):
        def body(i, _):
            n0 = pl.multiple_of(i * cols, cols)
            inv = 1.0 / dall[:, pl.ds(n0, cols)]
            code, prob = [], []
            for view in range(2):
                w = jnp.concatenate([vb[view], vb[view]], axis=1)
                code.append(e_scr[view, :, :, pl.ds(n0, cols)].reshape(cols, cols) * w * inv[view:view + 1, :])
                prob.append(f_scr[view, :, pl.ds(n0, cols)] * inv[2 + view:3 + view, :])
            for view in range(2):
                h = ((prob[view] - code[1 - view]) * fscale).astype(BF16)
                dacc[...] += _nn(h, zs[view][pl.ds(n0, cols), :])
                cst[view, pl.ds(n0, cols), :] = code[view].T
                out_copy(view, i).start()
            return 0
        lax.fori_loop(i * 2, i * 2 + 2, body, 0, unroll=True)

    def lbody(q, acc):
        for h in range(2):
            f, code = code_rows(q, h)
            lp = lrow[q, :, h * LANES:(h + 1) * LANES] - ld
            other = jnp.concatenate([code[mine:], code[:mine]], axis=0)
            acc = acc + other * lp
        return acc
    part = lax.fori_loop(0, blocks, lbody, jnp.zeros((2 * mine, LANES), F32), unroll=4)
    lossb[0, pos[0]] = jnp.sum(part.reshape(2 * mine // 8, 8, LANES), axis=0)

    def loss_send(st):
        ref = lossb.at[st, pos[st]]
        for d in DISTS:
            remote(ref, ref, l_ssem.at[st], l_rsem.at[st], env.peer(st, d))
        env.sent(lossb.at[st, :LINE - 1], l_ssem.at[st])

    def loss_recv(st):
        env.arrived(lossb.at[st, :LINE - 1], l_rsem.at[st])
        return (lossb[st, 0] + lossb[st, 1]) + (lossb[st, 2] + lossb[st, 3])

    loss_send(0)
    grun('sA11A13A12Q')
    columns(0)
    lossb[1, pos[1]] = loss_recv(0)
    loss_send(1)
    grun('f10B10f11B11f13B13f12B12g10g11A21g13g12A23')
    columns(1)
    lossb[2, pos[2]] = loss_recv(1)
    loss_send(2)
    grun('f20B20b10b11b13b12A22')
    columns(2)
    grun('f21B21f23B23')
    columns(3)
    dcp = remote(dacc, drecv, l_ssem.at[4], l_rsem.at[4], partner)
    grun('f22B22')
    losst[0] = loss_recv(2)
    lcp = remote(losst.at[0], losst.at[1], l_ssem.at[3], l_rsem.at[3], partner)
    lcp.wait_recv()
    loss_out[...] = jnp.sum(losst[0] + losst[1], keepdims=True) * (-1.0 / (2 * total_rows))
    dcp.wait_recv()
    drecv[...] = dacc[...] + drecv[...]
    gpc = pltpu.make_async_copy(drecv, gp_out, o_sem.at[1])
    gpc.start()
    grun('g20g21g23g22b20b21b23b22')
    gpc.wait()
    for view, out in enumerate((code1, code2)):
        pltpu.make_async_copy(cst.at[view], out, o_sem.at[2 + view]).wait()
    gg[0].all_sent()
    env.sent(losst.at[0], l_ssem.at[3])
    env.sent(dacc, l_ssem.at[4])
    env.drain()

    @pl.when(core == 1)
    def _():
        env.sent(sums.at[:, :, :LINE - 1], s_ssem.at[0])
        for st in range(AXES):
            env.sent(v_some(st), v_ssem.at[st])
        env.sent(dall.at[:, rows:], x_ssem.at[3])
        env.sent(vall, x_ssem.at[4])
        env.drain()


def solution(mesh):
    proto_size = mesh.shape['proto']
    data_size = mesh.shape['data']

    def local_step(emb_one, emb_two, protos):
        rows, dim = emb_one.shape
        cols = protos.shape[0]
        total_rows = rows * data_size
        total_protos = cols * proto_size
        mine = rows // proto_size
        vm = pl.BlockSpec(memory_space=pltpu.VMEM)
        hbm = pl.BlockSpec(memory_space=pltpu.HBM)
        free = pl.BlockSpec(memory_space=pl.ANY)
        nsem = (ITERS + 1) * AXES
        dma = lambda n: pltpu.SemaphoreType.DMA((n,))
        grid3 = (LINE,) * AXES
        packed = (2 * mine * dim // LANES, LANES)
        sds = jax.ShapeDtypeStruct
        code = sds((rows, cols), F32)
        zbuf = pltpu.VMEM((rows, dim), BF16)
        square = pltpu.VMEM((cols, dim), F32)
        rowbuf = pltpu.VMEM((proto_size, 2 * mine, cols), F32)
        small = pltpu.VMEM((ITERS, 4, LANES), F32)
        spread = pltpu.VMEM((2, cols, LANES), F32)
        args = [pltpu.with_memory_space_constraint(a, pltpu.HBM) for a in (emb_one, emb_two, protos)]
        code1, code2, loss, gall, gp = pl.pallas_call(
            functools.partial(step_kernel, total_rows, total_protos),
            out_shape=(code, code, sds((1, 1), F32),
                       sds(grid3 + packed, F32), sds((cols, dim), F32)),
            in_specs=[hbm] * 3,
            out_specs=(free, free, vm, free, free),
            scratch_shapes=[
                zbuf, zbuf, zbuf, zbuf, pltpu.VMEM((cols, dim), BF16),
                pltpu.VMEM((2, cols, rows), F32),
                pltpu.VMEM((2, cols // 8, 8, total_rows), F32),
                pltpu.VMEM(grid3 + (cols, dim), BF16),
                rowbuf, rowbuf,
                pltpu.VMEM(grid3 + (4, LANES), F32),
                pltpu.VMEM((2 * mine, dim), BF16),
                pltpu.VMEM((4, total_rows), F32),
                spread, spread,
                pltpu.VMEM((2, 8, total_rows), F32),
                pltpu.VMEM((ITERS, 4, total_rows), F32),
                small, small,
                pltpu.VMEM((ITERS + 1, AXES, LINE, 2, total_rows), F32),
                pltpu.VMEM((AXES, LINE, 8, LANES), F32),
                pltpu.VMEM((2, 8, LANES), F32),
                square, square,
                pltpu.VMEM(packed, F32),
                pltpu.VMEM((2, rows, cols), F32),
                dma(4), dma(1), dma(1), dma(1), dma(nsem),
                dma(5), dma(AG_SEMS), dma(1), dma(1),
                dma(AXES), dma(AXES), dma(5), dma(5),
                dma(5), dma(5), dma(4),
            ],
            compiler_params=pltpu.CompilerParams(collective_id=0, has_side_effects=True,
                                                 vmem_limit_bytes=44 * 2 ** 20),
        )(*args)
        blocked = sds((proto_size, mine, dim), F32)
        o1, o2, g1, g2, og = pl.pallas_call(
            functools.partial(write_kernel, mine),
            out_shape=(code, code, blocked, blocked, sds((cols, dim), F32)),
            in_specs=[vm] * 4,
            out_specs=(hbm,) * 5,
            scratch_shapes=[dma(9)],
            compiler_params=pltpu.CompilerParams(vmem_limit_bytes=2 ** 20),
        )(code1, code2, gall.reshape((proto_size,) + packed), gp)
        return o1, o2, loss[0, 0], g1.reshape(rows, dim), g2.reshape(rows, dim), og

    return jax.shard_map(
        local_step, mesh=mesh,
        in_specs=(P('data', None), P('data', None), P('proto', None)),
        out_specs=(P('data', 'proto'), P('data', 'proto'), P(), P('data', None), P('data', None), P('proto', None)),
        check_vma=False)
```

```python
import functools
import re

import jax
import jax.numpy as jnp
from jax import lax
from jax.experimental import pallas as pl
from jax.experimental.pallas import tpu as pltpu
from jax.sharding import PartitionSpec as P

TEMP_TAU = 0.1
ITERS = 3
LINE = 4
AXES = 3
MESH = pl.DeviceIdType.MESH
F32 = jnp.float32
BF16 = jnp.bfloat16
LANES = 128
SUM_CUTS = (0, 1408, 2816, 4096)
C_CUTS = (0, 80, 160, 256)
G_CUTS = ((0, 40, 88, 128), (0, 40, 80, 128))
AG_SEMS = 27
DISTS = (2, 1, 3)
WAYS = (1, 3)


def _nt(a, b):
    return lax.dot_general(a, b, (((1,), (1,)), ((), ())), preferred_element_type=F32)


def _nn(a, b):
    return jnp.dot(a, b, preferred_element_type=F32)


def _col_to_row(s):
    r = lax.broadcasted_iota(jnp.int32, (LANES, LANES), 0)
    c = lax.broadcasted_iota(jnp.int32, (LANES, LANES), 1)
    return jnp.sum(jnp.where(r == c, s, 0.0), axis=0, keepdims=True)


def _row_to_col(row, n=LANES, shift=0):
    r = lax.broadcasted_iota(jnp.int32, (n, LANES), 0)
    c = lax.broadcasted_iota(jnp.int32, (n, LANES), 1)
    return jnp.sum(jnp.where(c == r + shift, row, 0.0), axis=1, keepdims=True)


def _parts(cuts):
    return tuple(zip(cuts[:-1], cuts[1:]))


class _Env:
    def __init__(self):
        self.me = lax.axis_index('proto')
        self.core = lax.axis_index('data')
        me = self.me
        self.pos = [lax.rem(me, LINE), lax.rem(lax.div(me, LINE), LINE), lax.div(me, LINE * LINE)]
        self.stride = [1, LINE, LINE * LINE]
        self.pending = []
        self.partner = (me, 1 - self.core)

    def p(self, axis, d):
        return self.pos[axis] if isinstance(d, int) and d == 0 else lax.rem(self.pos[axis] + d, LINE)

    def peer(self, axis, d):
        return (self.me + (self.p(axis, d) - self.pos[axis]) * self.stride[axis], self.core)

    def remote(self, src, dst, ss, rs, dev):
        cp = pltpu.make_async_remote_copy(src, dst, ss, rs, device_id=dev, device_id_type=MESH)
        cp.start()
        return cp

    def sent(self, ref, ss):
        self.pending.append(pltpu.make_async_remote_copy(ref, ref, ss, ss, device_id=self.partner,
                                                         device_id_type=MESH))

    def arrived(self, ref, rs):
        pltpu.make_async_remote_copy(ref, ref, rs, rs, device_id=self.partner, device_id_type=MESH).wait_recv()

    def drain(self):
        for cp in self.pending:
            cp.wait_send()
        self.pending.clear()


class _Gather:
    def __init__(self, env, buf, cuts, ssem, rsem, twin=None, rows=None):
        self.env, self.buf, self.parts = env, buf, _parts(cuts)
        self.ssem, self.rsem, self.twin, self.rows = ssem, rsem, twin, rows

    def at(self, j, i0, i1, i2):
        ids = [None] * AXES
        for axis, i in zip((j, j + 1, j + 2), (i0, i1, i2)):
            ids[axis % AXES] = slice(None) if i is None else i
        r0, r1 = self.parts[j]
        return self.buf.at[ids[2], ids[1], ids[0], r0:r1, :]

    def p(self, j, level, d):
        return self.env.p((j + level) % AXES, d)

    def send(self, j, group, k, ref, level, d, src=None):
        self.env.remote(ref if src is None else src, ref, self.ssem.at[group], self.rsem.at[k],
                        self.env.peer((j + level) % AXES, d))

    def some(self, blocks):
        for level in range(AXES):
            width = LINE ** level
            if blocks <= width * (LINE - 1):
                lead = (0,) * (AXES - 1 - level)
                return self.buf.at[lead + (pl.ds(0, blocks // width),)]

    def recv(self, k, blocks):
        self.env.arrived(self.some(blocks), self.rsem.at[k])

    def all_sent(self):
        for group, blocks in enumerate((3, 8, 4, 32, 16)):
            self.env.sent(self.some(blocks), self.ssem.at[group])

    def s1_send(self, src=None):
        for d in DISTS:
            for j, (r0, r1) in enumerate(self.parts):
                ref = self.at(j, self.p(j, 0, 0), self.p(j, 1, 0), self.p(j, 2, 0))
                self.send(j, 0, d - 1, ref, 0, d, None if src is None else src.at[r0:r1, :])

    def s1_recv(self):
        for d in DISTS:
            self.recv(d - 1, 1)

    def chunk(self, j, level, k, m):
        if level == 1:
            return self.at(j, self.p(j, 0, k), self.p(j, 1, m), self.p(j, 2, 0))
        return self.at(j, None, self.p(j, 1, k), self.p(j, 2, m))

    def slot(self, level, k, d):
        return 12 * level - 9 + k + LINE * (d // 2)

    def a_send(self, level, k):
        for j in range(AXES):
            ref = self.chunk(j, level, k, 0)
            for d in WAYS:
                self.send(j, 2 * level - 1, self.slot(level, k, d), ref, level, d)

    def way(self, k):
        return 1 if k < 2 else 3

    def f_recv(self, level, k):
        self.recv(self.slot(level, k, self.way(k)), LINE ** (level - 1))

    def g_recv(self, level, k):
        self.recv(self.slot(level, k, LINE - self.way(k)), LINE ** (level - 1))

    def piece_send(self, *offsets):
        for k in offsets:
            for j in range(AXES):
                ref = self.chunk(j, 1, k, 0)
                for d in WAYS:
                    self.send(j, 3, self.slot(2, 0, d), ref, 2, d)

    def own_piece(self):
        self.piece_send(0)

    def other_pieces(self):
        self.piece_send(1, 3, 2)

    def b_send(self, level, k):
        d = self.way(k)
        for j in range(AXES):
            self.send(j, 2 * level, self.slot(level, k, 5), self.chunk(j, level, k, LINE - d), level, d)

    def b_recv(self, level, k):
        self.recv(self.slot(level, k, 5), LINE ** (level - 1))

    def t_send(self, k, m):
        ts, tr = self.twin
        for j in range(AXES):
            ref = self.chunk(j, 2, k, m)
            i = (k == 2) + (m == 2)
            self.env.remote(ref, ref, ts.at[0], tr.at[i], self.env.partner)

    def t_recv(self, group):
        part = (self.buf.at[:3, :3], self.buf.at[:3, :2], self.buf.at[0, 0])[group]
        self.env.arrived(part, self.twin[1].at[group])

    def run(self, ops):
        for op in re.findall('[a-zA-Z][0-9]*', ops):
            args = [int(c) for c in op[1:]]
            {'S': self.s1_send, 's': self.s1_recv, 'A': self.a_send, 'f': self.f_recv, 'g': self.g_recv,
             'B': self.b_send, 'b': self.b_recv, 'T': self.t_send, 'R': self.rows, 'U': self.t_recv, 'P': self.own_piece, 'Q': self.other_pieces}[op[0]](*args)


def write_kernel(mine, code1, code2, gfull, gp, o1, o2, g1, g2, og, sem):
    half = code1.shape[0] // 2
    pairs = [(gp, og)]
    for h in range(2):
        for src, dst in ((code1, o1), (code2, o2)):
            pairs.append((src.at[h * half:(h + 1) * half, :], dst.at[h * half:(h + 1) * half, :]))
        for view, dst in enumerate((g1, g2)):
            r = (2 * h + view) * mine
            pairs.append((gfull.at[:, r:r + mine, :], dst.at[:, :, h * LANES:(h + 1) * LANES]))
    copies = [pltpu.make_async_copy(src, dst, sem.at[i]) for i, (src, dst) in enumerate(pairs)]
    for cp in copies:
        cp.start()
    for cp in copies:
        cp.wait()


def step_kernel(total_rows, total_protos, z1h, z2h, ch,
                code1, code2, loss_out, gfull, gp_out,
                z1, z2, y1, y2, c_ref, f_scr, e_scr, cfull, lrow, frow, vall, zr, dall,
                cacc, vb, ub, stage, csend, crecv, sums, lossb, losst, dacc, drecv, dz, cst, vsrc,
                lsem, c_ssem, c_rsem, s_ssem, s_rsem, a_ssem, a_rsem, t_ssem, t_rsem,
                v_ssem, v_rsem, g_ssem, g_rsem, l_ssem, l_rsem, x_ssem, x_rsem, o_sem):
    env = _Env()
    me, core, pos, partner = env.me, env.core, env.pos, env.partner
    remote = env.remote
    rows, cols = z1.shape[0], c_ref.shape[0]
    both = zr.shape[0]
    mine = both // 2
    blocks = LINE ** AXES
    fscale = 1.0 / (2 * total_rows * TEMP_TAU)
    zs, ys = (z1, z2), (y1, y2)
    chunks, groups = rows // cols, cols // 8

    barrier = pltpu.get_barrier_semaphore()
    pl.semaphore_signal(barrier, inc=1, device_id=partner, device_id_type=MESH)
    for axis in range(AXES):
        for d in DISTS:
            pl.semaphore_signal(barrier, inc=1, device_id=env.peer(axis, d), device_id_type=MESH)
    loads = [pltpu.make_async_copy(src, dst, lsem.at[i]) for i, (src, dst) in enumerate(
        ((ch, c_ref), (z1h, z1), (z2h, z2), (ch, cfull.at[pos[2], pos[1], pos[0]])))]
    gg = [_Gather(env, gfull, cuts, g_ssem, g_rsem) for cuts in G_CUTS]

    def by_core(fn):
        for c in range(2):
            pl.when(core == c)(functools.partial(fn, c))

    def grun(ops):
        by_core(lambda c: gg[c].run(ops))

    for cp in loads[:3]:
        cp.start()

    def scores(view):
        cacc[view] = jnp.zeros((cols, LANES), F32)

        def body(i, _):
            n0 = pl.multiple_of(i * cols, cols)
            s = _nt(c_ref[...], zs[view][pl.ds(n0, cols), :])
            f = jnp.exp(s * (1.0 / TEMP_TAU))
            stage[0, 2 + view:3 + view, pl.ds(n0, cols)] = jnp.sum(f, axis=0, keepdims=True)
            e = f * f
            f_scr[view, :, pl.ds(n0, cols)] = f
            e_scr[view, :, :, pl.ds(n0, cols)] = e.reshape(groups, 8, cols)
            cacc[view] += e[:, :LANES] + e[:, LANES:]
            return 0
        lax.fori_loop(0, chunks, body, 0, unroll=8)
        zr[view * mine:(view + 1) * mine, :] = zs[view][pl.ds(pl.multiple_of(me * mine, mine), mine), :]

    def other_scores(view):
        def body(i, _):
            n0 = pl.multiple_of(i * cols, cols)
            f = jnp.exp(_nt(c_ref[...], ys[view][pl.ds(n0, cols), :]) * (1.0 / TEMP_TAU))
            e_scr[view, :, :, pl.ds(rows + n0, cols)] = (f * f).reshape(groups, 8, cols)
            return 0
        lax.fori_loop(0, chunks, body, 0, unroll=2)

    def score_block(offsets):
        z_, y_, x_ = (env.p(axis, d) for axis, d in zip((2, 1, 0), offsets))
        q = (z_ * LINE + y_) * LINE + x_
        l = _nt(zr[...], cfull[z_, y_, x_]) * (1.0 / TEMP_TAU)
        lrow[q] = l
        frow[q] = jnp.exp(l)

    def near(i):
        return i + lax.div(i, 2)

    def row_scores(piece):
        def spot(axis, d, rest):
            rest = list(rest)
            rest.insert(axis, d)
            score_block(rest)

        def body(i, _):
            a, b = near(lax.div(i, 3)), near(lax.rem(i, 3))
            if piece < 3:
                spot(0, near(jnp.int32(piece)), (a, b))
            elif piece < 6:
                spot(piece - 3, 2, (a, b))
            return 0

        def last(i, _):
            for axis in range(AXES):
                spot(axis, near(i), (2, 2))
            return 0
        if piece < 6:
            lax.fori_loop(0, 9, body, 0, unroll=True)
        else:
            lax.fori_loop(0, 3, last, 0, unroll=True)
            score_block((2, 2, 2))

    gc = _Gather(env, cfull, C_CUTS, a_ssem, a_rsem, (t_ssem, t_rsem), row_scores)

    def block(q):
        return lax.div(q, LINE * LINE), lax.rem(lax.div(q, LINE), LINE), lax.rem(q, LINE)

    def column_sums(it):
        for view in range(2):
            for h in range(2):
                k = 2 * view + h
                s = jnp.sum(cacc[view, h * LANES:(h + 1) * LANES, :], axis=1, keepdims=True)
                csend[it, k:k + 1, :] = _col_to_row(s)

    def spread(vrow):
        for view in range(2):
            for h in range(2):
                k = 2 * view + h
                vb[view, h * LANES:(h + 1) * LANES, :] = jnp.broadcast_to(
                    _row_to_col(vrow[k:k + 1, :]), (LANES, LANES))

    def exchange():
        return remote(csend.at[0], crecv.at[0], c_ssem.at[0], c_rsem.at[0], partner)

    def row_sums(it, width):
        tiles = [slice(l, l + LANES) for l in range(0, width, LANES)]
        for view in range(2):
            def body(g, acc, view=view):
                w = vb[view, pl.ds(pl.multiple_of(g * 8, 8), 8), :]
                return tuple(a + e_scr[view, g, :, ls] * w for a, ls in zip(acc, tiles))
            acc = lax.fori_loop(0, groups, body, tuple(jnp.zeros((8, LANES), F32) for _ in tiles), unroll=4)
            for a, ls in zip(acc, tiles):
                stage[it, view:view + 1, ls] = jnp.sum(a, axis=0, keepdims=True)

    def weighted_columns():
        tiles = [slice(l, l + LANES) for l in range(0, 2 * rows, LANES)]
        for view in range(2):
            us = [ub[view, :, ls] for ls in tiles]

            def body(g, _, view=view, us=us):
                terms = [e_scr[view, g, :, ls] * u for ls, u in zip(tiles, us)]
                chains = [sum(terms[t::LINE][1:], terms[t]) for t in range(LINE)]
                cacc[view, pl.ds(pl.multiple_of(g * 8, 8), 8), :] = (chains[0] + chains[1]) + (chains[2] + chains[3])
                return 0
            lax.fori_loop(0, groups, body, 0, unroll=4)

    def at_offset(oz, oy, ox):
        return (env.p(2, oz) * LINE + env.p(1, oy)) * LINE + env.p(0, ox)

    def broadcast_v():
        dst = vall.at[pos[2], pos[1], pos[0]]
        pltpu.make_async_copy(vsrc, dst, v_rsem.at[0]).start()
        order = DISTS + (0,)
        for oz in order:
            for oy in order:
                for ox in order:
                    there = at_offset(oz, oy, ox)
                    remote(vsrc, dst, v_ssem.at[3], v_rsem.at[0], (there, 0))
                    if oz or oy or ox:
                        group = 0 if oz else 1 if oy else 2
                        remote(vsrc, dst, v_ssem.at[group], v_rsem.at[0], (there, 1))

    def load_sums(it, value):
        for j, (l0, l1) in enumerate(_parts(SUM_CUTS)):
            sums[it, 0, pos[j], :, l0:l1] = value[:, l0:l1]

    def send_sums(it, st):
        for d in DISTS:
            for j, (l0, l1) in enumerate(_parts(SUM_CUTS)):
                ax = (st + j) % AXES
                src = sums.at[it, st, pos[ax], :, l0:l1]
                remote(src, src, s_ssem.at[0], s_rsem.at[it * AXES + st], env.peer(ax, d))

    def recv_sums(it, st):
        env.arrived(sums.at[it, st, :LINE - 1], s_rsem.at[it * AXES + st])
        tot = []
        for j, (l0, l1) in enumerate(_parts(SUM_CUTS)):
            s = [sums[it, st, i, :, l0:l1] for i in range(LINE)]
            t = (s[0] + s[1]) + (s[2] + s[3])
            tot.append(t)
            if st < AXES - 1:
                sums[it, st + 1, pos[(st + 1 + j) % AXES], :, l0:l1] = t
        return tot

    def denominators(st):
        if st == 0:
            load_sums(ITERS, stage[0, 2:4])
        else:
            tot = recv_sums(ITERS, st - 1)
        if st < AXES:
            send_sums(ITERS, st)
            return
        for (l0, l1), t in zip(_parts(SUM_CUTS), tot):
            dall[2:4, l0:l1] = t

    def hidden(slot):
        if slot in (1, 2):
            env.arrived(ys[slot - 1], x_rsem.at[slot - 1])
            other_scores(slot - 1)
        if slot in (3, 4, 5, 6):
            denominators(slot - 3)
        if slot == 6:
            gc.run('U0R0R1R2U1R3R4R5U2R6')

    @pl.when(core == 1)
    def _():
        loads[0].wait()
        for view in range(2):
            loads[1 + view].wait()
            scores(view)
        pl.semaphore_wait(barrier, 1 + AXES * (LINE - 1))
        column_sums(0)
        exchange().wait()
        total = csend[0] + crecv[0]
        for it in range(ITERS):
            last = it == ITERS - 1
            vrow = 1.0 / (float(total_protos) * total)
            if last:
                vsrc[...] = vrow
                broadcast_v()
            spread(vrow)
            row_sums(it, rows if it == 0 else 2 * rows)
            if it == 0:
                env.arrived(stage.at[0, :, rows:], x_rsem.at[2])
            load_sums(it, stage[it, 0:2])
            for st in range(AXES):
                send_sums(it, st)
                hidden(it * AXES + st)
                tot = recv_sums(it, st)
                if last:
                    send_sums(it, 1)
                    break
                if st < AXES - 1:
                    continue
                for (l0, l1), t in zip(_parts(SUM_CUTS), tot):
                    u = 1.0 / (float(total_rows) * t)
                    for view in range(2):
                        ub[view, :, l0:l1] = jnp.broadcast_to(u[view:view + 1], (8, l1 - l0))
            if not last:
                weighted_columns()
                column_sums(it + 1)
                total = csend[it + 1]

    @pl.when(core == 0)
    def _():
        loads[3].start()
        loads[0].wait()
        for view in range(2):
            loads[1 + view].wait()
            scores(view)
        column_sums(0)
        loads[3].wait()
        pl.semaphore_wait(barrier, 1 + AXES * (LINE - 1))
        cp = exchange()
        gc.run('SA10P')
        cp.wait()
        vrow = 1.0 / (float(total_protos) * (csend[0] + crecv[0]))
        spread(vrow)
        row_sums(0, rows)
        remote(stage.at[0, :, :rows], stage.at[0, :, rows:], x_ssem.at[2], x_rsem.at[2], partner)
        for i in range(2):
            remote(zs[i], ys[i], x_ssem.at[i], x_rsem.at[i], partner)
        gc.run('sA11A13A12QT00')
        gc.run('f10B10f11B11f13B13f12B12g10g11A21g13g12A23')
        gc.run('f20B20b10b11b13b12A22T10T30T20')
        gc.run('f21B21f23B23g20g21g23T01T03T11T13T31T33R0')
        gc.run('f22B22R1g22T21T23b20T02b21T12R2')
        gc.run('b23T32R3b22T22R4R5R6')
        gc.all_sent()
        for i, ref in enumerate((z1, z2, stage.at[0, :, :rows])):
            env.sent(ref, x_ssem.at[i])
        env.sent(cfull, t_ssem.at[0])
        env.drain()

    env.arrived(vall, v_rsem.at[0])

    def lanes(h):
        return slice(h * LANES, (h + 1) * LANES)

    def table(q):
        return lax.div(q, blocks // 2), pl.ds(pl.multiple_of(lax.rem(q, blocks // 2) * both, both), both)

    def sumbody(q, acc):
        z_, y_, x_ = block(q)
        view, part = table(q)
        for h in range(2):
            f = frow[q, :, lanes(h)]
            v0 = jnp.broadcast_to(vall[z_, y_, x_, h:h + 1, :], (mine, LANES))
            v1 = jnp.broadcast_to(vall[z_, y_, x_, 2 + h:3 + h, :], (mine, LANES))
            t = f * f * jnp.concatenate([v0, v1], axis=0)
            cst[view, part, lanes(h)] = t
            acc = (acc[0] + t, acc[1] + f)
        return acc

    zero = jnp.zeros((both, LANES), F32)
    rsum, den = (jnp.sum(a, axis=1, keepdims=True)
                 for a in lax.fori_loop(0, blocks, sumbody, (zero, zero), unroll=4))
    rc = jnp.broadcast_to(1.0 / rsum, (both, LANES))
    dc = jnp.broadcast_to(1.0 / den, (both, LANES))
    ld = jnp.broadcast_to(jnp.log(den), (both, LANES))

    def other_codes(q, h):
        view, part = table(q)
        code = cst[view, part, lanes(h)] * rc
        return jnp.concatenate([code[mine:], code[:mine]], axis=0)

    def dzbody(i, acc):
        hs = []
        for x_ in range(LINE):
            for h in range(2):
                q = i * LINE + x_
                hs.append(((frow[q, :, lanes(h)] * dc - other_codes(q, h)) * fscale).astype(BF16))
        cl = cfull[lax.div(i, LINE), lax.rem(i, LINE)].reshape(LINE * cols, cols)
        return acc + _nn(jnp.concatenate(hs, axis=1), cl)

    rowgrad = lax.fori_loop(0, LINE * LINE, dzbody, jnp.zeros((both, cols), F32), unroll=4)
    dz[...] = jnp.concatenate([rowgrad[:, :LANES], rowgrad[:, LANES:]], axis=0)

    own = pltpu.make_async_copy(dz, gfull.at[pos[2], pos[1], pos[0]], o_sem.at[0])
    own.start()
    by_core(lambda c: gg[c].s1_send(dz))
    own.wait()
    grun('A10P')

    @pl.when(core == 1)
    def _():
        recv_sums(ITERS - 1, 1)
        send_sums(ITERS - 1, 2)

    spread(vall[pos[2], pos[1], pos[0]])
    dacc[...] = jnp.zeros((cols, cols), F32)

    def out_copy(view, i):
        n0 = pl.multiple_of(i * cols, cols)
        return pltpu.make_async_copy(cst.at[view, pl.ds(n0, cols), :], (code1, code2)[view].at[pl.ds(n0, cols), :],
                                     o_sem.at[2 + view])

    def columns(i):
        def body(i, _):
            n0 = pl.multiple_of(i * cols, cols)
            inv = 1.0 / dall[:, pl.ds(n0, cols)]
            code, prob = [], []
            for view in range(2):
                w = jnp.concatenate([vb[view], vb[view]], axis=1)
                code.append(e_scr[view, :, :, pl.ds(n0, cols)].reshape(cols, cols) * w * inv[view:view + 1, :])
                prob.append(f_scr[view, :, pl.ds(n0, cols)] * inv[2 + view:3 + view, :])
            for view in range(2):
                h = ((prob[view] - code[1 - view]) * fscale).astype(BF16)
                dacc[...] += _nn(h, zs[view][pl.ds(n0, cols), :])
                cst[view, pl.ds(n0, cols), :] = code[view].T
                out_copy(view, i).start()
            return 0
        lax.fori_loop(i * 2, i * 2 + 2, body, 0, unroll=True)

    def lbody(q, acc):
        for h in range(2):
            acc = acc + other_codes(q, h) * (lrow[q, :, lanes(h)] - ld)
        return acc
    part = lax.fori_loop(0, blocks, lbody, jnp.zeros((both, LANES), F32), unroll=4)
    lossb[0, pos[0]] = jnp.sum(part.reshape(both // 8, 8, LANES), axis=0)

    def loss_send(st):
        ref = lossb.at[st, pos[st]]
        for d in DISTS:
            remote(ref, ref, l_ssem.at[st], l_rsem.at[st], env.peer(st, d))
        env.sent(lossb.at[st, :LINE - 1], l_ssem.at[st])

    def loss_recv(st):
        env.arrived(lossb.at[st, :LINE - 1], l_rsem.at[st])
        return (lossb[st, 0] + lossb[st, 1]) + (lossb[st, 2] + lossb[st, 3])

    loss_send(0)
    grun('sA11A13A12Q')

    @pl.when(core == 1)
    def _():
        for (l0, l1), t in zip(_parts(SUM_CUTS), recv_sums(ITERS - 1, AXES - 1)):
            dall[0:2, l0:l1] = t
        remote(dall.at[:, rows:], dall.at[:, :rows], x_ssem.at[3], x_rsem.at[3], partner)

    lossb[1, pos[1]] = loss_recv(0)
    loss_send(1)
    grun('f10B10f11B11f13B13f12B12g10g11A21g13g12A23')
    lossb[2, pos[2]] = loss_recv(1)
    loss_send(2)
    pl.when(core == 0)(lambda: env.arrived(dall.at[:, :rows], x_rsem.at[3]))
    columns(0)
    grun('f20B20b10b11b13b12A22')
    columns(1)
    columns(2)
    grun('f21B21f23B23')
    columns(3)
    dcp = remote(dacc, drecv, l_ssem.at[4], l_rsem.at[4], partner)
    grun('f22B22')
    losst[0] = loss_recv(2)
    lcp = remote(losst.at[0], losst.at[1], l_ssem.at[3], l_rsem.at[3], partner)
    lcp.wait_recv()
    loss_out[...] = jnp.sum(losst[0] + losst[1], keepdims=True) * (-1.0 / (2 * total_rows))
    dcp.wait_recv()
    drecv[...] = dacc[...] + drecv[...]
    gpc = pltpu.make_async_copy(drecv, gp_out, o_sem.at[1])
    gpc.start()
    grun('g20g21g23g22b20b21b23b22')
    gpc.wait()
    for view, out in enumerate((code1, code2)):
        pltpu.make_async_copy(cst.at[view], out, o_sem.at[2 + view]).wait()
    gg[0].all_sent()
    env.sent(losst.at[0], l_ssem.at[3])
    env.sent(dacc, l_ssem.at[4])
    env.drain()

    @pl.when(core == 1)
    def _():
        env.sent(sums.at[:, :, :LINE - 1], s_ssem.at[0])
        for i, ref in enumerate((vall.at[:LINE - 1], vall.at[0, :LINE - 1], vall.at[0, 0, :LINE - 1], vall)):
            env.sent(ref, v_ssem.at[i])
        env.sent(dall.at[:, rows:], x_ssem.at[3])
        env.drain()


def solution(mesh):
    proto_size = mesh.shape['proto']
    data_size = mesh.shape['data']

    def local_step(emb_one, emb_two, protos):
        rows, dim = emb_one.shape
        cols = protos.shape[0]
        total_rows = rows * data_size
        total_protos = cols * proto_size
        mine = rows // proto_size
        vm = pl.BlockSpec(memory_space=pltpu.VMEM)
        hbm = pl.BlockSpec(memory_space=pltpu.HBM)
        free = pl.BlockSpec(memory_space=pl.ANY)
        nsem = (ITERS + 1) * AXES
        dma = lambda n: pltpu.SemaphoreType.DMA((n,))
        one, few, many = dma(1), dma(5), dma(AG_SEMS)
        pair = 2 * mine
        grid3 = (LINE,) * AXES
        packed = (pair * dim // LANES, LANES)
        sds = jax.ShapeDtypeStruct
        code = sds((rows, cols), F32)
        zbuf = pltpu.VMEM((rows, dim), BF16)
        square = pltpu.VMEM((cols, dim), F32)
        rowbuf = pltpu.VMEM((proto_size, pair, cols), F32)
        small = pltpu.VMEM((ITERS, 4, LANES), F32)
        spread = pltpu.VMEM((2, cols, LANES), F32)
        args = [pltpu.with_memory_space_constraint(a, pltpu.HBM) for a in (emb_one, emb_two, protos)]
        code1, code2, loss, gall, gp = pl.pallas_call(
            functools.partial(step_kernel, total_rows, total_protos),
            out_shape=(code, code, sds((1, 1), F32),
                       sds(grid3 + packed, F32), sds((cols, dim), F32)),
            in_specs=[hbm] * 3,
            out_specs=(free, free, vm, free, free),
            scratch_shapes=[
                zbuf, zbuf, zbuf, zbuf, pltpu.VMEM((cols, dim), BF16),
                pltpu.VMEM((2, cols, rows), F32),
                pltpu.VMEM((2, cols // 8, 8, total_rows), F32),
                pltpu.VMEM(grid3 + (cols, dim), BF16),
                rowbuf, rowbuf,
                pltpu.VMEM(grid3 + (4, LANES), F32),
                pltpu.VMEM((pair, dim), BF16),
                pltpu.VMEM((4, total_rows), F32),
                spread, spread,
                pltpu.VMEM((2, 8, total_rows), F32),
                pltpu.VMEM((ITERS, 4, total_rows), F32),
                small, small,
                pltpu.VMEM((ITERS + 1, AXES, LINE, 2, total_rows), F32),
                pltpu.VMEM((AXES, LINE, 8, LANES), F32),
                pltpu.VMEM((2, 8, LANES), F32),
                square, square,
                pltpu.VMEM(packed, F32),
                pltpu.VMEM((2, rows, cols), F32),
                pltpu.VMEM((4, LANES), F32),
                few, one, one, one, dma(nsem),
                few, many, one, few, few, one, few, many, few, few, few, few, few,
            ],
            compiler_params=pltpu.CompilerParams(collective_id=0, has_side_effects=True,
                                                 vmem_limit_bytes=44 * 2 ** 20),
        )(*args)
        blocked = sds((proto_size, mine, dim), F32)
        o1, o2, g1, g2, og = pl.pallas_call(
            functools.partial(write_kernel, mine),
            out_shape=(code, code, blocked, blocked, sds((cols, dim), F32)),
            in_specs=[vm] * 4,
            out_specs=(hbm,) * 5,
            scratch_shapes=[dma(9)],
            compiler_params=pltpu.CompilerParams(vmem_limit_bytes=2 ** 20),
        )(code1, code2, gall.reshape((proto_size,) + packed), gp)
        return o1, o2, loss[0, 0], g1.reshape(rows, dim), g2.reshape(rows, dim), og

    return jax.shard_map(
        local_step, mesh=mesh,
        in_specs=(P('data', None), P('data', None), P('proto', None)),
        out_specs=(P('data', 'proto'), P('data', 'proto'), P(), P('data', None), P('data', None), P('proto', None)),
        check_vma=False)
```

```python
import functools
import re

import jax
import jax.numpy as jnp
from jax import lax
from jax.experimental import pallas as pl
from jax.experimental.pallas import tpu as pltpu
from jax.sharding import PartitionSpec as P

TEMP_TAU = 0.1
ITERS = 3
LINE = 4
AXES = 3
MESH = pl.DeviceIdType.MESH
F32 = jnp.float32
BF16 = jnp.bfloat16
LANES = 128
VIEWS = (0, 1)
SCALE = 1.0 / TEMP_TAU
SUM_CUTS = (0, 1408, 2816, 4096)
C_CUTS = (0, 88, 168, 256)
G_CUTS = ((0, 40, 88, 128), (0, 40, 80, 128))
AG_SEMS = 27
DISTS = (2, 1, 3)
WAYS = (1, 3)


def _nt(a, b):
    return lax.dot_general(a, b, (((1,), (1,)), ((), ())), preferred_element_type=F32)


def _nn(a, b):
    return jnp.dot(a, b, preferred_element_type=F32)


def _col_to_row(s):
    r = lax.broadcasted_iota(jnp.int32, (LANES, LANES), 0)
    c = lax.broadcasted_iota(jnp.int32, (LANES, LANES), 1)
    return jnp.sum(jnp.where(r == c, s, 0.0), axis=0, keepdims=True)


def _row_to_col(row, n=LANES, shift=0):
    r = lax.broadcasted_iota(jnp.int32, (n, LANES), 0)
    c = lax.broadcasted_iota(jnp.int32, (n, LANES), 1)
    return jnp.sum(jnp.where(c == r + shift, row, 0.0), axis=1, keepdims=True)


def _parts(cuts):
    return tuple(zip(cuts[:-1], cuts[1:]))


class _Env:
    def __init__(self):
        self.me = lax.axis_index('proto')
        self.core = lax.axis_index('data')
        me = self.me
        self.pos = [lax.rem(me, LINE), lax.rem(lax.div(me, LINE), LINE), lax.div(me, LINE * LINE)]
        self.stride = [1, LINE, LINE * LINE]
        self.pending = []
        self.partner = (me, 1 - self.core)

    def p(self, axis, d):
        return self.pos[axis] if isinstance(d, int) and d == 0 else lax.rem(self.pos[axis] + d, LINE)

    def peer(self, axis, d):
        return (self.me + (self.p(axis, d) - self.pos[axis]) * self.stride[axis], self.core)

    def remote(self, src, dst, ss, rs, dev):
        cp = pltpu.make_async_remote_copy(src, dst, ss, rs, device_id=dev, device_id_type=MESH)
        cp.start()
        return cp

    def sent(self, ref, ss):
        self.pending.append(pltpu.make_async_remote_copy(ref, ref, ss, ss, device_id=self.partner,
                                                         device_id_type=MESH))

    def arrived(self, ref, rs):
        pltpu.make_async_remote_copy(ref, ref, rs, rs, device_id=self.partner, device_id_type=MESH).wait_recv()

    def drain(self):
        for cp in self.pending:
            cp.wait_send()
        self.pending.clear()


class _Gather:
    def __init__(self, env, buf, cuts, ssem, rsem, twin=None, rows=None):
        self.env, self.buf, self.parts = env, buf, _parts(cuts)
        self.ssem, self.rsem, self.twin, self.rows = ssem, rsem, twin, rows

    def at(self, j, i0, i1, i2):
        ids = [None] * AXES
        for axis, i in zip((j, j + 1, j + 2), (i0, i1, i2)):
            ids[axis % AXES] = slice(None) if i is None else i
        r0, r1 = self.parts[j]
        return self.buf.at[ids[2], ids[1], ids[0], r0:r1, :]

    def p(self, j, level, d):
        return self.env.p((j + level) % AXES, d)

    def send(self, j, group, k, ref, level, d, src=None):
        self.env.remote(ref if src is None else src, ref, self.ssem.at[group], self.rsem.at[k],
                        self.env.peer((j + level) % AXES, d))

    def some(self, blocks):
        for level in range(AXES):
            width = LINE ** level
            if blocks <= width * (LINE - 1):
                lead = (0,) * (AXES - 1 - level)
                return self.buf.at[lead + (pl.ds(0, blocks // width),)]

    def recv(self, k, blocks):
        self.env.arrived(self.some(blocks), self.rsem.at[k])

    def all_sent(self):
        for group, blocks in enumerate((3, 8, 4, 32, 16)):
            self.env.sent(self.some(blocks), self.ssem.at[group])

    def s1_send(self, src=None):
        for d in DISTS:
            for j, (r0, r1) in enumerate(self.parts):
                ref = self.at(j, self.p(j, 0, 0), self.p(j, 1, 0), self.p(j, 2, 0))
                self.send(j, 0, d - 1, ref, 0, d, None if src is None else src.at[r0:r1, :])

    def s1_recv(self):
        for d in DISTS:
            self.recv(d - 1, 1)

    def chunk(self, j, level, k, m):
        if level == 1:
            return self.at(j, self.p(j, 0, k), self.p(j, 1, m), self.p(j, 2, 0))
        return self.at(j, None, self.p(j, 1, k), self.p(j, 2, m))

    def slot(self, level, k, d):
        return 12 * level - 9 + k + LINE * (d // 2)

    def a_send(self, level, k):
        for j in range(AXES):
            ref = self.chunk(j, level, k, 0)
            for d in WAYS:
                self.send(j, 2 * level - 1, self.slot(level, k, d), ref, level, d)

    def way(self, k):
        return 1 if k < 2 else 3

    def f_recv(self, level, k):
        self.recv(self.slot(level, k, self.way(k)), LINE ** (level - 1))

    def g_recv(self, level, k):
        self.recv(self.slot(level, k, LINE - self.way(k)), LINE ** (level - 1))

    def piece_send(self, *offsets):
        for k in offsets:
            for j in range(AXES):
                ref = self.chunk(j, 1, k, 0)
                for d in WAYS:
                    self.send(j, 3, self.slot(2, 0, d), ref, 2, d)

    def own_piece(self):
        self.piece_send(0)

    def other_pieces(self):
        self.piece_send(1, 3, 2)

    def b_send(self, level, k):
        d = self.way(k)
        for j in range(AXES):
            self.send(j, 2 * level, self.slot(level, k, 5), self.chunk(j, level, k, LINE - d), level, d)

    def b_recv(self, level, k):
        self.recv(self.slot(level, k, 5), LINE ** (level - 1))

    def t_send(self, k, m):
        ts, tr = self.twin
        for j in range(AXES):
            ref = self.chunk(j, 2, k, m)
            i = (k == 2) + (m == 2)
            self.env.remote(ref, ref, ts.at[0], tr.at[i], self.env.partner)

    def t_recv(self, group):
        part = (self.buf.at[:3, :3], self.buf.at[:3, :2], self.buf.at[0, 0])[group]
        self.env.arrived(part, self.twin[1].at[group])

    def run(self, ops):
        for op in re.findall('[a-zA-Z][0-9]*', ops):
            args = [int(c) for c in op[1:]]
            {'S': self.s1_send, 's': self.s1_recv, 'A': self.a_send, 'f': self.f_recv, 'g': self.g_recv,
             'B': self.b_send, 'b': self.b_recv, 'T': self.t_send, 'R': self.rows, 'U': self.t_recv, 'P': self.own_piece, 'Q': self.other_pieces}[op[0]](*args)


def write_kernel(mine, code1, code2, gfull, gp, o1, o2, g1, g2, og, sem):
    half = code1.shape[0] // 2
    pairs = [(gp, og)]
    for h in VIEWS:
        for src, dst in ((code1, o1), (code2, o2)):
            pairs.append((src.at[h * half:(h + 1) * half, :], dst.at[h * half:(h + 1) * half, :]))
        for view, dst in enumerate((g1, g2)):
            r = (2 * h + view) * mine
            pairs.append((gfull.at[:, r:r + mine, :], dst.at[:, :, h * LANES:(h + 1) * LANES]))
    copies = [pltpu.make_async_copy(src, dst, sem.at[i]) for i, (src, dst) in enumerate(pairs)]
    for cp in copies:
        cp.start()
    for cp in copies:
        cp.wait()


def step_kernel(total_rows, total_protos, z1h, z2h, ch,
                code1, code2, loss_out, gfull, gp_out,
                z1, z2, y1, y2, c_ref, f_scr, e_scr, cfull, lrow, frow, vall, zr, dall,
                cacc, vb, ub, stage, csend, crecv, sums, lossb, losst, dacc, drecv, dz, cst, vsrc,
                lsem, c_ssem, c_rsem, s_ssem, a_ssem, a_rsem, t_ssem, t_rsem,
                v_ssem, v_rsem, g_ssem, g_rsem, l_ssem, l_rsem, x_ssem, x_rsem, o_sem):
    env = _Env()
    me, core, pos, partner = env.me, env.core, env.pos, env.partner
    remote = env.remote
    rows, cols = z1.shape[0], c_ref.shape[0]
    both = zr.shape[0]
    mine = both // 2
    blocks = LINE ** AXES
    fscale = 1.0 / (2 * total_rows * TEMP_TAU)
    zs, ys = (z1, z2), (y1, y2)
    chunks, groups = rows // cols, cols // 8

    loads = [pltpu.make_async_copy(src, dst, lsem.at[i]) for i, (src, dst) in enumerate(
        ((ch, c_ref), (z1h, z1), (z2h, z2), (ch, cfull.at[pos[2], pos[1], pos[0]])))]
    gg = [_Gather(env, gfull, cuts, g_ssem, g_rsem) for cuts in G_CUTS]

    def by_core(fn):
        for c in VIEWS:
            pl.when(core == c)(functools.partial(fn, c))

    def grun(ops):
        by_core(lambda c: gg[c].run(ops))

    for cp in loads[:3]:
        cp.start()
    barrier = pltpu.get_barrier_semaphore()
    pl.semaphore_signal(barrier, inc=1, device_id=partner, device_id_type=MESH)
    for axis in range(AXES):
        for d in DISTS:
            pl.semaphore_signal(barrier, inc=1, device_id=env.peer(axis, d), device_id_type=MESH)

    def scores(view):
        cacc[view] = jnp.zeros((cols, LANES), F32)

        def body(i, _):
            n0 = pl.multiple_of(i * cols, cols)
            s = _nt(c_ref[...], zs[view][pl.ds(n0, cols), :])
            f = jnp.exp(s * SCALE)
            stage[0, 2 + view:3 + view, pl.ds(n0, cols)] = jnp.sum(f, axis=0, keepdims=True)
            e = f * f
            f_scr[view, :, pl.ds(n0, cols)] = f
            e_scr[view, :, :, pl.ds(n0, cols)] = e.reshape(groups, 8, cols)
            cacc[view] += e[:, :LANES] + e[:, LANES:]
            return 0
        lax.fori_loop(0, chunks, body, 0, unroll=8)
        zr[view * mine:(view + 1) * mine, :] = zs[view][pl.ds(pl.multiple_of(me * mine, mine), mine), :]

    def other_scores(view):
        def body(i, _):
            n0 = pl.multiple_of(i * cols, cols)
            f = jnp.exp(_nt(c_ref[...], ys[view][pl.ds(n0, cols), :]) * SCALE)
            e_scr[view, :, :, pl.ds(rows + n0, cols)] = (f * f).reshape(groups, 8, cols)
            return 0
        lax.fori_loop(0, chunks, body, 0, unroll=2)

    def score_block(offsets):
        z_, y_, x_ = (env.p(axis, d) for axis, d in zip((2, 1, 0), offsets))
        q = (z_ * LINE + y_) * LINE + x_
        l = _nt(zr[...], cfull[z_, y_, x_]) * SCALE
        lrow[q] = l
        frow[q] = jnp.exp(l)

    def near(i):
        return i + lax.div(i, 2)

    def row_scores(piece):
        def spot(axis, d, rest):
            rest = list(rest)
            rest.insert(axis, d)
            score_block(rest)

        def body(i, _):
            a, b = near(lax.div(i, 3)), near(lax.rem(i, 3))
            if piece < 3:
                spot(0, near(jnp.int32(piece)), (a, b))
            elif piece < 6:
                spot(piece - 3, 2, (a, b))
            return 0

        def last(i, _):
            for axis in range(AXES):
                spot(axis, near(i), (2, 2))
            return 0
        if piece < 6:
            lax.fori_loop(0, 9, body, 0, unroll=True)
        else:
            lax.fori_loop(0, 3, last, 0, unroll=True)
            score_block((2, 2, 2))

    gc = _Gather(env, cfull, C_CUTS, a_ssem, a_rsem, (t_ssem, t_rsem), row_scores)

    def block(q):
        return lax.div(q, LINE * LINE), lax.rem(lax.div(q, LINE), LINE), lax.rem(q, LINE)

    def column_sums(it):
        for view in VIEWS:
            for h in VIEWS:
                k = 2 * view + h
                s = jnp.sum(cacc[view, h * LANES:(h + 1) * LANES, :], axis=1, keepdims=True)
                csend[it, k:k + 1, :] = _col_to_row(s)

    def spread(vrow):
        for view in VIEWS:
            for h in VIEWS:
                k = 2 * view + h
                vb[view, h * LANES:(h + 1) * LANES, :] = jnp.broadcast_to(
                    _row_to_col(vrow[k:k + 1, :]), (LANES, LANES))

    def exchange():
        return remote(csend.at[0], crecv.at[0], c_ssem.at[0], c_rsem.at[0], partner)

    def row_sums(it, width):
        tiles = [slice(l, l + LANES) for l in range(0, width, LANES)]
        for view in VIEWS:
            def body(g, acc, view=view):
                w = vb[view, pl.ds(pl.multiple_of(g * 8, 8), 8), :]
                return tuple(a + e_scr[view, g, :, ls] * w for a, ls in zip(acc, tiles))
            acc = lax.fori_loop(0, groups, body, tuple(jnp.zeros((8, LANES), F32) for _ in tiles), unroll=4)
            for a, ls in zip(acc, tiles):
                stage[it, view:view + 1, ls] = jnp.sum(a, axis=0, keepdims=True)

    def weighted_columns():
        tiles = [slice(l, l + LANES) for l in range(0, 2 * rows, LANES)]
        for view in VIEWS:
            us = [ub[view, :, ls] for ls in tiles]

            def body(g, _, view=view, us=us):
                terms = [e_scr[view, g, :, ls] * u for ls, u in zip(tiles, us)]
                chains = [sum(terms[t::LINE][1:], terms[t]) for t in range(LINE)]
                cacc[view, pl.ds(pl.multiple_of(g * 8, 8), 8), :] = (chains[0] + chains[1]) + (chains[2] + chains[3])
                return 0
            lax.fori_loop(0, groups, body, 0, unroll=4)

    def at_offset(oz, oy, ox):
        return (env.p(2, oz) * LINE + env.p(1, oy)) * LINE + env.p(0, ox)

    def broadcast_v():
        dst = vall.at[pos[2], pos[1], pos[0]]
        pltpu.make_async_copy(vsrc, dst, v_rsem.at[0]).start()
        order = DISTS + (0,)
        for oz in order:
            for oy in order:
                for ox in order:
                    there = at_offset(oz, oy, ox)
                    remote(vsrc, dst, v_ssem.at[3], v_rsem.at[0], (there, 0))
                    if oz or oy or ox:
                        group = 0 if oz else 1 if oy else 2
                        remote(vsrc, dst, v_ssem.at[group], v_rsem.at[0], (there, 1))

    def within(lo, hi):
        return [(j, max(l0, lo), min(l1, hi)) for j, (l0, l1) in enumerate(_parts(SUM_CUTS)) if l0 < hi and l1 > lo]

    def load_sums(it, part, hi):
        for j, l0, l1 in within(0, hi):
            sums[it, 0, pos[j], :, l0:l1] = stage[part + (slice(l0, l1),)]

    def send_sums(it, st):
        for d in DISTS:
            for j, l0, l1 in within(0, rows if it + st == 0 else total_rows):
                ax = (st + j) % AXES
                src = sums.at[it, st, pos[ax], :, l0:l1]
                remote(src, src, s_ssem.at[2 if it else min(st, 1)], a_rsem.at[it * AXES + st], env.peer(ax, d))

    def send_first():
        for d in DISTS + (0,):
            for j, l0, l1 in within(rows, total_rows):
                src = sums.at[0, 0, pos[j], :, l0:l1]
                if d:
                    remote(src, src, x_ssem.at[3], a_rsem.at[0], (env.peer(j, d)[0], 1))
                else:
                    remote(src, src, x_ssem.at[3], x_rsem.at[3], partner)

    def recv_sums(it, st):
        if it + st == 0:
            env.arrived(sums.at[0, 0, 0, :, rows:], x_rsem.at[3])
        env.arrived(sums.at[it, st, :LINE - 1], a_rsem.at[it * AXES + st])
        tot = []
        for j, (l0, l1) in enumerate(_parts(SUM_CUTS)):
            s = [sums[it, st, i, :, l0:l1] for i in range(LINE)]
            t = (s[0] + s[1]) + (s[2] + s[3])
            tot.append(t)
            if st < AXES - 1:
                sums[it, st + 1, pos[(st + 1 + j) % AXES], :, l0:l1] = t
        return tot

    def denominators(st):
        if st == 0:
            env.arrived(stage.at[0, :, rows:], x_rsem.at[2])
            load_sums(ITERS, (0, slice(2, 4)), total_rows)
        else:
            tot = recv_sums(ITERS, st - 1)
        if st < AXES:
            send_sums(ITERS, st)
            return
        for (l0, l1), t in zip(_parts(SUM_CUTS), tot):
            dall[2:4, l0:l1] = t

    def hidden(slot):
        if slot in (1, 2):
            env.arrived(ys[slot - 1], x_rsem.at[slot - 1])
            other_scores(slot - 1)
        if slot in (3, 4, 5, 6):
            denominators(slot - 3)
        if slot == 6:
            gc.run('U0R0R1R2U1R3R4R5U2R6')

    @pl.when(core == 1)
    def _():
        loads[0].wait()
        for view in VIEWS:
            loads[1 + view].wait()
            scores(view)
        pl.semaphore_wait(barrier, 1 + AXES * (LINE - 1))
        column_sums(0)
        exchange().wait()
        total = csend[0] + crecv[0]
        for it in range(ITERS):
            last = it == ITERS - 1
            vrow = 1.0 / (float(total_protos) * total)
            if last:
                vsrc[...] = vrow
                broadcast_v()
            spread(vrow)
            row_sums(it, rows if it == 0 else 2 * rows)
            load_sums(it, (it, slice(0, 2)), rows if it == 0 else total_rows)
            for st in range(AXES):
                send_sums(it, st)
                hidden(it * AXES + st)
                tot = recv_sums(it, st)
                if last:
                    send_sums(it, 1)
                    break
                if st < AXES - 1:
                    continue
                for (l0, l1), t in zip(_parts(SUM_CUTS), tot):
                    u = 1.0 / (float(total_rows) * t)
                    for view in VIEWS:
                        ub[view, :, l0:l1] = jnp.broadcast_to(u[view:view + 1], (8, l1 - l0))
            if not last:
                weighted_columns()
                column_sums(it + 1)
                total = csend[it + 1]

    @pl.when(core == 0)
    def _():
        loads[3].start()
        loads[0].wait()
        for view in VIEWS:
            loads[1 + view].wait()
            scores(view)
        column_sums(0)
        loads[3].wait()
        pl.semaphore_wait(barrier, 1 + AXES * (LINE - 1))
        cp = exchange()
        gc.run('S')
        cp.wait()
        vrow = 1.0 / (float(total_protos) * (csend[0] + crecv[0]))
        spread(vrow)
        row_sums(0, rows)
        for j, l0, l1 in within(rows, total_rows):
            sums[0, 0, pos[j], :, l0:l1] = stage[0, 0:2, l0 - rows:l1 - rows]
        send_first()
        gc.run('A10P')
        remote(stage.at[0, :, :rows], stage.at[0, :, rows:], x_ssem.at[2], x_rsem.at[2], partner)
        for i in VIEWS:
            remote(zs[i], ys[i], x_ssem.at[i], x_rsem.at[i], partner)
        gc.run('sA11A13A12QT00')
        gc.run('f10B10f11B11f13B13f12B12g10g11A21g13g12A23')
        gc.run('f20B20b10b11b13b12A22T10T30T20')
        gc.run('f21B21f23B23g20g21g23T01T03T11T13T31T33R0')
        gc.run('f22B22R1g22T21T23b20T02b21T12R2')
        gc.run('b23T32R3b22T22R4R5R6')
        gc.all_sent()
        for i, ref in enumerate((z1, z2, stage.at[0, :, :rows], sums.at[0, 0, :2])):
            env.sent(ref, x_ssem.at[i])
        env.sent(cfull, t_ssem.at[0])
        env.drain()

    env.arrived(vall, v_rsem.at[0])

    def lanes(h):
        return slice(h * LANES, (h + 1) * LANES)

    def table(q):
        return lax.div(q, blocks // 2), pl.ds(pl.multiple_of(lax.rem(q, blocks // 2) * both, both), both)

    def sumbody(q, acc):
        z_, y_, x_ = block(q)
        view, part = table(q)
        for h in VIEWS:
            f = frow[q, :, lanes(h)]
            v0 = jnp.broadcast_to(vall[z_, y_, x_, h:h + 1, :], (mine, LANES))
            v1 = jnp.broadcast_to(vall[z_, y_, x_, 2 + h:3 + h, :], (mine, LANES))
            t = f * f * jnp.concatenate([v0, v1], axis=0)
            cst[view, part, lanes(h)] = t
            acc = (acc[0] + t, acc[1] + f)
        return acc

    zero = jnp.zeros((both, LANES), F32)
    rsum, den = (jnp.sum(a, axis=1, keepdims=True)
                 for a in lax.fori_loop(0, blocks, sumbody, (zero, zero), unroll=4))
    rc = jnp.broadcast_to(1.0 / rsum, (both, LANES))
    dc = jnp.broadcast_to(1.0 / den, (both, LANES))
    ld = jnp.broadcast_to(jnp.log(den), (both, LANES))

    def other_codes(q, h):
        view, part = table(q)
        code = cst[view, part, lanes(h)] * rc
        return jnp.concatenate([code[mine:], code[:mine]], axis=0)

    def dzbody(i, acc):
        hs = []
        for x_ in range(LINE):
            for h in VIEWS:
                q = i * LINE + x_
                hs.append(((frow[q, :, lanes(h)] * dc - other_codes(q, h)) * fscale).astype(BF16))
        cl = cfull[lax.div(i, LINE), lax.rem(i, LINE)].reshape(LINE * cols, cols)
        return acc + _nn(jnp.concatenate(hs, axis=1), cl)

    rowgrad = lax.fori_loop(0, LINE * LINE, dzbody, jnp.zeros((both, cols), F32), unroll=4)
    dz[...] = jnp.concatenate([rowgrad[:, :LANES], rowgrad[:, LANES:]], axis=0)

    own = pltpu.make_async_copy(dz, gfull.at[pos[2], pos[1], pos[0]], o_sem.at[0])
    own.start()
    by_core(lambda c: gg[c].s1_send(dz))
    own.wait()

    @pl.when(core == 1)
    def _():
        recv_sums(ITERS - 1, 1)
        send_sums(ITERS - 1, 2)

    spread(vall[pos[2], pos[1], pos[0]])
    dacc[...] = jnp.zeros((cols, cols), F32)

    def out_copy(view, i):
        n0 = pl.multiple_of(i * cols, cols)
        return pltpu.make_async_copy(cst.at[view, pl.ds(n0, cols), :], (code1, code2)[view].at[pl.ds(n0, cols), :],
                                     o_sem.at[2 + view])

    def columns(i):
        def body(i, _):
            n0 = pl.multiple_of(i * cols, cols)
            inv = 1.0 / dall[:, pl.ds(n0, cols)]
            code, prob = [], []
            for view in VIEWS:
                w = jnp.concatenate([vb[view], vb[view]], axis=1)
                code.append(e_scr[view, :, :, pl.ds(n0, cols)].reshape(cols, cols) * w * inv[view:view + 1, :])
                prob.append(f_scr[view, :, pl.ds(n0, cols)] * inv[2 + view:3 + view, :])
            for view in VIEWS:
                h = ((prob[view] - code[1 - view]) * fscale).astype(BF16)
                dacc[...] += _nn(h, zs[view][pl.ds(n0, cols), :])
                cst[view, pl.ds(n0, cols), :] = code[view].T
                out_copy(view, i).start()
            return 0
        lax.fori_loop(i * 2, i * 2 + 2, body, 0, unroll=True)

    def lbody(q, acc):
        for h in VIEWS:
            acc = acc + other_codes(q, h) * (lrow[q, :, lanes(h)] - ld)
        return acc
    part = lax.fori_loop(0, blocks, lbody, jnp.zeros((both, LANES), F32), unroll=4)
    grun('A10P')
    lossb[0, pos[0]] = jnp.sum(part.reshape(both // 8, 8, LANES), axis=0)

    def loss_send(st):
        ref = lossb.at[st, pos[st]]
        for d in DISTS:
            remote(ref, ref, l_ssem.at[st], l_rsem.at[st], env.peer(st, d))
        env.sent(lossb.at[st, :LINE - 1], l_ssem.at[st])

    def loss_recv(st):
        env.arrived(lossb.at[st, :LINE - 1], l_rsem.at[st])
        return (lossb[st, 0] + lossb[st, 1]) + (lossb[st, 2] + lossb[st, 3])

    loss_send(0)
    grun('sA11A13A12f10B10Q')

    @pl.when(core == 1)
    def _():
        for (l0, l1), t in zip(_parts(SUM_CUTS), recv_sums(ITERS - 1, AXES - 1)):
            dall[0:2, l0:l1] = t
        remote(dall.at[:, rows:], dall.at[:, :rows], x_ssem.at[3], x_rsem.at[4], partner)

    lossb[1, pos[1]] = loss_recv(0)
    loss_send(1)
    grun('f11B11f13B13f12B12g10g11A21g13g12A23')
    lossb[2, pos[2]] = loss_recv(1)
    loss_send(2)
    pl.when(core == 0)(lambda: env.arrived(dall.at[:, :rows], x_rsem.at[4]))
    columns(0)
    grun('f20B20b10b11b13b12A22')
    columns(1)
    columns(2)
    grun('f21B21f23B23')
    columns(3)
    dcp = remote(dacc, drecv, l_ssem.at[4], l_rsem.at[4], partner)
    grun('f22B22')
    losst[0] = loss_recv(2)
    lcp = remote(losst.at[0], losst.at[1], l_ssem.at[3], l_rsem.at[3], partner)
    lcp.wait_recv()
    loss_out[...] = jnp.sum(losst[0] + losst[1], keepdims=True) * (-1.0 / (2 * total_rows))
    dcp.wait_recv()
    drecv[...] = dacc[...] + drecv[...]
    gpc = pltpu.make_async_copy(drecv, gp_out, o_sem.at[1])
    gpc.start()
    grun('g20g21g23g22b20b21b23b22')
    gpc.wait()
    for view, out in enumerate((code1, code2)):
        pltpu.make_async_copy(cst.at[view], out, o_sem.at[2 + view]).wait()
    gg[0].all_sent()
    env.sent(losst.at[0], l_ssem.at[3])
    env.sent(dacc, l_ssem.at[4])
    env.drain()

    @pl.when(core == 1)
    def _():
        for i, ref in enumerate((sums.at[0, 0, :AXES, :, :rows], sums.at[0, 1:, :AXES], sums.at[1:, :, :AXES])):
            env.sent(ref, s_ssem.at[i])
        for i, ref in enumerate((vall.at[:LINE - 1], vall.at[0, :LINE - 1], vall.at[0, 0, :LINE - 1], vall)):
            env.sent(ref, v_ssem.at[i])
        env.sent(dall.at[:, rows:], x_ssem.at[3])
        env.drain()


def solution(mesh):
    proto_size = mesh.shape['proto']
    data_size = mesh.shape['data']

    def local_step(emb_one, emb_two, protos):
        rows, dim = emb_one.shape
        cols = protos.shape[0]
        total_rows = rows * data_size
        total_protos = cols * proto_size
        mine = rows // proto_size
        vm = pl.BlockSpec(memory_space=pltpu.VMEM)
        hbm = pl.BlockSpec(memory_space=pltpu.HBM)
        free = pl.BlockSpec(memory_space=pl.ANY)
        dma = lambda n: pltpu.SemaphoreType.DMA((n,))
        one, few, many = dma(1), dma(5), dma(AG_SEMS)
        pair = 2 * mine
        grid3 = (LINE,) * AXES
        packed = (pair * dim // LANES, LANES)
        sds = jax.ShapeDtypeStruct
        code = sds((rows, cols), F32)
        zbuf = pltpu.VMEM((rows, dim), BF16)
        square = pltpu.VMEM((cols, dim), F32)
        rowbuf = pltpu.VMEM((proto_size, pair, cols), F32)
        small = pltpu.VMEM((ITERS, 4, LANES), F32)
        spread = pltpu.VMEM((2, cols, LANES), F32)
        args = [pltpu.with_memory_space_constraint(a, pltpu.HBM) for a in (emb_one, emb_two, protos)]
        code1, code2, loss, gall, gp = pl.pallas_call(
            functools.partial(step_kernel, total_rows, total_protos),
            out_shape=(code, code, sds((1, 1), F32),
                       sds(grid3 + packed, F32), sds((cols, dim), F32)),
            in_specs=[hbm] * 3,
            out_specs=(free, free, vm, free, free),
            scratch_shapes=[
                zbuf, zbuf, zbuf, zbuf, pltpu.VMEM((cols, dim), BF16),
                pltpu.VMEM((2, cols, rows), F32),
                pltpu.VMEM((2, cols // 8, 8, total_rows), F32),
                pltpu.VMEM(grid3 + (cols, dim), BF16),
                rowbuf, rowbuf,
                pltpu.VMEM(grid3 + (4, LANES), F32),
                pltpu.VMEM((pair, dim), BF16),
                pltpu.VMEM((4, total_rows), F32),
                spread, spread,
                pltpu.VMEM((2, 8, total_rows), F32),
                pltpu.VMEM((ITERS, 4, total_rows), F32),
                small, small,
                pltpu.VMEM((ITERS + 1, AXES, LINE, 2, total_rows), F32),
                pltpu.VMEM((AXES, LINE, 8, LANES), F32),
                pltpu.VMEM((2, 8, LANES), F32),
                square, square,
                pltpu.VMEM(packed, F32),
                pltpu.VMEM((2, rows, cols), F32),
                pltpu.VMEM((4, LANES), F32),
                few, one, one, few,
                few, many, one, few, few, one, few, many, few, few, few, few, few,
            ],
            compiler_params=pltpu.CompilerParams(collective_id=0, has_side_effects=True,
                                                 vmem_limit_bytes=44 * 2 ** 20),
        )(*args)
        blocked = sds((proto_size, mine, dim), F32)
        o1, o2, g1, g2, og = pl.pallas_call(
            functools.partial(write_kernel, mine),
            out_shape=(code, code, blocked, blocked, sds((cols, dim), F32)),
            in_specs=[vm] * 4,
            out_specs=(hbm,) * 5,
            scratch_shapes=[dma(9)],
            compiler_params=pltpu.CompilerParams(vmem_limit_bytes=2 ** 20),
        )(code1, code2, gall.reshape((proto_size,) + packed), gp)
        return o1, o2, loss[0, 0], g1.reshape(rows, dim), g2.reshape(rows, dim), og

    return jax.shard_map(
        local_step, mesh=mesh,
        in_specs=(P('data', None), P('data', None), P('proto', None)),
        out_specs=(P('data', 'proto'), P('data', 'proto'), P(), P('data', None), P('data', None), P('proto', None)),
        check_vma=False)
```

```python
import functools
import re

import jax
import jax.numpy as jnp
from jax import lax
from jax.experimental import pallas as pl
from jax.experimental.pallas import tpu as pltpu
from jax.sharding import PartitionSpec as P

TEMP_TAU = 0.1
ITERS = 3
LINE = 4
AXES = 3
MESH = pl.DeviceIdType.MESH
F32 = jnp.float32
BF16 = jnp.bfloat16
LANES = 128
VIEWS = (0, 1)
SCALE = 1.0 / TEMP_TAU
SUM_CUTS = (0, 1408, 2816, 4096)
C_CUTS = (0, 88, 168, 256)
G_CUTS = ((0, 40, 88, 128), (0, 40, 80, 128))
AG_SEMS = 25
DISTS = (2, 1, 3)
WAYS = (1, 3)


def _nt(a, b):
    return lax.dot_general(a, b, (((1,), (1,)), ((), ())), preferred_element_type=F32)


def _nn(a, b):
    return jnp.dot(a, b, preferred_element_type=F32)


def _col_to_row(s):
    r = lax.broadcasted_iota(jnp.int32, (LANES, LANES), 0)
    c = lax.broadcasted_iota(jnp.int32, (LANES, LANES), 1)
    return jnp.sum(jnp.where(r == c, s, 0.0), axis=0, keepdims=True)


def _row_to_col(row, n=LANES, shift=0):
    r = lax.broadcasted_iota(jnp.int32, (n, LANES), 0)
    c = lax.broadcasted_iota(jnp.int32, (n, LANES), 1)
    return jnp.sum(jnp.where(c == r + shift, row, 0.0), axis=1, keepdims=True)


def _parts(cuts):
    return tuple(zip(cuts[:-1], cuts[1:]))


class _Env:
    def __init__(self):
        self.me = lax.axis_index('proto')
        self.core = lax.axis_index('data')
        me = self.me
        self.pos = [lax.rem(me, LINE), lax.rem(lax.div(me, LINE), LINE), lax.div(me, LINE * LINE)]
        self.stride = [1, LINE, LINE * LINE]
        self.pending = []
        self.partner = (me, 1 - self.core)

    def p(self, axis, d):
        return self.pos[axis] if isinstance(d, int) and d == 0 else lax.rem(self.pos[axis] + d, LINE)

    def peer(self, axis, d):
        return (self.me + (self.p(axis, d) - self.pos[axis]) * self.stride[axis], self.core)

    def remote(self, src, dst, ss, rs, dev):
        cp = pltpu.make_async_remote_copy(src, dst, ss, rs, device_id=dev, device_id_type=MESH)
        cp.start()
        return cp

    def sent(self, ref, ss):
        self.pending.append(pltpu.make_async_remote_copy(ref, ref, ss, ss, device_id=self.partner,
                                                         device_id_type=MESH))

    def arrived(self, ref, rs):
        pltpu.make_async_remote_copy(ref, ref, rs, rs, device_id=self.partner, device_id_type=MESH).wait_recv()

    def drain(self):
        for cp in self.pending:
            cp.wait_send()
        self.pending.clear()


class _Gather:
    def __init__(self, env, buf, cuts, ssem, rsem, twin=None, rows=None):
        self.env, self.buf, self.parts = env, buf, _parts(cuts)
        self.ssem, self.rsem, self.twin, self.rows = ssem, rsem, twin, rows

    def at(self, j, i0, i1, i2):
        ids = [None] * AXES
        for axis, i in zip((j, j + 1, j + 2), (i0, i1, i2)):
            ids[axis % AXES] = slice(None) if i is None else i
        r0, r1 = self.parts[j]
        return self.buf.at[ids[2], ids[1], ids[0], r0:r1, :]

    def p(self, j, level, d):
        return self.env.p((j + level) % AXES, d)

    def send(self, j, group, k, ref, level, d, src=None):
        self.env.remote(ref if src is None else src, ref, self.ssem.at[group], self.rsem.at[k],
                        self.env.peer((j + level) % AXES, d))

    def some(self, blocks):
        for level in range(AXES):
            width = LINE ** level
            if blocks <= width * (LINE - 1):
                lead = (0,) * (AXES - 1 - level)
                return self.buf.at[lead + (pl.ds(0, blocks // width),)]

    def recv(self, k, blocks):
        self.env.arrived(self.some(blocks), self.rsem.at[k])

    def all_sent(self):
        for group, blocks in enumerate((3, 8, 4, 32, 16)):
            self.env.sent(self.some(blocks), self.ssem.at[group])

    def s1_send(self, src=None):
        for d in DISTS:
            for j, (r0, r1) in enumerate(self.parts):
                ref = self.at(j, self.p(j, 0, 0), self.p(j, 1, 0), self.p(j, 2, 0))
                self.send(j, 0, 0, ref, 0, d, None if src is None else src.at[r0:r1, :])

    def s1_recv(self):
        self.recv(0, 3)

    def chunk(self, j, level, k, m):
        if level == 1:
            return self.at(j, self.p(j, 0, k), self.p(j, 1, m), self.p(j, 2, 0))
        return self.at(j, None, self.p(j, 1, k), self.p(j, 2, m))

    def slot(self, level, k, d):
        return 1 + 12 * (level - 1) + k + LINE * (d // 2)

    def a_send(self, level, k):
        for j in range(AXES):
            ref = self.chunk(j, level, k, 0)
            for d in WAYS:
                self.send(j, 2 * level - 1, self.slot(level, k, d), ref, level, d)

    def way(self, k):
        return 1 if k < 2 else 3

    def f_recv(self, level, k):
        self.recv(self.slot(level, k, self.way(k)), LINE ** (level - 1))

    def g_recv(self, level, k):
        self.recv(self.slot(level, k, LINE - self.way(k)), LINE ** (level - 1))

    def piece_send(self, *offsets):
        for k in offsets:
            for j in range(AXES):
                ref = self.chunk(j, 1, k, 0)
                for d in WAYS:
                    self.send(j, 3, self.slot(2, 0, d), ref, 2, d)

    def own_piece(self):
        self.piece_send(0)

    def other_pieces(self):
        self.piece_send(1, 3, 2)

    def b_send(self, level, k):
        d = self.way(k)
        for j in range(AXES):
            self.send(j, 2 * level, self.slot(level, k, 5), self.chunk(j, level, k, LINE - d), level, d)

    def b_recv(self, level, k):
        self.recv(self.slot(level, k, 5), LINE ** (level - 1))

    def t_send(self, k, m):
        ts, tr = self.twin
        for j in range(AXES):
            ref = self.chunk(j, 2, k, m)
            i = (k == 2) + (m == 2)
            self.env.remote(ref, ref, ts.at[0], tr.at[i], self.env.partner)

    def t_recv(self, group):
        part = (self.buf.at[:3, :3], self.buf.at[:3, :2], self.buf.at[0, 0])[group]
        self.env.arrived(part, self.twin[1].at[group])

    def run(self, ops):
        for op in re.findall('[a-zA-Z][0-9]*', ops):
            args = [int(c) for c in op[1:]]
            {'S': self.s1_send, 's': self.s1_recv, 'A': self.a_send, 'f': self.f_recv, 'g': self.g_recv,
             'B': self.b_send, 'b': self.b_recv, 'T': self.t_send, 'R': self.rows, 'U': self.t_recv, 'P': self.own_piece, 'Q': self.other_pieces}[op[0]](*args)


def write_kernel(mine, code1, code2, gfull, gp, o1, o2, g1, g2, og, sem):
    half = code1.shape[0] // 2
    pairs = [(gp, og)]
    for h in VIEWS:
        for src, dst in ((code1, o1), (code2, o2)):
            pairs.append((src.at[h * half:(h + 1) * half, :], dst.at[h * half:(h + 1) * half, :]))
        for view, dst in enumerate((g1, g2)):
            r = (2 * h + view) * mine
            pairs.append((gfull.at[:, r:r + mine, :], dst.at[:, :, h * LANES:(h + 1) * LANES]))
    copies = [pltpu.make_async_copy(src, dst, sem.at[i]) for i, (src, dst) in enumerate(pairs)]
    for cp in copies:
        cp.start()
    for cp in copies:
        cp.wait()


def step_kernel(total_rows, total_protos, z1h, z2h, ch,
                code1, code2, loss_out, gfull, gp_out,
                z1, z2, y1, y2, c_ref, f_scr, e_scr, cfull, lrow, frow, vall, zr, dall,
                cacc, vb, ub, stage, csend, crecv, sums, lossb, losst, dacc, drecv, dz, cst, vsrc,
                lsem, c_ssem, c_rsem, s_ssem, a_ssem, a_rsem, t_ssem, t_rsem,
                v_ssem, v_rsem, g_ssem, g_rsem, l_ssem, l_rsem, x_ssem, x_rsem, o_sem):
    env = _Env()
    me, core, pos, partner = env.me, env.core, env.pos, env.partner
    remote = env.remote
    rows, cols = z1.shape[0], c_ref.shape[0]
    both = zr.shape[0]
    mine = both // 2
    blocks = LINE ** AXES
    fscale = 1.0 / (2 * total_rows * TEMP_TAU)
    zs, ys = (z1, z2), (y1, y2)
    chunks, groups = rows // cols, cols // 8

    loads = [pltpu.make_async_copy(src, dst, lsem.at[i]) for i, (src, dst) in enumerate(
        ((ch, c_ref), (z1h, z1), (z2h, z2), (ch, cfull.at[pos[2], pos[1], pos[0]])))]
    gg = [_Gather(env, gfull, cuts, g_ssem, g_rsem) for cuts in G_CUTS]

    def by_core(fn):
        for c in VIEWS:
            pl.when(core == c)(functools.partial(fn, c))

    def grun(ops):
        by_core(lambda c: gg[c].run(ops))

    for cp in loads[:3]:
        cp.start()
    barrier = pltpu.get_barrier_semaphore()
    pl.semaphore_signal(barrier, inc=1, device_id=partner, device_id_type=MESH)
    for axis in range(AXES):
        for d in DISTS:
            pl.semaphore_signal(barrier, inc=1, device_id=env.peer(axis, d), device_id_type=MESH)

    def scores(view):
        cacc[view] = jnp.zeros((cols, LANES), F32)

        def body(i, _):
            n0 = pl.multiple_of(i * cols, cols)
            s = _nt(c_ref[...], zs[view][pl.ds(n0, cols), :])
            f = jnp.exp(s * SCALE)
            stage[0, 2 + view:3 + view, pl.ds(n0, cols)] = jnp.sum(f, axis=0, keepdims=True)
            e = f * f
            f_scr[view, :, pl.ds(n0, cols)] = f
            e_scr[view, :, :, pl.ds(n0, cols)] = e.reshape(groups, 8, cols)
            cacc[view] += e[:, :LANES] + e[:, LANES:]
            return 0
        lax.fori_loop(0, chunks, body, 0, unroll=8)
        zr[view * mine:(view + 1) * mine, :] = zs[view][pl.ds(pl.multiple_of(me * mine, mine), mine), :]

    def other_scores(view):
        def body(i, _):
            n0 = pl.multiple_of(i * cols, cols)
            f = jnp.exp(_nt(c_ref[...], ys[view][pl.ds(n0, cols), :]) * SCALE)
            e_scr[view, :, :, pl.ds(rows + n0, cols)] = (f * f).reshape(groups, 8, cols)
            return 0
        lax.fori_loop(0, chunks, body, 0, unroll=2)

    def score_block(offsets):
        z_, y_, x_ = (env.p(axis, d) for axis, d in zip((2, 1, 0), offsets))
        q = (z_ * LINE + y_) * LINE + x_
        l = _nt(zr[...], cfull[z_, y_, x_]) * SCALE
        lrow[q] = l
        frow[q] = jnp.exp(l)

    def near(i):
        return i + lax.div(i, 2)

    def row_scores(piece):
        def spot(axis, d, rest):
            rest = list(rest)
            rest.insert(axis, d)
            score_block(rest)

        def body(i, _):
            a, b = near(lax.div(i, 3)), near(lax.rem(i, 3))
            if piece < 3:
                spot(0, near(jnp.int32(piece)), (a, b))
            elif piece < 6:
                spot(piece - 3, 2, (a, b))
            return 0

        def last(i, _):
            for axis in range(AXES):
                spot(axis, near(i), (2, 2))
            return 0
        if piece < 6:
            lax.fori_loop(0, 9, body, 0, unroll=True)
        else:
            lax.fori_loop(0, 3, last, 0, unroll=True)
            score_block((2, 2, 2))

    gc = _Gather(env, cfull, C_CUTS, a_ssem, a_rsem, (t_ssem, t_rsem), row_scores)

    def block(q):
        return lax.div(q, LINE * LINE), lax.rem(lax.div(q, LINE), LINE), lax.rem(q, LINE)

    def column_sums(it):
        for view in VIEWS:
            for h in VIEWS:
                k = 2 * view + h
                s = jnp.sum(cacc[view, h * LANES:(h + 1) * LANES, :], axis=1, keepdims=True)
                csend[it, k:k + 1, :] = _col_to_row(s)

    def spread(vrow):
        for view in VIEWS:
            for h in VIEWS:
                k = 2 * view + h
                vb[view, h * LANES:(h + 1) * LANES, :] = jnp.broadcast_to(
                    _row_to_col(vrow[k:k + 1, :]), (LANES, LANES))

    def exchange():
        return remote(csend.at[0], crecv.at[0], c_ssem.at[0], c_rsem.at[0], partner)

    def row_sums(it, width):
        tiles = [slice(l, l + LANES) for l in range(0, width, LANES)]
        for view in VIEWS:
            def body(g, acc, view=view):
                w = vb[view, pl.ds(pl.multiple_of(g * 8, 8), 8), :]
                return tuple(a + e_scr[view, g, :, ls] * w for a, ls in zip(acc, tiles))
            acc = lax.fori_loop(0, groups, body, tuple(jnp.zeros((8, LANES), F32) for _ in tiles), unroll=8)
            for a, ls in zip(acc, tiles):
                stage[it, view:view + 1, ls] = jnp.sum(a, axis=0, keepdims=True)

    def weighted_columns():
        tiles = [slice(l, l + LANES) for l in range(0, 2 * rows, LANES)]
        for view in VIEWS:
            us = [ub[view, :, ls] for ls in tiles]

            def body(g, _, view=view, us=us):
                terms = [e_scr[view, g, :, ls] * u for ls, u in zip(tiles, us)]
                chains = [sum(terms[t::LINE][1:], terms[t]) for t in range(LINE)]
                cacc[view, pl.ds(pl.multiple_of(g * 8, 8), 8), :] = (chains[0] + chains[1]) + (chains[2] + chains[3])
                return 0
            lax.fori_loop(0, groups, body, 0, unroll=8)

    def at_offset(oz, oy, ox):
        return (env.p(2, oz) * LINE + env.p(1, oy)) * LINE + env.p(0, ox)

    def broadcast_v():
        dst = vall.at[pos[2], pos[1], pos[0]]
        pltpu.make_async_copy(vsrc, dst, v_rsem.at[0]).start()
        order = DISTS + (0,)
        for oz in order:
            for oy in order:
                for ox in order:
                    there = at_offset(oz, oy, ox)
                    if oz or oy or ox:
                        group = 0 if oz else 1 if oy else 2
                        remote(vsrc, dst, v_ssem.at[group], v_rsem.at[0], (there, 1))
                    remote(vsrc, dst, v_ssem.at[3], v_rsem.at[0], (there, 0))

    def within(lo, hi):
        return [(j, max(l0, lo), min(l1, hi)) for j, (l0, l1) in enumerate(_parts(SUM_CUTS)) if l0 < hi and l1 > lo]

    def load_sums(it, part, hi):
        for j, l0, l1 in within(0, hi):
            sums[it, 0, pos[j], :, l0:l1] = stage[part + (slice(l0, l1),)]

    def send_sums(it, st):
        for d in DISTS:
            for j, l0, l1 in within(0, rows if it + st == 0 else total_rows):
                ax = (st + j) % AXES
                src = sums.at[it, st, pos[ax], :, l0:l1]
                remote(src, src, s_ssem.at[2 if it else min(st, 1)], a_rsem.at[it * AXES + st], env.peer(ax, d))

    def send_first():
        for d in DISTS + (0,):
            for j, l0, l1 in within(rows, total_rows):
                src = sums.at[0, 0, pos[j], :, l0:l1]
                if d:
                    remote(src, src, x_ssem.at[3], a_rsem.at[0], (env.peer(j, d)[0], 1))
                else:
                    remote(src, src, x_ssem.at[3], x_rsem.at[3], partner)

    def recv_sums(it, st):
        if it + st == 0:
            env.arrived(sums.at[0, 0, 0, :, rows:], x_rsem.at[3])
        env.arrived(sums.at[it, st, :LINE - 1], a_rsem.at[it * AXES + st])
        tot = []
        for j, (l0, l1) in enumerate(_parts(SUM_CUTS)):
            s = [sums[it, st, i, :, l0:l1] for i in range(LINE)]
            t = (s[0] + s[1]) + (s[2] + s[3])
            tot.append(t)
            if st < AXES - 1:
                sums[it, st + 1, pos[(st + 1 + j) % AXES], :, l0:l1] = t
        return tot

    def denominators(st):
        if st == 0:
            env.arrived(stage.at[0, :, rows:], x_rsem.at[2])
            load_sums(ITERS, (0, slice(2, 4)), total_rows)
        else:
            tot = recv_sums(ITERS, st - 1)
        if st < AXES:
            send_sums(ITERS, st)
            return
        for (l0, l1), t in zip(_parts(SUM_CUTS), tot):
            dall[2:4, l0:l1] = t

    def hidden(slot):
        if slot in (1, 2):
            env.arrived(ys[slot - 1], x_rsem.at[slot - 1])
            other_scores(slot - 1)
        if slot == 6:
            denominators(0)
            gc.run('U0R0R1R2U1R3R4R5U2R6')

    @pl.when(core == 1)
    def _():
        loads[0].wait()
        for view in VIEWS:
            loads[1 + view].wait()
            scores(view)
        pl.semaphore_wait(barrier, 1 + AXES * (LINE - 1))
        column_sums(0)
        exchange().wait()
        total = csend[0] + crecv[0]
        for it in range(ITERS):
            last = it == ITERS - 1
            vrow = 1.0 / (float(total_protos) * total)
            if last:
                vsrc[...] = vrow
                broadcast_v()
            spread(vrow)
            row_sums(it, rows if it == 0 else 2 * rows)
            load_sums(it, (it, slice(0, 2)), rows if it == 0 else total_rows)
            for st in range(AXES):
                send_sums(it, st)
                hidden(it * AXES + st)
                tot = recv_sums(it, st)
                if last:
                    send_sums(it, 1)
                    denominators(1)
                    break
                if st < AXES - 1:
                    continue
                for (l0, l1), t in zip(_parts(SUM_CUTS), tot):
                    u = 1.0 / (float(total_rows) * t)
                    for view in VIEWS:
                        ub[view, :, l0:l1] = jnp.broadcast_to(u[view:view + 1], (8, l1 - l0))
            if not last:
                weighted_columns()
                column_sums(it + 1)
                total = csend[it + 1]

    @pl.when(core == 0)
    def _():
        loads[3].start()
        loads[0].wait()
        for view in VIEWS:
            loads[1 + view].wait()
            scores(view)
        column_sums(0)
        loads[3].wait()
        pl.semaphore_wait(barrier, 1 + AXES * (LINE - 1))
        cp = exchange()
        gc.run('S')
        cp.wait()
        vrow = 1.0 / (float(total_protos) * (csend[0] + crecv[0]))
        spread(vrow)
        row_sums(0, rows)
        for j, l0, l1 in within(rows, total_rows):
            sums[0, 0, pos[j], :, l0:l1] = stage[0, 0:2, l0 - rows:l1 - rows]
        send_first()
        gc.run('A10P')
        remote(stage.at[0, :, :rows], stage.at[0, :, rows:], x_ssem.at[2], x_rsem.at[2], partner)
        for i in VIEWS:
            remote(zs[i], ys[i], x_ssem.at[i], x_rsem.at[i], partner)
        gc.run('sA11A13A12QT00')
        gc.run('f10B10f11B11f13B13f12B12g10g11A21g13g12A23')
        gc.run('f20B20b10b11b13b12A22T10T30T20')
        gc.run('f21B21f23B23g20g21g23T01T03T11T13T31T33R0')
        gc.run('f22B22R1g22T21T23b20T02b21T12R2')
        gc.run('b23T32R3b22T22R4R5R6')
        gc.all_sent()
        for i, ref in enumerate((z1, z2, stage.at[0, :, :rows], sums.at[0, 0, :2])):
            env.sent(ref, x_ssem.at[i])
        env.sent(cfull, t_ssem.at[0])
        env.drain()

    env.arrived(vall, v_rsem.at[0])

    def lanes(h):
        return slice(h * LANES, (h + 1) * LANES)

    def table(q):
        return lax.div(q, blocks // 2), pl.ds(pl.multiple_of(lax.rem(q, blocks // 2) * both, both), both)

    def sumbody(q, acc):
        z_, y_, x_ = block(q)
        view, part = table(q)
        for h in VIEWS:
            f = frow[q, :, lanes(h)]
            v0 = jnp.broadcast_to(vall[z_, y_, x_, h:h + 1, :], (mine, LANES))
            v1 = jnp.broadcast_to(vall[z_, y_, x_, 2 + h:3 + h, :], (mine, LANES))
            t = f * f * jnp.concatenate([v0, v1], axis=0)
            cst[view, part, lanes(h)] = t
            acc = (acc[0] + t, acc[1] + f)
        return acc

    zero = jnp.zeros((both, LANES), F32)
    rsum, den = (jnp.sum(a, axis=1, keepdims=True)
                 for a in lax.fori_loop(0, blocks, sumbody, (zero, zero), unroll=8))
    rc = jnp.broadcast_to(1.0 / rsum, (both, LANES))
    dc = jnp.broadcast_to(1.0 / den, (both, LANES))
    ld = jnp.broadcast_to(jnp.log(den), (both, LANES))

    def other_codes(q, h):
        view, part = table(q)
        code = cst[view, part, lanes(h)] * rc
        return jnp.concatenate([code[mine:], code[:mine]], axis=0)

    def dzbody(i, acc):
        hs = []
        for x_ in range(LINE):
            for h in VIEWS:
                q = i * LINE + x_
                hs.append(((frow[q, :, lanes(h)] * dc - other_codes(q, h)) * fscale).astype(BF16))
        cl = cfull[lax.div(i, LINE), lax.rem(i, LINE)].reshape(LINE * cols, cols)
        return acc + _nn(jnp.concatenate(hs, axis=1), cl)

    rowgrad = lax.fori_loop(0, LINE * LINE, dzbody, jnp.zeros((both, cols), F32), unroll=8)
    dz[...] = jnp.concatenate([rowgrad[:, :LANES], rowgrad[:, LANES:]], axis=0)

    own = pltpu.make_async_copy(dz, gfull.at[pos[2], pos[1], pos[0]], o_sem.at[0])
    own.start()
    by_core(lambda c: gg[c].s1_send(dz))
    own.wait()

    @pl.when(core == 1)
    def _():
        recv_sums(ITERS - 1, 1)
        send_sums(ITERS - 1, 2)
        denominators(2)

    spread(vall[pos[2], pos[1], pos[0]])
    dacc[...] = jnp.zeros((cols, cols), F32)

    def out_copy(view, i):
        n0 = pl.multiple_of(i * cols, cols)
        return pltpu.make_async_copy(cst.at[view, pl.ds(n0, cols), :], (code1, code2)[view].at[pl.ds(n0, cols), :],
                                     o_sem.at[2 + view])

    def columns(i):
        def body(i, _):
            n0 = pl.multiple_of(i * cols, cols)
            inv = 1.0 / dall[:, pl.ds(n0, cols)]
            code, prob = [], []
            for view in VIEWS:
                w = jnp.concatenate([vb[view], vb[view]], axis=1)
                code.append(e_scr[view, :, :, pl.ds(n0, cols)].reshape(cols, cols) * w * inv[view:view + 1, :])
                prob.append(f_scr[view, :, pl.ds(n0, cols)] * inv[2 + view:3 + view, :])
            for view in VIEWS:
                h = ((prob[view] - code[1 - view]) * fscale).astype(BF16)
                dacc[...] += _nn(h, zs[view][pl.ds(n0, cols), :])
                cst[view, pl.ds(n0, cols), :] = code[view].T
                out_copy(view, i).start()
            return 0
        lax.fori_loop(i * 2, i * 2 + 2, body, 0, unroll=True)

    def lbody(q, acc):
        for h in VIEWS:
            acc = acc + other_codes(q, h) * (lrow[q, :, lanes(h)] - ld)
        return acc
    part = lax.fori_loop(0, blocks, lbody, jnp.zeros((both, LANES), F32), unroll=4)
    grun('A10P')
    lossb[0, pos[0]] = jnp.sum(part.reshape(both // 8, 8, LANES), axis=0)

    def loss_send(st):
        ref = lossb.at[st, pos[st]]
        for d in DISTS:
            remote(ref, ref, l_ssem.at[st], l_rsem.at[st], env.peer(st, d))
        env.sent(lossb.at[st, :LINE - 1], l_ssem.at[st])

    def loss_recv(st):
        env.arrived(lossb.at[st, :LINE - 1], l_rsem.at[st])
        return (lossb[st, 0] + lossb[st, 1]) + (lossb[st, 2] + lossb[st, 3])

    loss_send(0)
    grun('sA11A13A12f10B10Q')

    @pl.when(core == 1)
    def _():
        for (l0, l1), t in zip(_parts(SUM_CUTS), recv_sums(ITERS - 1, AXES - 1)):
            dall[0:2, l0:l1] = t
        denominators(AXES)
        remote(dall.at[:, rows:], dall.at[:, :rows], x_ssem.at[3], x_rsem.at[4], partner)

    lossb[1, pos[1]] = loss_recv(0)
    loss_send(1)
    grun('f11B11f13B13f12B12g10g11A21g13g12A23')
    lossb[2, pos[2]] = loss_recv(1)
    loss_send(2)
    pl.when(core == 0)(lambda: env.arrived(dall.at[:, :rows], x_rsem.at[4]))
    columns(0)
    grun('f20B20b10b11b13b12A22')
    columns(1)
    columns(2)
    grun('f21B21f23B23')
    columns(3)
    dcp = remote(dacc, drecv, l_ssem.at[4], l_rsem.at[4], partner)
    grun('f22B22')
    losst[0] = loss_recv(2)
    lcp = remote(losst.at[0], losst.at[1], l_ssem.at[3], l_rsem.at[3], partner)
    lcp.wait_recv()
    loss_out[...] = jnp.sum(losst[0] + losst[1], keepdims=True) * (-1.0 / (2 * total_rows))
    dcp.wait_recv()
    drecv[...] = dacc[...] + drecv[...]
    gpc = pltpu.make_async_copy(drecv, gp_out, o_sem.at[1])
    gpc.start()
    grun('g20g21g23g22b20b21b23b22')
    gpc.wait()
    for view, out in enumerate((code1, code2)):
        pltpu.make_async_copy(cst.at[view], out, o_sem.at[2 + view]).wait()
    gg[0].all_sent()
    env.sent(losst.at[0], l_ssem.at[3])
    env.sent(dacc, l_ssem.at[4])
    env.drain()

    @pl.when(core == 1)
    def _():
        for i, ref in enumerate((sums.at[0, 0, :AXES, :, :rows], sums.at[0, 1:, :AXES], sums.at[1:, :, :AXES])):
            env.sent(ref, s_ssem.at[i])
        for i, ref in enumerate((vall.at[:LINE - 1], vall.at[0, :LINE - 1], vall.at[0, 0, :LINE - 1], vall)):
            env.sent(ref, v_ssem.at[i])
        env.sent(dall.at[:, rows:], x_ssem.at[3])
        env.drain()


def solution(mesh):
    proto_size = mesh.shape['proto']
    data_size = mesh.shape['data']

    def local_step(emb_one, emb_two, protos):
        rows, dim = emb_one.shape
        cols = protos.shape[0]
        total_rows = rows * data_size
        total_protos = cols * proto_size
        mine = rows // proto_size
        vm = pl.BlockSpec(memory_space=pltpu.VMEM)
        hbm = pl.BlockSpec(memory_space=pltpu.HBM)
        free = pl.BlockSpec(memory_space=pl.ANY)
        dma = lambda n: pltpu.SemaphoreType.DMA((n,))
        one, few, many = dma(1), dma(5), dma(AG_SEMS)
        pair = 2 * mine
        grid3 = (LINE,) * AXES
        packed = (pair * dim // LANES, LANES)
        sds = jax.ShapeDtypeStruct
        code = sds((rows, cols), F32)
        zbuf = pltpu.VMEM((rows, dim), BF16)
        square = pltpu.VMEM((cols, dim), F32)
        rowbuf = pltpu.VMEM((proto_size, pair, cols), F32)
        small = pltpu.VMEM((ITERS, 4, LANES), F32)
        spread = pltpu.VMEM((2, cols, LANES), F32)
        args = [pltpu.with_memory_space_constraint(a, pltpu.HBM) for a in (emb_one, emb_two, protos)]
        code1, code2, loss, gall, gp = pl.pallas_call(
            functools.partial(step_kernel, total_rows, total_protos),
            out_shape=(code, code, sds((1, 1), F32),
                       sds(grid3 + packed, F32), sds((cols, dim), F32)),
            in_specs=[hbm] * 3,
            out_specs=(free, free, vm, free, free),
            scratch_shapes=[
                zbuf, zbuf, zbuf, zbuf, pltpu.VMEM((cols, dim), BF16),
                pltpu.VMEM((2, cols, rows), F32),
                pltpu.VMEM((2, cols // 8, 8, total_rows), F32),
                pltpu.VMEM(grid3 + (cols, dim), BF16),
                rowbuf, rowbuf,
                pltpu.VMEM(grid3 + (4, LANES), F32),
                pltpu.VMEM((pair, dim), BF16),
                pltpu.VMEM((4, total_rows), F32),
                spread, spread,
                pltpu.VMEM((2, 8, total_rows), F32),
                pltpu.VMEM((ITERS, 4, total_rows), F32),
                small, small,
                pltpu.VMEM((ITERS + 1, AXES, LINE, 2, total_rows), F32),
                pltpu.VMEM((AXES, LINE, 8, LANES), F32),
                pltpu.VMEM((2, 8, LANES), F32),
                square, square,
                pltpu.VMEM(packed, F32),
                pltpu.VMEM((2, rows, cols), F32),
                pltpu.VMEM((4, LANES), F32),
                few, one, one, few,
                few, many, one, few, few, one, few, many, few, few, few, few, few,
            ],
            compiler_params=pltpu.CompilerParams(collective_id=0, has_side_effects=True,
                                                 vmem_limit_bytes=44 * 2 ** 20),
        )(*args)
        blocked = sds((proto_size, mine, dim), F32)
        o1, o2, g1, g2, og = pl.pallas_call(
            functools.partial(write_kernel, mine),
            out_shape=(code, code, blocked, blocked, sds((cols, dim), F32)),
            in_specs=[vm] * 4,
            out_specs=(hbm,) * 5,
            scratch_shapes=[dma(9)],
            compiler_params=pltpu.CompilerParams(vmem_limit_bytes=2 ** 20),
        )(code1, code2, gall.reshape((proto_size,) + packed), gp)
        return o1, o2, loss[0, 0], g1.reshape(rows, dim), g2.reshape(rows, dim), og

    return jax.shard_map(
        local_step, mesh=mesh,
        in_specs=(P('data', None), P('data', None), P('proto', None)),
        out_specs=(P('data', 'proto'), P('data', 'proto'), P(), P('data', None), P('data', None), P('proto', None)),
        check_vma=False)
```

```python
import functools
import re

import jax
import jax.numpy as jnp
from jax import lax
from jax.experimental import pallas as pl
from jax.experimental.pallas import tpu as pltpu
from jax.sharding import PartitionSpec as P

TEMP_TAU = 0.1
ITERS = 3
LINE = 4
AXES = 3
MESH = pl.DeviceIdType.MESH
F32 = jnp.float32
BF16 = jnp.bfloat16
LANES = 128
VIEWS = (0, 1)
SCALE = 1.0 / TEMP_TAU
SUM_CUTS = (0, 1408, 2816, 4096)
C_CUTS = (0, 88, 168, 256)
G_CUTS = ((0, 40, 88, 128), (0, 40, 80, 128))
AG_SEMS = 22
DISTS = (2, 1, 3)
WAYS = (1, 3)


def _nt(a, b):
    return lax.dot_general(a, b, (((1,), (1,)), ((), ())), preferred_element_type=F32)


def _nn(a, b):
    return jnp.dot(a, b, preferred_element_type=F32)


def _col_to_row(s):
    r = lax.broadcasted_iota(jnp.int32, (LANES, LANES), 0)
    c = lax.broadcasted_iota(jnp.int32, (LANES, LANES), 1)
    return jnp.sum(jnp.where(r == c, s, 0.0), axis=0, keepdims=True)


def _row_to_col(row, n=LANES, shift=0):
    r = lax.broadcasted_iota(jnp.int32, (n, LANES), 0)
    c = lax.broadcasted_iota(jnp.int32, (n, LANES), 1)
    return jnp.sum(jnp.where(c == r + shift, row, 0.0), axis=1, keepdims=True)


def _parts(cuts):
    return tuple(zip(cuts[:-1], cuts[1:]))


class _Env:
    def __init__(self):
        self.me = lax.axis_index('proto')
        self.core = lax.axis_index('data')
        me = self.me
        self.pos = [lax.rem(me, LINE), lax.rem(lax.div(me, LINE), LINE), lax.div(me, LINE * LINE)]
        self.stride = [1, LINE, LINE * LINE]
        self.pending = []
        self.partner = (me, 1 - self.core)

    def p(self, axis, d):
        return self.pos[axis] if isinstance(d, int) and d == 0 else lax.rem(self.pos[axis] + d, LINE)

    def peer(self, axis, d):
        return (self.me + (self.p(axis, d) - self.pos[axis]) * self.stride[axis], self.core)

    def remote(self, src, dst, ss, rs, dev):
        cp = pltpu.make_async_remote_copy(src, dst, ss, rs, device_id=dev, device_id_type=MESH)
        cp.start()
        return cp

    def sent(self, ref, ss):
        self.pending.append(pltpu.make_async_remote_copy(ref, ref, ss, ss, device_id=self.partner,
                                                         device_id_type=MESH))

    def arrived(self, ref, rs):
        pltpu.make_async_remote_copy(ref, ref, rs, rs, device_id=self.partner, device_id_type=MESH).wait_recv()

    def drain(self):
        for cp in self.pending:
            cp.wait_send()
        self.pending.clear()


class _Gather:
    def __init__(self, env, buf, cuts, ssem, rsem, twin=None, rows=None):
        self.env, self.buf, self.parts = env, buf, _parts(cuts)
        self.ssem, self.rsem, self.twin, self.rows = ssem, rsem, twin, rows

    def at(self, j, i0, i1, i2):
        ids = [None] * AXES
        for axis, i in zip((j, j + 1, j + 2), (i0, i1, i2)):
            ids[axis % AXES] = slice(None) if i is None else i
        r0, r1 = self.parts[j]
        return self.buf.at[ids[2], ids[1], ids[0], r0:r1, :]

    def p(self, j, level, d):
        return self.env.p((j + level) % AXES, d)

    def send(self, j, group, k, ref, level, d, src=None):
        self.env.remote(ref if src is None else src, ref, self.ssem.at[group], self.rsem.at[k],
                        self.env.peer((j + level) % AXES, d))

    def some(self, blocks):
        for level in range(AXES):
            width = LINE ** level
            if blocks <= width * (LINE - 1):
                lead = (0,) * (AXES - 1 - level)
                return self.buf.at[lead + (pl.ds(0, blocks // width),)]

    def recv(self, k, blocks):
        self.env.arrived(self.some(blocks), self.rsem.at[k])

    def all_sent(self):
        for group, blocks in enumerate((3, 8, 4, 32, 16)):
            self.env.sent(self.some(blocks), self.ssem.at[group])

    def s1_send(self, src=None):
        for d in DISTS:
            for j, (r0, r1) in enumerate(self.parts):
                ref = self.at(j, self.p(j, 0, 0), self.p(j, 1, 0), self.p(j, 2, 0))
                self.send(j, 0, 0, ref, 0, d, None if src is None else src.at[r0:r1, :])

    def s1_recv(self):
        self.recv(0, 3)

    def chunk(self, j, level, k, m):
        if level == 1:
            return self.at(j, self.p(j, 0, k), self.p(j, 1, m), self.p(j, 2, 0))
        return self.at(j, None, self.p(j, 1, k), self.p(j, 2, m))

    def slot(self, level, k, d):
        return 1 + 9 * (level - 1) + k + LINE * (d // 2)

    def a_send(self, level, k):
        for j in range(AXES):
            ref = self.chunk(j, level, k, 0)
            for d in WAYS:
                self.send(j, 2 * level - 1, self.slot(level, k, d), ref, level, d)

    def way(self, k):
        return 1 if k < 2 else 3

    def f_recv(self, level, k):
        self.recv(self.slot(level, k, self.way(k)), LINE ** (level - 1))

    def g_recv(self, level, k):
        self.recv(self.slot(level, k, LINE - self.way(k)), LINE ** (level - 1))

    def piece_send(self, *offsets):
        for k in offsets:
            for j in range(AXES):
                ref = self.chunk(j, 1, k, 0)
                for d in WAYS:
                    self.send(j, 3, self.slot(2, 0, d), ref, 2, d)

    def own_piece(self):
        self.piece_send(0)

    def other_pieces(self):
        self.piece_send(1, 3, 2)

    def b_send(self, level, k):
        d = self.way(k)
        for j in range(AXES):
            self.send(j, 2 * level, self.slot(level, k if level > 1 else 0, 5), self.chunk(j, level, k, LINE - d), level, d)

    def b_recv(self, level, k):
        self.recv(self.slot(level, k, 5), LINE)

    def t_send(self, k, m):
        ts, tr = self.twin
        for j in range(AXES):
            ref = self.chunk(j, 2, k, m)
            i = (k == 2) + (m == 2)
            self.env.remote(ref, ref, ts.at[0], tr.at[i], self.env.partner)

    def t_recv(self, group):
        part = (self.buf.at[:3, :3], self.buf.at[:3, :2], self.buf.at[0, 0])[group]
        self.env.arrived(part, self.twin[1].at[group])

    def run(self, ops):
        for op in re.findall('[a-zA-Z][0-9]*', ops):
            args = [int(c) for c in op[1:]]
            {'S': self.s1_send, 's': self.s1_recv, 'A': self.a_send, 'f': self.f_recv, 'g': self.g_recv,
             'B': self.b_send, 'b': self.b_recv, 'T': self.t_send, 'R': self.rows, 'U': self.t_recv, 'P': self.own_piece, 'Q': self.other_pieces}[op[0]](*args)


def write_kernel(mine, code1, code2, gfull, gp, o1, o2, g1, g2, og, sem):
    half = code1.shape[0] // 2
    pairs = [(gp, og)]
    for h in VIEWS:
        for src, dst in ((code1, o1), (code2, o2)):
            pairs.append((src.at[h * half:(h + 1) * half, :], dst.at[h * half:(h + 1) * half, :]))
        for view, dst in enumerate((g1, g2)):
            r = (2 * h + view) * mine
            pairs.append((gfull.at[:, r:r + mine, :], dst.at[:, :, h * LANES:(h + 1) * LANES]))
    copies = [pltpu.make_async_copy(src, dst, sem.at[i]) for i, (src, dst) in enumerate(pairs)]
    for cp in copies:
        cp.start()
    for cp in copies:
        cp.wait()


def step_kernel(total_rows, total_protos, z1h, z2h, ch,
                code1, code2, loss_out, gfull, gp_out,
                z1, z2, y1, y2, c_ref, f_scr, e_scr, cfull, lrow, frow, vall, zr, dall,
                cacc, vb, ub, stage, csend, crecv, sums, lossb, losst, dacc, drecv, dz, cst, vsrc,
                lsem, c_ssem, c_rsem, s_ssem, a_ssem, a_rsem, t_ssem, t_rsem,
                v_ssem, v_rsem, g_ssem, g_rsem, l_ssem, l_rsem, x_ssem, x_rsem, o_sem):
    env = _Env()
    me, core, pos, partner = env.me, env.core, env.pos, env.partner
    remote = env.remote
    rows, cols = z1.shape[0], c_ref.shape[0]
    both = zr.shape[0]
    mine = both // 2
    blocks = LINE ** AXES
    fscale = 1.0 / (2 * total_rows * TEMP_TAU)
    zs, ys = (z1, z2), (y1, y2)
    chunks, groups = rows // cols, cols // 8

    loads = [pltpu.make_async_copy(src, dst, lsem.at[i]) for i, (src, dst) in enumerate(
        ((ch, c_ref), (z1h, z1), (z2h, z2), (ch, cfull.at[pos[2], pos[1], pos[0]])))]
    gg = [_Gather(env, gfull, cuts, g_ssem, g_rsem) for cuts in G_CUTS]

    def by_core(fn):
        for c in VIEWS:
            pl.when(core == c)(functools.partial(fn, c))

    def grun(ops):
        by_core(lambda c: gg[c].run(ops))

    for cp in loads[:3]:
        cp.start()
    barrier = pltpu.get_barrier_semaphore()
    pl.semaphore_signal(barrier, inc=1, device_id=partner, device_id_type=MESH)
    for axis in range(AXES):
        for d in DISTS:
            pl.semaphore_signal(barrier, inc=1, device_id=env.peer(axis, d), device_id_type=MESH)

    def scores(view):
        cacc[view] = jnp.zeros((cols, LANES), F32)

        def body(i, _):
            n0 = pl.multiple_of(i * cols, cols)
            s = _nt(c_ref[...], zs[view][pl.ds(n0, cols), :])
            f = jnp.exp(s * SCALE)
            stage[0, 2 + view:3 + view, pl.ds(n0, cols)] = jnp.sum(f, axis=0, keepdims=True)
            e = f * f
            f_scr[view, :, pl.ds(n0, cols)] = f
            e_scr[view, :, :, pl.ds(n0, cols)] = e.reshape(groups, 8, cols)
            cacc[view] += e[:, :LANES] + e[:, LANES:]
            return 0
        lax.fori_loop(0, chunks, body, 0, unroll=8)
        zr[view * mine:(view + 1) * mine, :] = zs[view][pl.ds(pl.multiple_of(me * mine, mine), mine), :]

    def other_scores(view):
        def body(i, _):
            n0 = pl.multiple_of(i * cols, cols)
            f = jnp.exp(_nt(c_ref[...], ys[view][pl.ds(n0, cols), :]) * SCALE)
            e_scr[view, :, :, pl.ds(rows + n0, cols)] = (f * f).reshape(groups, 8, cols)
            return 0
        lax.fori_loop(0, chunks, body, 0, unroll=2)

    def score_block(offsets):
        z_, y_, x_ = (env.p(axis, d) for axis, d in zip((2, 1, 0), offsets))
        q = (z_ * LINE + y_) * LINE + x_
        l = _nt(zr[...], cfull[z_, y_, x_]) * SCALE
        lrow[q] = l
        frow[q] = jnp.exp(l)

    def near(i):
        return i + lax.div(i, 2)

    def row_scores(piece):
        def spot(axis, d, rest):
            rest = list(rest)
            rest.insert(axis, d)
            score_block(rest)

        def body(i, _):
            a, b = near(lax.div(i, 3)), near(lax.rem(i, 3))
            if piece < 3:
                spot(0, near(jnp.int32(piece)), (a, b))
            elif piece < 6:
                spot(piece - 3, 2, (a, b))
            return 0

        def last(i, _):
            for axis in range(AXES):
                spot(axis, near(i), (2, 2))
            return 0
        if piece < 6:
            lax.fori_loop(0, 9, body, 0, unroll=True)
        else:
            lax.fori_loop(0, 3, last, 0, unroll=True)
            score_block((2, 2, 2))

    gc = _Gather(env, cfull, C_CUTS, a_ssem, a_rsem, (t_ssem, t_rsem), row_scores)

    def block(q):
        return lax.div(q, LINE * LINE), lax.rem(lax.div(q, LINE), LINE), lax.rem(q, LINE)

    def column_sums(it):
        for view in VIEWS:
            for h in VIEWS:
                k = 2 * view + h
                s = jnp.sum(cacc[view, h * LANES:(h + 1) * LANES, :], axis=1, keepdims=True)
                csend[it, k:k + 1, :] = _col_to_row(s)

    def spread(vrow):
        for view in VIEWS:
            for h in VIEWS:
                k = 2 * view + h
                vb[view, h * LANES:(h + 1) * LANES, :] = jnp.broadcast_to(
                    _row_to_col(vrow[k:k + 1, :]), (LANES, LANES))

    def exchange():
        return remote(csend.at[0], crecv.at[0], c_ssem.at[0], c_rsem.at[0], partner)

    def row_sums(it, width):
        tiles = [slice(l, l + LANES) for l in range(0, width, LANES)]
        for view in VIEWS:
            def body(g, acc, view=view):
                w = vb[view, pl.ds(pl.multiple_of(g * 8, 8), 8), :]
                return tuple(a + e_scr[view, g, :, ls] * w for a, ls in zip(acc, tiles))
            acc = lax.fori_loop(0, groups, body, tuple(jnp.zeros((8, LANES), F32) for _ in tiles), unroll=8)
            for a, ls in zip(acc, tiles):
                stage[it, view:view + 1, ls] = jnp.sum(a, axis=0, keepdims=True)

    def weighted_columns():
        tiles = [slice(l, l + LANES) for l in range(0, 2 * rows, LANES)]
        for view in VIEWS:
            us = [ub[view, :, ls] for ls in tiles]

            def body(g, _, view=view, us=us):
                terms = [e_scr[view, g, :, ls] * u for ls, u in zip(tiles, us)]
                chains = [sum(terms[t::LINE][1:], terms[t]) for t in range(LINE)]
                cacc[view, pl.ds(pl.multiple_of(g * 8, 8), 8), :] = (chains[0] + chains[1]) + (chains[2] + chains[3])
                return 0
            lax.fori_loop(0, groups, body, 0, unroll=8)

    def at_offset(oz, oy, ox):
        return (env.p(2, oz) * LINE + env.p(1, oy)) * LINE + env.p(0, ox)

    def broadcast_v():
        dst = vall.at[pos[2], pos[1], pos[0]]
        pltpu.make_async_copy(vsrc, dst, v_rsem.at[0]).start()
        order = DISTS + (0,)
        for oz in order:
            for oy in order:
                for ox in order:
                    there = at_offset(oz, oy, ox)
                    if oz or oy or ox:
                        group = 0 if oz else 1 if oy else 2
                        remote(vsrc, dst, v_ssem.at[group], v_rsem.at[0], (there, 1))
                    remote(vsrc, dst, v_ssem.at[3], v_rsem.at[0], (there, 0))

    def within(lo, hi):
        return [(j, max(l0, lo), min(l1, hi)) for j, (l0, l1) in enumerate(_parts(SUM_CUTS)) if l0 < hi and l1 > lo]

    def load_sums(it, part, hi):
        for j, l0, l1 in within(0, hi):
            sums[it, 0, pos[j], :, l0:l1] = stage[part + (slice(l0, l1),)]

    def send_sums(it, st):
        for d in DISTS:
            for j, l0, l1 in within(0, rows if it + st == 0 else total_rows):
                ax = (st + j) % AXES
                src = sums.at[it, st, pos[ax], :, l0:l1]
                remote(src, src, s_ssem.at[2 if it else min(st, 1)], a_rsem.at[it * AXES + st], env.peer(ax, d))

    def send_first():
        for d in DISTS + (0,):
            for j, l0, l1 in within(rows, total_rows):
                src = sums.at[0, 0, pos[j], :, l0:l1]
                if d:
                    remote(src, src, x_ssem.at[3], a_rsem.at[0], (env.peer(j, d)[0], 1))
                else:
                    remote(src, src, x_ssem.at[3], x_rsem.at[3], partner)

    def recv_sums(it, st):
        if it + st == 0:
            env.arrived(sums.at[0, 0, 0, :, rows:], x_rsem.at[3])
        env.arrived(sums.at[it, st, :LINE - 1], a_rsem.at[it * AXES + st])
        tot = []
        for j, (l0, l1) in enumerate(_parts(SUM_CUTS)):
            s = [sums[it, st, i, :, l0:l1] for i in range(LINE)]
            t = (s[0] + s[1]) + (s[2] + s[3])
            tot.append(t)
            if st < AXES - 1:
                sums[it, st + 1, pos[(st + 1 + j) % AXES], :, l0:l1] = t
        return tot

    def denominators(st):
        if st == 0:
            env.arrived(stage.at[0, :, rows:], x_rsem.at[2])
            load_sums(ITERS, (0, slice(2, 4)), total_rows)
        else:
            tot = recv_sums(ITERS, st - 1)
        if st < AXES:
            send_sums(ITERS, st)
            return
        for (l0, l1), t in zip(_parts(SUM_CUTS), tot):
            dall[2:4, l0:l1] = t

    def hidden(slot):
        if slot in (1, 2):
            env.arrived(ys[slot - 1], x_rsem.at[slot - 1])
            other_scores(slot - 1)
        if slot == 6:
            denominators(0)
            gc.run('U0R0R1R2U1R3R4R5U2R6')

    @pl.when(core == 1)
    def _():
        loads[0].wait()
        for view in VIEWS:
            loads[1 + view].wait()
            scores(view)
        pl.semaphore_wait(barrier, 1 + AXES * (LINE - 1))
        column_sums(0)
        exchange().wait()
        total = csend[0] + crecv[0]
        for it in range(ITERS):
            last = it == ITERS - 1
            vrow = 1.0 / (float(total_protos) * total)
            if last:
                vsrc[...] = vrow
                broadcast_v()
            spread(vrow)
            row_sums(it, rows if it == 0 else 2 * rows)
            load_sums(it, (it, slice(0, 2)), rows if it == 0 else total_rows)
            for st in range(AXES):
                send_sums(it, st)
                hidden(it * AXES + st)
                tot = recv_sums(it, st)
                if last:
                    send_sums(it, 1)
                    denominators(1)
                    break
                if st < AXES - 1:
                    continue
                for (l0, l1), t in zip(_parts(SUM_CUTS), tot):
                    u = 1.0 / (float(total_rows) * t)
                    for view in VIEWS:
                        ub[view, :, l0:l1] = jnp.broadcast_to(u[view:view + 1], (8, l1 - l0))
            if not last:
                weighted_columns()
                column_sums(it + 1)
                total = csend[it + 1]

    @pl.when(core == 0)
    def _():
        loads[3].start()
        loads[0].wait()
        for view in VIEWS:
            loads[1 + view].wait()
            scores(view)
        column_sums(0)
        loads[3].wait()
        pl.semaphore_wait(barrier, 1 + AXES * (LINE - 1))
        cp = exchange()
        gc.run('S')
        cp.wait()
        vrow = 1.0 / (float(total_protos) * (csend[0] + crecv[0]))
        spread(vrow)
        row_sums(0, rows)
        for j, l0, l1 in within(rows, total_rows):
            sums[0, 0, pos[j], :, l0:l1] = stage[0, 0:2, l0 - rows:l1 - rows]
        send_first()
        gc.run('A10P')
        remote(stage.at[0, :, :rows], stage.at[0, :, rows:], x_ssem.at[2], x_rsem.at[2], partner)
        for i in VIEWS:
            remote(zs[i], ys[i], x_ssem.at[i], x_rsem.at[i], partner)
        gc.run('sA11A13A12QT00')
        gc.run('f10B10f11B11f13B13f12B12g10g11A21g13g12A23')
        gc.run('f20B20b10A22T10T30T20')
        gc.run('f21B21f23B23g20g21g23T01T03T11T13T31T33R0')
        gc.run('f22B22R1g22T21T23b20T02b21T12R2')
        gc.run('b23T32R3b22T22R4R5R6')
        gc.all_sent()
        for i, ref in enumerate((z1, z2, stage.at[0, :, :rows], sums.at[0, 0, :2])):
            env.sent(ref, x_ssem.at[i])
        env.sent(cfull, t_ssem.at[0])
        env.drain()

    env.arrived(vall, v_rsem.at[0])

    def lanes(h):
        return slice(h * LANES, (h + 1) * LANES)

    def table(q):
        return lax.div(q, blocks // 2), pl.ds(pl.multiple_of(lax.rem(q, blocks // 2) * both, both), both)

    def sumbody(q, acc):
        z_, y_, x_ = block(q)
        view, part = table(q)
        for h in VIEWS:
            f = frow[q, :, lanes(h)]
            v0 = jnp.broadcast_to(vall[z_, y_, x_, h:h + 1, :], (mine, LANES))
            v1 = jnp.broadcast_to(vall[z_, y_, x_, 2 + h:3 + h, :], (mine, LANES))
            t = f * f * jnp.concatenate([v0, v1], axis=0)
            cst[view, part, lanes(h)] = t
            acc = (acc[0] + t, acc[1] + f)
        return acc

    zero = jnp.zeros((both, LANES), F32)
    rsum, den = (jnp.sum(a, axis=1, keepdims=True)
                 for a in lax.fori_loop(0, blocks, sumbody, (zero, zero), unroll=8))
    rc = jnp.broadcast_to(1.0 / rsum, (both, LANES))
    dc = jnp.broadcast_to(1.0 / den, (both, LANES))
    ld = jnp.broadcast_to(jnp.log(den), (both, LANES))

    def other_codes(q, h):
        view, part = table(q)
        code = cst[view, part, lanes(h)] * rc
        return jnp.concatenate([code[mine:], code[:mine]], axis=0)

    def dzbody(i, acc):
        hs = []
        for x_ in range(LINE):
            for h in VIEWS:
                q = i * LINE + x_
                hs.append(((frow[q, :, lanes(h)] * dc - other_codes(q, h)) * fscale).astype(BF16))
        cl = cfull[lax.div(i, LINE), lax.rem(i, LINE)].reshape(LINE * cols, cols)
        return acc + _nn(jnp.concatenate(hs, axis=1), cl)

    rowgrad = lax.fori_loop(0, LINE * LINE, dzbody, jnp.zeros((both, cols), F32), unroll=8)
    dz[...] = jnp.concatenate([rowgrad[:, :LANES], rowgrad[:, LANES:]], axis=0)

    own = pltpu.make_async_copy(dz, gfull.at[pos[2], pos[1], pos[0]], o_sem.at[0])
    own.start()
    by_core(lambda c: gg[c].s1_send(dz))
    own.wait()

    @pl.when(core == 1)
    def _():
        recv_sums(ITERS - 1, 1)
        send_sums(ITERS - 1, 2)
        denominators(2)

    spread(vall[pos[2], pos[1], pos[0]])
    dacc[...] = jnp.zeros((cols, cols), F32)

    def out_copy(view, i):
        n0 = pl.multiple_of(i * cols, cols)
        return pltpu.make_async_copy(cst.at[view, pl.ds(n0, cols), :], (code1, code2)[view].at[pl.ds(n0, cols), :],
                                     o_sem.at[2 + view])

    def columns(i):
        def body(i, _):
            n0 = pl.multiple_of(i * cols, cols)
            inv = 1.0 / dall[:, pl.ds(n0, cols)]
            code, prob = [], []
            for view in VIEWS:
                w = jnp.concatenate([vb[view], vb[view]], axis=1)
                code.append(e_scr[view, :, :, pl.ds(n0, cols)].reshape(cols, cols) * w * inv[view:view + 1, :])
                prob.append(f_scr[view, :, pl.ds(n0, cols)] * inv[2 + view:3 + view, :])
            for view in VIEWS:
                h = ((prob[view] - code[1 - view]) * fscale).astype(BF16)
                dacc[...] += _nn(h, zs[view][pl.ds(n0, cols), :])
                cst[view, pl.ds(n0, cols), :] = code[view].T
                out_copy(view, i).start()
            return 0
        lax.fori_loop(i * 2, i * 2 + 2, body, 0, unroll=True)

    def lbody(q, acc):
        for h in VIEWS:
            acc = acc + other_codes(q, h) * (lrow[q, :, lanes(h)] - ld)
        return acc
    part = lax.fori_loop(0, blocks, lbody, jnp.zeros((both, LANES), F32), unroll=4)
    grun('A10P')
    lossb[0, pos[0]] = jnp.sum(part.reshape(both // 8, 8, LANES), axis=0)

    def loss_send(st):
        ref = lossb.at[st, pos[st]]
        for d in DISTS:
            remote(ref, ref, l_ssem.at[st], l_rsem.at[st], env.peer(st, d))
        env.sent(lossb.at[st, :LINE - 1], l_ssem.at[st])

    def loss_recv(st):
        env.arrived(lossb.at[st, :LINE - 1], l_rsem.at[st])
        return (lossb[st, 0] + lossb[st, 1]) + (lossb[st, 2] + lossb[st, 3])

    loss_send(0)
    grun('sA11A13A12f10B10Q')

    @pl.when(core == 1)
    def _():
        for (l0, l1), t in zip(_parts(SUM_CUTS), recv_sums(ITERS - 1, AXES - 1)):
            dall[0:2, l0:l1] = t
        denominators(AXES)
        remote(dall.at[:, rows:], dall.at[:, :rows], x_ssem.at[3], x_rsem.at[4], partner)

    lossb[1, pos[1]] = loss_recv(0)
    loss_send(1)
    grun('f11B11f13B13f12B12g10g11A21g13g12A23')
    lossb[2, pos[2]] = loss_recv(1)
    loss_send(2)
    pl.when(core == 0)(lambda: env.arrived(dall.at[:, :rows], x_rsem.at[4]))
    columns(0)
    grun('f20B20b10A22')
    columns(1)
    columns(2)
    grun('f21B21f23B23')
    columns(3)
    dcp = remote(dacc, drecv, l_ssem.at[4], l_rsem.at[4], partner)
    grun('f22B22')
    losst[0] = loss_recv(2)
    lcp = remote(losst.at[0], losst.at[1], l_ssem.at[3], l_rsem.at[3], partner)
    lcp.wait_recv()
    loss_out[...] = jnp.sum(losst[0] + losst[1], keepdims=True) * (-1.0 / (2 * total_rows))
    dcp.wait_recv()
    drecv[...] = dacc[...] + drecv[...]
    gpc = pltpu.make_async_copy(drecv, gp_out, o_sem.at[1])
    gpc.start()
    grun('g20g21g23g22b20b21b23b22')
    gpc.wait()
    for view, out in enumerate((code1, code2)):
        pltpu.make_async_copy(cst.at[view], out, o_sem.at[2 + view]).wait()
    gg[0].all_sent()
    env.sent(losst.at[0], l_ssem.at[3])
    env.sent(dacc, l_ssem.at[4])
    env.drain()

    @pl.when(core == 1)
    def _():
        for i, ref in enumerate((sums.at[0, 0, :AXES, :, :rows], sums.at[0, 1:, :AXES], sums.at[1:, :, :AXES])):
            env.sent(ref, s_ssem.at[i])
        for i, ref in enumerate((vall.at[:LINE - 1], vall.at[0, :LINE - 1], vall.at[0, 0, :LINE - 1], vall)):
            env.sent(ref, v_ssem.at[i])
        env.sent(dall.at[:, rows:], x_ssem.at[3])
        env.drain()


def solution(mesh):
    proto_size = mesh.shape['proto']
    data_size = mesh.shape['data']

    def local_step(emb_one, emb_two, protos):
        rows, dim = emb_one.shape
        cols = protos.shape[0]
        total_rows = rows * data_size
        total_protos = cols * proto_size
        mine = rows // proto_size
        vm = pl.BlockSpec(memory_space=pltpu.VMEM)
        hbm = pl.BlockSpec(memory_space=pltpu.HBM)
        free = pl.BlockSpec(memory_space=pl.ANY)
        dma = lambda n: pltpu.SemaphoreType.DMA((n,))
        one, four, few, many = dma(1), dma(4), dma(5), dma(AG_SEMS)
        pair = 2 * mine
        grid3 = (LINE,) * AXES
        packed = (pair * dim // LANES, LANES)
        sds = jax.ShapeDtypeStruct
        code = sds((rows, cols), F32)
        zbuf = pltpu.VMEM((rows, dim), BF16)
        square = pltpu.VMEM((cols, dim), F32)
        rowbuf = pltpu.VMEM((proto_size, pair, cols), F32)
        small = pltpu.VMEM((ITERS, 4, LANES), F32)
        spread = pltpu.VMEM((2, cols, LANES), F32)
        args = [pltpu.with_memory_space_constraint(a, pltpu.HBM) for a in (emb_one, emb_two, protos)]
        code1, code2, loss, gall, gp = pl.pallas_call(
            functools.partial(step_kernel, total_rows, total_protos),
            out_shape=(code, code, sds((1, 1), F32),
                       sds(grid3 + packed, F32), sds((cols, dim), F32)),
            in_specs=[hbm] * 3,
            out_specs=(free, free, vm, free, free),
            scratch_shapes=[
                zbuf, zbuf, zbuf, zbuf, pltpu.VMEM((cols, dim), BF16),
                pltpu.VMEM((2, cols, rows), F32),
                pltpu.VMEM((2, cols // 8, 8, total_rows), F32),
                pltpu.VMEM(grid3 + (cols, dim), BF16),
                rowbuf, rowbuf,
                pltpu.VMEM(grid3 + (4, LANES), F32),
                pltpu.VMEM((pair, dim), BF16),
                pltpu.VMEM((4, total_rows), F32),
                spread, spread,
                pltpu.VMEM((2, 8, total_rows), F32),
                pltpu.VMEM((ITERS, 4, total_rows), F32),
                small, small,
                pltpu.VMEM((ITERS + 1, AXES, LINE, 2, total_rows), F32),
                pltpu.VMEM((AXES, LINE, 8, LANES), F32),
                pltpu.VMEM((2, 8, LANES), F32),
                square, square,
                pltpu.VMEM(packed, F32),
                pltpu.VMEM((2, rows, cols), F32),
                pltpu.VMEM((4, LANES), F32),
                four, one, one, four,
                few, many, one, four, four, one, few, many, few, few, four, few, four,
            ],
            compiler_params=pltpu.CompilerParams(collective_id=0, has_side_effects=True,
                                                 vmem_limit_bytes=44 * 2 ** 20),
        )(*args)
        blocked = sds((proto_size, mine, dim), F32)
        o1, o2, g1, g2, og = pl.pallas_call(
            functools.partial(write_kernel, mine),
            out_shape=(code, code, blocked, blocked, sds((cols, dim), F32)),
            in_specs=[vm] * 4,
            out_specs=(hbm,) * 5,
            scratch_shapes=[dma(9)],
            compiler_params=pltpu.CompilerParams(vmem_limit_bytes=2 ** 20),
        )(code1, code2, gall.reshape((proto_size,) + packed), gp)
        return o1, o2, loss[0, 0], g1.reshape(rows, dim), g2.reshape(rows, dim), og

    return jax.shard_map(
        local_step, mesh=mesh,
        in_specs=(P('data', None), P('data', None), P('proto', None)),
        out_specs=(P('data', 'proto'), P('data', 'proto'), P(), P('data', None), P('data', None), P('proto', None)),
        check_vma=False)
```
